8 devices in a mesh: batch: 1 (over z), gz: 2 (over y), gy: 2 (over x), gx: 2 (over core).
Axes of the slice: x: 2, y: 2, z: 1, core: 2. Of those that a mesh axis runs over, the one named last changes fastest.
Arguments:
- rhs_grid: float32 [256, 256, 256], P(('batch', 'gz'), 'gy', 'gx')
- init_grid: float32 [256, 256, 256], P(('batch', 'gz'), 'gy', 'gx')
- coarse_inv: float32 [512, 512], replicated
Outputs:
- output: float32 [256, 256, 256], P(('batch', 'gz'), 'gy', 'gx')
All inputs are finite; a program needn't handle non-finite values.
Results may differ from the reference program's by a relative error of at most 0.001.
Values sent between devices are 32-bit elements.
A program may use at most 1 GiB of HBM per device.

```python
import jax
import jax.numpy as jnp
from jax import lax

COARSE = 8
LEVELS = 5
CYCLES = 2
SWEEPS = 2
MODES = 8
N = COARSE * 2 ** LEVELS
OMEGA = 2.0 / 3.0


def with_ghosts(iterate, axis_id):
    extent = iterate.shape[axis_id]
    first_face = lax.slice_in_dim(iterate, 0, 1, axis=axis_id)
    last_face = lax.slice_in_dim(iterate, extent - 1, extent, axis=axis_id)
    return jnp.concatenate([-first_face, iterate, -last_face], axis=axis_id)


def neighbour_sum(iterate):
    nbr_total = jnp.zeros_like(iterate)
    for axis_id in range(3):
        extent = iterate.shape[axis_id]
        padded = with_ghosts(iterate, axis_id)
        nbr_total = nbr_total + lax.slice_in_dim(padded, 0, extent, axis=axis_id) + lax.slice_in_dim(padded, 2, extent + 2, axis=axis_id)
    return nbr_total


def jacobi(iterate, source, edge_cells):
    return (1.0 - OMEGA) * iterate + (OMEGA / 6.0) * (source * (1.0 / (edge_cells * edge_cells)) + neighbour_sum(iterate))


def residual(iterate, source, edge_cells):
    return source - (6.0 * iterate - neighbour_sum(iterate)) * float(edge_cells * edge_cells)


def restrict(fine_grid):
    dim_z, dim_y, dim_x = fine_grid.shape
    return fine_grid.reshape(dim_z // 2, 2, dim_y // 2, 2, dim_x // 2, 2).mean(axis=(1, 3, 5))


def prolong(coarse):
    for axis_id in range(3):
        extent = coarse.shape[axis_id]
        padded = with_ghosts(coarse, axis_id)
        low_child = 0.75 * coarse + 0.25 * lax.slice_in_dim(padded, 0, extent, axis=axis_id)
        high_child = 0.75 * coarse + 0.25 * lax.slice_in_dim(padded, 2, extent + 2, axis=axis_id)
        new_shape = list(coarse.shape)
        new_shape[axis_id] = 2 * extent
        coarse = jnp.stack([low_child, high_child], axis=axis_id + 1).reshape(new_shape)
    return coarse


def vcycle(iterate, source, level_id, coarse_inv):
    if level_id == LEVELS:
        flat_rhs = source.reshape(-1)
        return jnp.dot(coarse_inv, flat_rhs, precision=lax.Precision.HIGHEST).reshape(source.shape)
    edge_cells = N // 2 ** level_id
    for sweep_id in range(SWEEPS):
        iterate = jacobi(iterate, source, edge_cells)
    coarse_rhs = restrict(residual(iterate, source, edge_cells))
    correction = vcycle(jnp.zeros_like(coarse_rhs), coarse_rhs, level_id + 1, coarse_inv)
    iterate = iterate + prolong(correction)
    for sweep_id in range(SWEEPS):
        iterate = jacobi(iterate, source, edge_cells)
    return iterate


def smooth_field(rand_key, extent):
    coeffs = jax.random.normal(rand_key, (MODES, MODES, MODES), jnp.float32)
    wavenum = jnp.arange(1, MODES + 1).astype(jnp.float32)
    weight = (wavenum[:, None, None] ** 2 + wavenum[None, :, None] ** 2 + wavenum[None, None, :] ** 2) ** -0.5
    centres = (jnp.arange(extent).astype(jnp.float32) + 0.5) / extent
    sine_table = jnp.sin(jnp.pi * wavenum[:, None] * centres[None, :])
    smooth = jnp.einsum('abc,ai,bj,ck->ijk', coeffs * weight, sine_table, sine_table, sine_table)
    return smooth / jnp.sqrt(jnp.mean(smooth * smooth))


def coarse_inverse(rand_key):
    scale_key, diag_key = jax.random.split(rand_key)
    cell_ids = jnp.arange(COARSE)
    line_diag = 2.0 + (cell_ids == 0).astype(jnp.float32) + (cell_ids == COARSE - 1).astype(jnp.float32)
    line_op = jnp.diag(line_diag) - jnp.eye(COARSE, k=1, dtype=jnp.float32) - jnp.eye(COARSE, k=-1, dtype=jnp.float32)
    identity = jnp.eye(COARSE, dtype=jnp.float32)
    laplace = (jnp.kron(jnp.kron(line_op, identity), identity) + jnp.kron(jnp.kron(identity, line_op), identity) + jnp.kron(jnp.kron(identity, identity), line_op)) * float(COARSE * COARSE)
    shift_scale = jax.random.uniform(scale_key, (), jnp.float32, 0.5, 1.5)
    shifts = 30.0 * shift_scale * jax.random.uniform(diag_key, (COARSE ** 3,), jnp.float32, 0.5, 1.5)
    return jnp.linalg.inv(laplace + jnp.diag(shifts))


def setup_inputs(seed: int = 0, part: int = 0) -> dict:
    key_list = jax.random.split(jax.random.key(seed), 5)
    rhs_smooth_key = jax.random.fold_in(key_list[0], part)
    rhs_noise_key = jax.random.fold_in(key_list[1], part)
    init_smooth_key = jax.random.fold_in(key_list[2], part)
    init_noise_key = jax.random.fold_in(key_list[3], part)
    rhs_grid = 30.0 * smooth_field(rhs_smooth_key, N) + 10.0 * jax.random.normal(rhs_noise_key, (N, N, N), jnp.float32)
    init_grid = smooth_field(init_smooth_key, N) + 0.5 * jax.random.normal(init_noise_key, (N, N, N), jnp.float32)
    coarse_inv = coarse_inverse(key_list[4])
    return {'rhs_grid': rhs_grid, 'init_grid': init_grid, 'coarse_inv': coarse_inv}


def reference(rhs_grid, init_grid, coarse_inv):
    iterate = init_grid
    for cycle_id in range(CYCLES):
        iterate = vcycle(iterate, rhs_grid, 0, coarse_inv)
    return iterate
```

```python
import jax
import jax.numpy as jnp
from jax import lax
from jax.experimental import pallas as pl
from jax.experimental.pallas import tpu as pltpu
from jax.sharding import PartitionSpec as P

OMEGA = 2.0 / 3.0
C6 = OMEGA / 6.0
CYCLES = 2
MESH = pl.DeviceIdType.MESH
F32 = jnp.float32
SUB, LN = 8, 128
HALO_PLANES = {1: 4, 2: 5}


class Level:
    def __init__(self, idx, n, off, shape, pos, split):
        self.idx, self.n, self.shape = idx, n, shape
        self.oz, self.oy, self.ox = off
        self.split = split
        if split:
            self.lo = tuple(o - p * n for o, p in zip(off, pos))
            self.hi = tuple(l + 2 * n for l in self.lo)
        else:
            self.lo = off
            self.hi = tuple(o + n for o in off)
        wide = SUB if (split and idx > 0) else 0
        self.zs = self.oz - wide * pos[0] if wide else self.oz
        self.ys = self.oy - wide * pos[1] if wide else self.oy
        self.nzb = (n + wide) // SUB
        self.nyt = (n + wide) // SUB
        if split:
            self.ghosts = [(jnp.where(pos[0] == 0, self.oz - 1, self.oz + n), jnp.where(pos[0] == 0, self.oz, self.oz + n - 1))]
        else:
            self.ghosts = [(self.oz - 1, self.oz), (self.oz + n, self.oz + n - 1)]


def solve_kernel(f_hbm, u_hbm, c_hbm, out_hbm,
                 ua, ub, fr, tr, v1a, v1b, b1, v2a, v2b, b2, v3a, v3b, b3, v4a, v4b, b4, e5, b5, cinv,
                 xs, xg, yp, yg, p1s, p1r, p2s, p2r, g3, ssem, rsem, lsem):
    pz, py, px = lax.axis_index('gz'), lax.axis_index('gy'), lax.axis_index('gx')
    pos = (pz, py, px)
    lane = lax.broadcasted_iota(jnp.int32, (SUB, LN), 1)
    row = lax.broadcasted_iota(jnp.int32, (SUB, LN), 0)
    levels = [
        Level(0, LN, (1, SUB, 0), (130, 144), pos, True),
        Level(1, 64, (9, 16, 32), (82, 96), pos, True),
        Level(2, 32, (9, 16, 48), (50, 64), pos, True),
        Level(3, 32, (1, 16, 48), (34, 72), pos, False),
        Level(4, 16, (1, 16, 48), (18, 48), pos, False),
        Level(5, SUB, (1, 16, 48), (10, 32), pos, False),
    ]
    lev0 = levels[0]
    bnd = jnp.where(px == 0, 0, 127)
    recv = 127 - bnd
    sh_in = jnp.where(px == 0, 1, 127)
    sh_out = LN - sh_in

    def dev(code):
        ids = {}
        if code & 4:
            ids['gz'] = 1 - pz
        if code & 2:
            ids['gy'] = 1 - py
        if code & 1:
            ids['gx'] = 1 - px
        return ids

    def remote(src, dst, k, code):
        return pltpu.make_async_remote_copy(src_ref=src, dst_ref=dst, send_sem=ssem.at[k], recv_sem=rsem.at[k],
                                            device_id=dev(code), device_id_type=MESH)

    def loop(n, body):
        lax.fori_loop(0, n, lambda i, c: (body(i), c)[1], 0)

    load_u = pltpu.make_async_copy(u_hbm, ua.at[pl.ds(1, LN), pl.ds(SUB, LN), :], lsem.at[0])
    load_f = pltpu.make_async_copy(f_hbm, fr, lsem.at[1])
    load_c = [pltpu.make_async_copy(c_hbm.at[:, pl.ds(LN * j, LN)], cinv.at[j], lsem.at[2 + j]) for j in range(4)]
    load_u.start()
    load_f.start()
    for copy in load_c:
        copy.start()

    def zero(ref):
        planes, rows = ref.shape[0], ref.shape[1]

        def body(i):
            ref[i] = jnp.zeros((rows, LN), F32)
        loop(planes, body)

    for ref in (v1a, v1b, b1, v2a, v2b, b2, v3a, v3b, b3, v4a, v4b, b4, e5):
        zero(ref)

    def zero_rows(i):
        for ref in (ua, ub):
            ref[i, pl.ds(0, SUB), :] = jnp.zeros((SUB, LN), F32)
            ref[i, pl.ds(136, SUB), :] = jnp.zeros((SUB, LN), F32)
    loop(130, zero_rows)

    barrier = pltpu.get_barrier_semaphore()
    for code in range(1, SUB):
        pl.semaphore_signal(barrier, inc=1, device_id=dev(code), device_id_type=MESH)
    pl.semaphore_wait(barrier, 7)

    def coefs(lev, y0):
        r = row + y0
        inside = (r >= lev.lo[1]) & (r < lev.hi[1]) & (lane >= lev.lo[2]) & (lane < lev.hi[2])
        one, nil = jnp.ones((SUB, LN), F32), jnp.zeros((SUB, LN), F32)
        nb = (jnp.where(r == lev.lo[1], one, nil) + jnp.where(r == lev.hi[1] - 1, one, nil)
              + jnp.where(lane == lev.lo[2], one, nil) + jnp.where(lane == lev.hi[2] - 1, one, nil))
        return inside, nb

    def zghost_tile(lev, ref, y0):
        for ghost, face in lev.ghosts:
            ref[ghost, pl.ds(y0, SUB), :] = -ref[face, pl.ds(y0, SUB), :]

    def zghost(lev, ref):
        loop(lev.shape[1] // SUB, lambda t: zghost_tile(lev, ref, pl.multiple_of(SUB * t, SUB)))

    def plain_sum(src, z0, y0):
        u = src[pl.ds(z0 - 1, 10), pl.ds(y0, SUB), :]
        c = u[1:9]
        s = u[0:SUB] + u[2:10]
        s = s + src[pl.ds(z0, SUB), pl.ds(y0 - 1, SUB), :] + src[pl.ds(z0, SUB), pl.ds(y0 + 1, SUB), :]
        return c, s

    def full_sum(lev, src, z0, y0, ghost):
        c, s = plain_sum(src, z0, y0)
        if lev.idx:
            return c, s + pltpu.roll(c, 1, 2) + pltpu.roll(c, 127, 2)
        k = z0 - 1
        g = jnp.stack([pltpu.roll(ghost, lax.rem(recv + LN - (k + j), LN), 1) for j in range(SUB)])
        inner = pltpu.roll(c, sh_in, 2)
        outer = pltpu.roll(c, sh_out, 2)
        s = s + jnp.where((lane == bnd)[None], 0.0, inner) + jnp.where((lane == recv)[None], g, outer)
        return c, s

    def pack_block(block, k, pk):
        for j in range(SUB):
            pk = jnp.where(lane == k + j, pltpu.roll(block[j], lax.rem(k + j + LN - recv, LN), 1), pk)
        return pk

    def sweep(lev, src, dst, rhs, par=0):
        first = rhs is None

        def ytile(t):
            y0 = pl.multiple_of(lev.ys + SUB * t, SUB)
            inside, nb = coefs(lev, y0)
            cc = (1.0 - OMEGA) - C6 * nb
            if first:
                ca, cb = jnp.where(inside, C6 * (cc + 1.0), 0.0), jnp.where(inside, C6 * C6, 0.0)
            elif lev.idx:
                ca, cb = jnp.where(inside, cc, 0.0), jnp.where(inside, C6, 0.0)
            else:
                ca, cb = cc, C6
            ghost = None if lev.idx else xg[par, pl.ds(pl.multiple_of(SUB * t, SUB), SUB), :]

            def zblk(k, pk):
                z0 = lev.zs + SUB * k
                c, s = full_sum(lev, src, z0, y0, ghost)
                if lev.idx == 0:
                    s = s + fr[pl.ds(SUB * k, SUB), pl.ds(pl.multiple_of(SUB * t, SUB), SUB), :] * (1.0 / 65536.0)
                elif not first:
                    s = s + rhs[pl.ds(z0, SUB), pl.ds(y0, SUB), :]
                new = ca * c + cb * s
                dst[pl.ds(z0, SUB), pl.ds(y0, SUB), :] = new
                return pk if lev.idx else pack_block(new, SUB * k, pk)

            pk = lax.fori_loop(0, lev.nzb, zblk, jnp.zeros((SUB, LN), F32))
            if lev.idx == 0:
                xs[1 - par, pl.ds(pl.multiple_of(SUB * t, SUB), SUB), :] = pk
            zghost_tile(lev, dst, y0)

        loop(lev.nyt, ytile)

    def residual_pass(lev, src, rhs, par=0):
        def ytile(t):
            y0 = pl.multiple_of(lev.oy + SUB * t, SUB)
            t0 = pl.multiple_of(SUB * t, SUB)
            _, nb = coefs(lev, y0)
            dd = 6.0 + nb
            ghost = None if lev.idx else xg[par, pl.ds(t0, SUB), :]

            def zblk(k):
                z0 = lev.oz + SUB * k
                c, s = full_sum(lev, src, z0, y0, ghost)
                if lev.idx == 0:
                    b = fr[pl.ds(SUB * k, SUB), pl.ds(t0, SUB), :] * (1.0 / 65536.0)
                else:
                    b = rhs[pl.ds(z0, SUB), pl.ds(y0, SUB), :]
                r = (b + (s - dd * c)).reshape(4, 2, SUB, LN)
                tr[pl.ds(4 * k, 4), pl.ds(t0, SUB), :] = r[:, 0] + r[:, 1]
            loop(lev.n // SUB, zblk)
        loop(lev.n // SUB, ytile)

    def pair_rows(zc, j):
        s = tr[zc, pl.ds(16 * j, SUB, stride=2), :] + tr[zc, pl.ds(16 * j + 1, SUB, stride=2), :]
        return s + pltpu.roll(s, 127, 1)

    def restrict_to(fine, coarse, dst, pack):
        half = fine.n // 2
        own = (lane >= coarse.ox) & (lane < coarse.ox + half)
        idx = jnp.clip(fine.ox + 2 * (lane - coarse.ox), 0, 127)
        face = jnp.where(px == 0, coarse.ox + half - SUB, coarse.ox)
        group = lane // SUB

        def ytile(j):
            y0 = pl.multiple_of(coarse.oy + SUB * j, SUB)

            def zgrp(q):
                pk = jnp.zeros((SUB, LN), F32)
                for i in range(min(16, half)):
                    zc = 16 * q + i
                    s = jnp.take_along_axis(pair_rows(zc, j), idx, axis=1)
                    s = jnp.where(own, 0.5 * s, 0.0)
                    dst[coarse.oz + zc, pl.ds(y0, SUB), :] = s
                    if pack is not None:
                        pk = jnp.where(group == i, pltpu.roll(s, lax.rem(SUB * i + LN - face, LN), 1), pk)
                if pack is not None:
                    pack[q, pl.ds(pl.multiple_of(SUB * j, SUB), SUB), :] = pk
            loop(max(1, half // 16), zgrp)
        loop(half // SUB, ytile)

    def restrict_packed(fine, me):
        idx = fine.ox + 2 * (lane % 16)
        group = lane // 16
        for j in range(2):
            def zgrp(q):
                pk = jnp.zeros((SUB, LN), F32)
                for i in range(SUB):
                    s = jnp.take_along_axis(pair_rows(SUB * q + i, j), idx, axis=1)
                    pk = jnp.where(group == i, 0.5 * s, pk)
                g3[me, q, pl.ds(SUB * j, SUB), :] = pk
            loop(2, zgrp)

    def prolong_add(fine, coarse, esrc, dst, cbase, pack_par=None):
        back_z = (fine.oz - fine.zs) // 2
        back_y = (fine.oy - fine.ys) // 2
        wide = 0 if fine.nyt * SUB == fine.n else 1
        nct = fine.n // 16 + wide
        cy_s = cbase[1] - 2 * back_y
        fy_s = fine.oy - 4 * back_y
        cz_s = cbase[0] - back_z - 1
        ncz = 4 * fine.nzb + 2
        xf = lane - fine.ox
        half = lax.shift_right_arithmetic(xf, 1)
        odd = xf - 2 * half
        i0 = half + cbase[2]
        i1 = i0 + 2 * odd - 1
        inx = (lane >= fine.lo[2]) & (lane < fine.hi[2])
        edge = (lane == fine.lo[2]) | (lane == fine.hi[2] - 1)
        wx = jnp.where(inx, jnp.where(edge, 0.5, 0.75), 0.0)
        wn = jnp.where(inx, 0.25, 0.0)
        i0 = jnp.clip(i0, 0, 127)
        i1 = jnp.clip(i1, 0, 127)

        def spread(v):
            return wx * jnp.take_along_axis(v, i0, axis=1) + wn * jnp.take_along_axis(v, i1, axis=1)

        def ctile(t):
            cy = pl.multiple_of(cy_s + SUB * t, SUB)
            fy = pl.multiple_of(fy_s + 16 * t, SUB)
            r = row + cy
            iny = (r >= coarse.lo[1]) & (r < coarse.hi[1])
            wny = jnp.where(iny, 0.25, 0.0)
            wde = jnp.where(iny, jnp.where(r == coarse.lo[1], 0.5, 0.75), 0.0)
            wdo = jnp.where(iny, jnp.where(r == coarse.hi[1] - 1, 0.5, 0.75), 0.0)

            def plane(i):
                for q in range(2):
                    z = 2 * i + q
                    e = esrc[cz_s + z, pl.ds(cy, SUB), :]
                    dn = esrc[cz_s + z, pl.ds(cy - 1, SUB), :]
                    up = esrc[cz_s + z, pl.ds(cy + 1, SUB), :]
                    tr[z, pl.ds(fy, SUB, stride=2), :] = spread(wde * e + wny * dn)
                    tr[z, pl.ds(fy + 1, SUB, stride=2), :] = spread(wdo * e + wny * up)
            loop(ncz // 2, plane)
        loop(nct, ctile)

        def ytile(t):
            y0 = pl.multiple_of(fine.ys + SUB * t, SUB)

            def zblk(k, pk):
                z0 = fine.zs + SUB * k
                tb = tr[pl.ds(4 * k, 6), pl.ds(y0, SUB), :]
                mid = 0.75 * tb[1:5]
                add = jnp.stack([mid + 0.25 * tb[0:4], mid + 0.25 * tb[2:6]], axis=1).reshape(SUB, SUB, LN)
                new = dst[pl.ds(z0, SUB), pl.ds(y0, SUB), :] + add
                dst[pl.ds(z0, SUB), pl.ds(y0, SUB), :] = new
                return pk if pack_par is None else pack_block(new, SUB * k, pk)

            pk = lax.fori_loop(0, fine.nzb, zblk, jnp.zeros((SUB, LN), F32))
            if pack_par is not None:
                xs[pack_par, pl.ds(pl.multiple_of(SUB * t, SUB), SUB), :] = pk
            zghost_tile(fine, dst, y0)
        loop(fine.nyt, ytile)

    zface = jnp.where(pz == 0, LN, 1)
    zdst = jnp.where(pz == 0, 0, 129)
    yface = jnp.where(py == 0, 135, SUB)
    yghost = jnp.where(py == 0, 136, 7)

    def exchange0(buf, par):
        cx = remote(xs.at[par], xg.at[par], par, 1)
        cx.start()
        cz = remote(buf.at[zface, pl.ds(SUB, LN), :], buf.at[zdst, pl.ds(SUB, LN), :], 2 + par, 4)
        cz.start()

        def take_rows(i):
            for j in range(SUB):
                yp[par, pl.ds(SUB * i + j, 1), :] = buf[SUB * i + j + 1, pl.ds(yface, 1), :]
        loop(16, take_rows)
        cy = remote(yp.at[par], yg.at[par], 4 + par, 2)
        cy.start()
        cy.wait()

        def put_rows(i):
            for j in range(SUB):
                buf[SUB * i + j + 1, pl.ds(yghost, 1), :] = yg[par, pl.ds(SUB * i + j, 1), :]
        loop(16, put_rows)
        cx.wait()
        cz.wait()

    def exchange_wide(lev, ref, sendp, recvp, k):
        n, h = lev.n, HALO_PLANES[lev.idx]
        cx = remote(sendp, recvp, k, 1)
        cx.start()
        cx.wait()
        halo = jnp.where(px == 0, lev.ox + n, lev.ox - SUB)
        inh = (lane >= halo) & (lane < halo + SUB)

        def ytile(t):
            y0 = pl.multiple_of(lev.oy + SUB * t, SUB)

            def zgrp(q):
                pk = recvp[q, pl.ds(pl.multiple_of(SUB * t, SUB), SUB), :]
                for i in range(16):
                    z = lev.oz + 16 * q + i
                    moved = pltpu.roll(pk, lax.rem(halo + LN - SUB * i, LN), 1)
                    ref[z, pl.ds(y0, SUB), :] = jnp.where(inh, moved, ref[z, pl.ds(y0, SUB), :])
            loop(n // 16, zgrp)
        loop(n // SUB, ytile)
        fy = pl.multiple_of(jnp.where(py == 0, lev.oy + n - SUB, lev.oy), SUB)
        hy = pl.multiple_of(jnp.where(py == 0, lev.oy - SUB, lev.oy + n), SUB)
        fz = jnp.where(pz == 0, lev.oz + n - h, lev.oz)
        hz = jnp.where(pz == 0, lev.oz - h, lev.oz + n)
        copies = [
            remote(ref.at[pl.ds(lev.oz, n), pl.ds(fy, SUB), :], ref.at[pl.ds(lev.oz, n), pl.ds(hy, SUB), :], k + 1, 2),
            remote(ref.at[pl.ds(fz, h), pl.ds(lev.oy, n), :], ref.at[pl.ds(hz, h), pl.ds(lev.oy, n), :], k + 2, 4),
            remote(ref.at[pl.ds(fz, h), pl.ds(fy, SUB), :], ref.at[pl.ds(hz, h), pl.ds(hy, SUB), :], k + 3, 6),
        ]
        for c in copies:
            c.start()
        for c in copies:
            c.wait()
        zghost(lev, ref)

    me = 4 * pz + 2 * py + px

    def gather3():
        copies = [remote(g3.at[me], g3.at[me], 14 + code, code) for code in range(1, SUB)]
        for c in copies:
            c.start()
        for c in copies:
            c.wait()
        lev = levels[3]

        def ytile(t):
            y0 = pl.multiple_of(lev.oy + SUB * t, SUB)
            by = t // 2
            r0 = pl.multiple_of(SUB * (t % 2), SUB)

            def zgrp(q):
                bz = q // 2
                total = None
                lo = g3[4 * bz + 2 * by, q % 2, pl.ds(r0, SUB), :]
                hi = g3[4 * bz + 2 * by + 1, q % 2, pl.ds(r0, SUB), :]
                for i in range(SUB):
                    a = pltpu.roll(lo, (lev.ox - 16 * i) % LN, 1)
                    b = pltpu.roll(hi, (lev.ox + 16 - 16 * i) % LN, 1)
                    v = jnp.where((lane >= lev.ox) & (lane < lev.ox + 16), a,
                                  jnp.where((lane >= lev.ox + 16) & (lane < lev.ox + 32), b, 0.0))
                    b3[lev.oz + SUB * q + i, pl.ds(y0, SUB), :] = v
            loop(4, zgrp)
        loop(4, ytile)
        zghost(lev, b3)

    def coarse_solve():
        lev = levels[5]

        def zstep(z, acc):
            b = b5[lev.oz + z, pl.ds(lev.oy, SUB), :] * 64.0
            acc = list(acc)
            for x in range(SUB):
                col = jnp.broadcast_to(b[:, lev.ox + x:lev.ox + x + 1], (SUB, LN))
                for j in range(4):
                    acc[j] = acc[j] + cinv[j, pl.ds(z * 64 + x, SUB, stride=SUB), :] * col
            return tuple(acc)
        acc = lax.fori_loop(0, SUB, zstep, (jnp.zeros((SUB, LN), F32),) * 4)
        lines = [jnp.broadcast_to(jnp.sum(a, axis=0, keepdims=True), (SUB, LN)) for a in acc]
        own = (lane >= lev.ox) & (lane < lev.ox + SUB)
        for z in range(SUB):
            idx = jnp.clip((z % 2) * 64 + row * SUB + lane - lev.ox, 0, 127)
            e5[lev.oz + z, pl.ds(lev.oy, SUB), :] = jnp.where(own, jnp.take_along_axis(lines[z // 2], idx, axis=1), 0.0)
        zghost(lev, e5)

    def base_of(lev):
        return (lev.oz, lev.oy, lev.ox)

    def local_visit(fine, va, vb, rhs, descend, ecoarse, coarse, cbase):
        sweep(fine, rhs, va, None)
        zghost(fine, va)
        residual_pass(fine, va, rhs)
        descend()
        prolong_add(fine, coarse, ecoarse, va, cbase)
        sweep(fine, va, vb, rhs)
        sweep(fine, vb, va, rhs)

    def descend4():
        restrict_to(levels[4], levels[5], b5, None)
        coarse_solve()

    def descend3():
        restrict_to(levels[3], levels[4], b4, None)
        zghost(levels[4], b4)
        local_visit(levels[4], v4a, v4b, b4, descend4, e5, levels[5], base_of(levels[5]))

    def descend2():
        restrict_packed(levels[2], me)
        gather3()
        local_visit(levels[3], v3a, v3b, b3, descend3, v4a, levels[4], base_of(levels[4]))

    def descend1():
        restrict_to(levels[1], levels[2], b2, p2s)
        exchange_wide(levels[2], b2, p2s, p2r, 10)
        oz, oy, ox = base_of(levels[3])
        local_visit(levels[2], v2a, v2b, b2, descend2, v3a, levels[3], (oz + 16 * pz, oy + 16 * py, ox + 16 * px))

    def pack_initial(t):
        y0 = pl.multiple_of(SUB + SUB * t, SUB)
        pk = lax.fori_loop(0, 16, lambda k, pk: pack_block(ua[pl.ds(1 + SUB * k, SUB), pl.ds(y0, SUB), :], SUB * k, pk),
                           jnp.zeros((SUB, LN), F32))
        xs[0, pl.ds(pl.multiple_of(SUB * t, SUB), SUB), :] = pk
        zghost_tile(lev0, ua, y0)

    load_u.wait()
    loop(16, pack_initial)
    load_f.wait()
    for copy in load_c:
        copy.wait()

    def cycle(_):
        exchange0(ua, 0)
        sweep(lev0, ua, ub, fr, 0)
        exchange0(ub, 1)
        sweep(lev0, ub, ua, fr, 1)
        exchange0(ua, 0)
        residual_pass(lev0, ua, fr, 0)
        restrict_to(lev0, levels[1], b1, p1s)
        exchange_wide(levels[1], b1, p1s, p1r, 6)
        local_visit(levels[1], v1a, v1b, b1, descend1, v2a, levels[2], base_of(levels[2]))
        prolong_add(lev0, levels[1], v1a, ua, base_of(levels[1]), 0)
        exchange0(ua, 0)
        sweep(lev0, ua, ub, fr, 0)
        exchange0(ub, 1)
        sweep(lev0, ub, ua, fr, 1)

    loop(CYCLES, cycle)

    store = pltpu.make_async_copy(ua.at[pl.ds(1, LN), pl.ds(SUB, LN), :], out_hbm, lsem.at[0])
    store.start()
    store.wait()


def solution(mesh):
    grid_spec = P(('batch', 'gz'), 'gy', 'gx')

    def vmem(*shape):
        return pltpu.VMEM(shape, F32)

    scratch = [vmem(130, 144, LN), vmem(130, 144, LN), vmem(LN, LN, LN), vmem(66, 144, LN)]
    for shape in ((82, 96), (50, 64), (34, 72), (18, 48)):
        scratch += [vmem(*shape, LN)] * 3
    scratch += [vmem(10, 32, LN), vmem(10, 32, LN), vmem(4, 512, LN)]
    scratch += [vmem(2, LN, LN)] * 4
    scratch += [vmem(4, 64, LN)] * 2 + [vmem(2, 32, LN)] * 2 + [vmem(SUB, 2, 16, LN)]
    scratch += [pltpu.SemaphoreType.DMA((22,)), pltpu.SemaphoreType.DMA((22,)), pltpu.SemaphoreType.DMA((6,))]

    call = pl.pallas_call(
        solve_kernel,
        out_shape=jax.ShapeDtypeStruct((LN, LN, LN), F32),
        in_specs=[pl.BlockSpec(memory_space=pl.ANY)] * 3,
        out_specs=pl.BlockSpec(memory_space=pl.ANY),
        scratch_shapes=scratch,
        name='multigrid',
        compiler_params=pltpu.CompilerParams(collective_id=0, has_side_effects=True, vmem_limit_bytes=67043328),
    )
    return jax.shard_map(call, mesh=mesh, in_specs=(grid_spec, grid_spec, P()), out_specs=grid_spec, check_vma=False)
```

```python
import jax
import jax.numpy as jnp
from jax import lax
from jax.experimental import pallas as pl
from jax.experimental.pallas import tpu as pltpu
from jax.sharding import PartitionSpec as P

OMEGA = 2.0 / 3.0
C6 = OMEGA / 6.0
CYCLES = 2
MESH = pl.DeviceIdType.MESH
F32 = jnp.float32
SUB, GRP, LN = 8, 16, 128
HALO_PLANES = {1: 4, 2: 5}
BACK = LN - 1
INV_G2 = 1.0 / 65536.0


class Level:
    def __init__(self, idx, n, off, shape, pos, split):
        self.idx, self.n, self.shape = idx, n, shape
        self.oz, self.oy, self.ox = off
        self.split = split
        if split:
            self.lo = tuple(o - p * n for o, p in zip(off, pos))
            self.hi = tuple(l + 2 * n for l in self.lo)
        else:
            self.lo = off
            self.hi = tuple(o + n for o in off)
        wide = SUB if (split and idx > 0) else 0
        self.zs = self.oz - wide * pos[0] if wide else self.oz
        self.ys = self.oy - wide * pos[1] if wide else self.oy
        self.nzb = (n + wide) // SUB
        self.nyt = (n + wide) // SUB
        if split:
            self.ghosts = [(jnp.where(pos[0] == 0, self.oz - 1, self.oz + n), jnp.where(pos[0] == 0, self.oz, self.oz + n - 1))]
        else:
            self.ghosts = [(self.oz - 1, self.oz), (self.oz + n, self.oz + n - 1)]


def solve_kernel(f_hbm, u_hbm, c_hbm, out_hbm,
                 ua, ub, fr, tr, xr, sx, v1, b1, v2, b2, v3, b3, v4, b4, e5, b5, cinv,
                 xs, xg, yp, yg, p1s, p1r, p2s, p2r, g3, ssem, rsem, lsem):
    pz, py, px = lax.axis_index('gz'), lax.axis_index('gy'), lax.axis_index('gx')
    pos = (pz, py, px)
    lane = lax.broadcasted_iota(jnp.int32, (SUB, LN), 1)
    row = lax.broadcasted_iota(jnp.int32, (SUB, LN), 0)
    nil = jnp.zeros((SUB, LN), F32)
    levels = [
        Level(0, LN, (1, SUB, 0), (130, 144), pos, True),
        Level(1, 64, (9, GRP, 32), (82, 96), pos, True),
        Level(2, 32, (9, GRP, 48), (50, 64), pos, True),
        Level(3, 32, (1, GRP, 48), (34, 72), pos, False),
        Level(4, GRP, (1, GRP, 48), (18, 48), pos, False),
        Level(5, SUB, (1, GRP, 48), (10, 32), pos, False),
    ]
    lev0 = levels[0]
    low_x = px == 0
    face_lane = jnp.where(low_x, (lane + 1) & BACK, lane)
    out_lane = jnp.where(low_x, lane, (lane + 1) & BACK)

    def dev(code):
        ids = {}
        if code & 4:
            ids['gz'] = 1 - pz
        if code & 2:
            ids['gy'] = 1 - py
        if code & 1:
            ids['gx'] = 1 - px
        return ids

    def remote(src, dst, k, code):
        return pltpu.make_async_remote_copy(src_ref=src, dst_ref=dst, send_sem=ssem.at[k], recv_sem=rsem.at[k],
                                            device_id=dev(code), device_id_type=MESH)

    def loop(n, body):
        lax.fori_loop(0, n, lambda i, c: (body(i), c)[1], 0)

    def tile(i):
        return pl.multiple_of(SUB * i, SUB)

    def load(t):
        rows = pl.ds(tile(t), SUB)
        return (pltpu.make_async_copy(u_hbm.at[:, rows, :], ua.at[pl.ds(1, LN), pl.ds(tile(t + 1), SUB), :], lsem.at[t]),
                pltpu.make_async_copy(f_hbm.at[:, rows, :], fr.at[:, rows, :], lsem.at[GRP + t]))

    def start_load(t):
        for copy in load(t):
            copy.start()
    loop(GRP, start_load)
    load_c = [pltpu.make_async_copy(c_hbm.at[:, pl.ds(LN * j, LN)], cinv.at[j], lsem.at[32 + j]) for j in range(4)]
    for copy in load_c:
        copy.start()

    def zero(ref):
        def body(i):
            ref[i] = jnp.zeros(ref.shape[1:], F32)
        loop(ref.shape[0], body)

    for ref in (v1.at[0], v1.at[1], b1, v2.at[0], v2.at[1], b2, v3.at[0], v3.at[1], b3, v4.at[0], v4.at[1], b4, e5):
        zero(ref)

    def zero_rows(i):
        for buf in (ua, ub):
            buf[i, pl.ds(0, SUB), :] = nil
            buf[i, pl.ds(136, SUB), :] = nil
    loop(130, zero_rows)
    zout = jnp.where(pz == 0, 0, 129)

    def zero_plane(t):
        for buf in (ua, ub):
            buf[zout, pl.ds(tile(t), SUB), :] = nil
    loop(18, zero_plane)

    barrier = pltpu.get_barrier_semaphore()
    for code in range(1, SUB):
        pl.semaphore_signal(barrier, inc=1, device_id=dev(code), device_id_type=MESH)
    pl.semaphore_wait(barrier, 7)

    def coefs(lev, y0):
        r = row + y0
        inside = (r >= lev.lo[1]) & (r < lev.hi[1]) & (lane >= lev.lo[2]) & (lane < lev.hi[2])
        one = jnp.ones((SUB, LN), F32)
        nb = (jnp.where(r == lev.lo[1], one, nil) + jnp.where(r == lev.hi[1] - 1, one, nil)
              + jnp.where(lane == lev.lo[2], one, nil) + jnp.where(lane == lev.hi[2] - 1, one, nil))
        return inside, nb

    def zghost_tile(lev, ref, y0):
        for ghost, face in lev.ghosts:
            ref[ghost, pl.ds(y0, SUB), :] = -ref[face, pl.ds(y0, SUB), :]

    def zghost(lev, ref):
        loop(lev.shape[1] // SUB, lambda t: zghost_tile(lev, ref, tile(t)))

    def blocks(count, per, body):
        def step(i):
            for k in range(per):
                body(i * per + k)
        loop(count // per, step)

    def roll_sums(src, zs, nzb, y0):
        for z in range(SUB * nzb):
            c = src[zs + z, pl.ds(y0, SUB), :]
            sx[z] = pltpu.roll(c, 1, 1) + pltpu.roll(c, BACK, 1)

    def stencil(src, zs, k, y0):
        z0 = zs + SUB * k
        v = src[pl.ds(z0 - 1, SUB + 2), pl.ds(y0, SUB), :]
        s = v[0:SUB] + v[2:SUB + 2]
        s = s + src[pl.ds(z0, SUB), pl.ds(y0 - 1, SUB), :] + src[pl.ds(z0, SUB), pl.ds(y0 + 1, SUB), :]
        return v[1:SUB + 1], s + sx[pl.ds(SUB * k, SUB)]

    def sweep(lev, src, dst, rhs):
        first = rhs is None

        def ytile(t):
            y0 = pl.multiple_of(lev.ys + SUB * t, SUB)
            inside, nb = coefs(lev, y0)
            cc = (1.0 - OMEGA) - C6 * nb
            if first:
                ca, cb = jnp.where(inside, C6 * (cc + 1.0), 0.0), jnp.where(inside, C6 * C6, 0.0)
            else:
                ca, cb = jnp.where(inside, cc, 0.0), jnp.where(inside, C6, 0.0)
            roll_sums(src, lev.zs, lev.nzb, y0)

            def block(k):
                c, s = stencil(src, lev.zs, k, y0)
                z0 = lev.zs + SUB * k
                if not first:
                    s = s + rhs[pl.ds(z0, SUB), pl.ds(y0, SUB), :]
                dst[pl.ds(z0, SUB), pl.ds(y0, SUB), :] = ca * c + cb * s
            blocks(lev.nzb, 3 if lev.nzb == 9 else 2 if lev.nzb == 4 else 1, block)
            zghost_tile(lev, dst, y0)
        loop(lev.nyt, ytile)

    def residual_pass(lev, src, rhs):
        def ytile(t):
            y0 = pl.multiple_of(lev.oy + SUB * t, SUB)
            _, nb = coefs(lev, y0)
            dd = 6.0 + nb
            roll_sums(src, lev.oz, lev.n // SUB, y0)

            def block(k):
                c, s = stencil(src, lev.oz, k, y0)
                r = (rhs[pl.ds(lev.oz + SUB * k, SUB), pl.ds(y0, SUB), :] + (s - dd * c)).reshape(4, 2, SUB, LN)
                tr[pl.ds(4 * k, 4), pl.ds(tile(t), SUB), :] = r[:, 0] + r[:, 1]
            blocks(lev.n // SUB, max(1, lev.n // GRP // 2), block)
        loop(lev.n // SUB, ytile)

    def roll_sums0(src, par, t):
        rows = pl.ds(tile(t + 1), SUB)
        ghost = xg[par, pl.ds(tile(t), SUB), :]
        left = jnp.where(low_x, 0.0, ghost)
        right = jnp.where(low_x, ghost, 0.0)
        zlow = jnp.where(pz == 0, 1.0, 0.0)
        below, here = src[0, rows, :], src[1, rows, :]
        for z in range(LN):
            above = src[z + 2, rows, :]
            a = jnp.where(lane == (z - 1) % LN, left, here) + below
            b = jnp.where(lane == z, right, here) + above
            s = pltpu.roll(a, 1, 1) + pltpu.roll(b, BACK, 1) - jnp.where(out_lane == z, here, 0.0)
            if z == 0:
                s = s - zlow * here
            if z == LN - 1:
                s = s - (1.0 - zlow) * here
            sx[z] = s
            below, here = here, above

    def cells0(src, t, z):
        y0, planes = tile(t + 1), pl.ds(z + 1, GRP)
        s = sx[pl.ds(z, GRP)] + src[planes, pl.ds(y0 - 1, SUB), :] + src[planes, pl.ds(y0 + 1, SUB), :]
        return src[planes, pl.ds(y0, SUB), :], s + fr[pl.ds(z, GRP), pl.ds(tile(t), SUB), :]

    def yedge(t):
        r = row + tile(t + 1)
        return jnp.where((r == lev0.lo[1]) | (r == lev0.hi[1] - 1), 1.0, 0.0)

    def sweep0(src, dst, par):
        def ytile(t):
            roll_sums0(src, par, t)
            cc = (1.0 - OMEGA) - C6 * yedge(t)

            def block(k, pk):
                c, s = cells0(src, t, GRP * k)
                new = cc * c + C6 * s
                dst[pl.ds(GRP * k + 1, GRP), pl.ds(tile(t + 1), SUB), :] = new
                for j in range(GRP):
                    pk = jnp.where(face_lane == GRP * k + j, new[j], pk)
                return pk
            xs[1 - par, pl.ds(tile(t), SUB), :] = lax.fori_loop(0, SUB, block, nil)
        loop(GRP, ytile)

    def residual0():
        def ytile(t):
            roll_sums0(ua, 0, t)
            dd = 6.0 + yedge(t)

            def block(k):
                c, s = cells0(ua, t, GRP * k)
                ub[pl.ds(GRP * k + 1, GRP), pl.ds(tile(t + 1), SUB), :] = s - dd * c
            loop(SUB, block)
        loop(GRP, ytile)

    def pair_sums(fine, j):
        for zc in range(fine.n // 2):
            lo, hi = pl.ds(GRP * j, SUB, stride=2), pl.ds(GRP * j + 1, SUB, stride=2)
            if fine.idx:
                s = tr[zc, lo, :] + tr[zc, hi, :]
                sx[zc] = 0.5 * (s + pltpu.roll(s, BACK, 1))
                continue
            lo, hi = pl.ds(GRP * j + SUB, SUB, stride=2), pl.ds(GRP * j + SUB + 1, SUB, stride=2)
            e = ub[2 * zc + 1, lo, :] + ub[2 * zc + 1, hi, :]
            o = ub[2 * zc + 2, lo, :] + ub[2 * zc + 2, hi, :]
            s = pltpu.roll(e, -2 * zc % LN, 1) + pltpu.roll(e + o, (-2 * zc - 1) % LN, 1)
            sx[zc] = 0.5 * (s + pltpu.roll(o, (-2 * zc - 2) % LN, 1))

    def restrict_to(fine, coarse, dst, pack):
        half = fine.n // 2
        own = (lane >= coarse.ox) & (lane < coarse.ox + half)
        idx = (fine.ox + 2 * (lane - coarse.ox)) & BACK
        pidx = fine.ox + 2 * (jnp.where(low_x, half - SUB, 0) + lane % SUB)
        group = lane // SUB
        step = min(GRP, half // 2)

        def ytile(j):
            rows = pl.ds(pl.multiple_of(coarse.oy + SUB * j, SUB), SUB)
            pair_sums(fine, j)

            def move(q):
                for i in range(step):
                    z = step * q + i
                    dst[coarse.oz + z, rows, :] = jnp.where(own, jnp.take_along_axis(sx[z], idx, axis=1), 0.0)
            loop(half // step, move)

            def collect(q):
                pk = nil
                for i in range(GRP):
                    pk = jnp.where(group == i, jnp.take_along_axis(sx[GRP * q + i], pidx, axis=1), pk)
                pack[q, pl.ds(tile(j), SUB), :] = pk
            if pack is not None:
                loop(half // GRP, collect)
        loop(half // SUB, ytile)

    def restrict_packed(fine, me):
        idx = fine.ox + 2 * (lane % GRP)
        group = lane // GRP

        def ytile(j):
            pair_sums(fine, j)

            def collect(q):
                pk = nil
                for i in range(SUB):
                    pk = jnp.where(group == i, jnp.take_along_axis(sx[SUB * q + i], idx, axis=1), pk)
                g3[me, q, pl.ds(tile(j), SUB), :] = pk
            loop(2, collect)
        loop(2, ytile)

    def prolong_add(fine, coarse, esrc, dst, cbase):
        back_z = (fine.oz - fine.zs) // 2
        back_y = (fine.oy - fine.ys) // 2
        nct = fine.n // GRP + (0 if fine.nyt * SUB == fine.n else 1)
        cy_s = cbase[1] - 2 * back_y
        fy_s = fine.oy - 4 * back_y
        cz_s = cbase[0] - back_z - 1
        ncz = 4 * fine.nzb + 2
        xf = lane - fine.ox
        half = lax.shift_right_arithmetic(xf, 1)
        odd = xf - 2 * half
        i0 = half + cbase[2]
        i1 = jnp.clip(i0 + 2 * odd - 1, 0, BACK)
        i0 = jnp.clip(i0, 0, BACK)
        inx = (lane >= fine.lo[2]) & (lane < fine.hi[2])
        edge = (lane == fine.lo[2]) | (lane == fine.hi[2] - 1)
        wx = jnp.where(inx, jnp.where(edge, 0.5, 0.75), 0.0)
        wn = jnp.where(inx, 0.25, 0.0)

        def spread(z):
            for t in range(nct + 2):
                v = esrc[cz_s + z, pl.ds(pl.multiple_of(cy_s + SUB * (t - 1), SUB), SUB), :]
                xr[z, pl.ds(SUB * t, SUB), :] = (wx * jnp.take_along_axis(v, i0, axis=1)
                                                 + wn * jnp.take_along_axis(v, i1, axis=1))

        def spread_two(z):
            spread(2 * z)
            spread(2 * z + 1)
        loop(ncz // 2, spread_two)

        def ctile(t):
            fy = pl.multiple_of(fy_s + GRP * t, SUB)
            r = row + (cy_s + SUB * t)
            iny = (r >= coarse.lo[1]) & (r < coarse.hi[1])
            wny = jnp.where(iny, 0.25, 0.0)
            wde = jnp.where(iny, jnp.where(r == coarse.lo[1], 0.5, 0.75), 0.0)
            wdo = jnp.where(iny, jnp.where(r == coarse.hi[1] - 1, 0.5, 0.75), 0.0)

            def plane(i):
                for q in range(2):
                    z = 2 * i + q
                    e = xr[z, pl.ds(tile(t + 1), SUB), :]
                    tr[z, pl.ds(fy, SUB, stride=2), :] = wde * e + wny * xr[z, pl.ds(tile(t + 1) - 1, SUB), :]
                    tr[z, pl.ds(fy + 1, SUB, stride=2), :] = wdo * e + wny * xr[z, pl.ds(tile(t + 1) + 1, SUB), :]
            loop(ncz // 2, plane)
        loop(nct, ctile)

        def ytile(t):
            y0 = pl.multiple_of(fine.ys + SUB * t, SUB)
            rows = pl.ds(y0, SUB)
            pk = nil
            for k in range(fine.nzb):
                z0 = fine.zs + SUB * k
                tb = tr[pl.ds(4 * k, 6), rows, :]
                mid = 0.75 * tb[1:5]
                add = jnp.stack([mid + 0.25 * tb[0:4], mid + 0.25 * tb[2:6]], axis=1).reshape(SUB, SUB, LN)
                if fine.idx:
                    dst[pl.ds(z0, SUB), rows, :] = dst[pl.ds(z0, SUB), rows, :] + add
                    continue
                for j in range(SUB):
                    z = SUB * k + j
                    new = dst[1 + z, rows, :] + pltpu.roll(add[j], z, 1)
                    dst[1 + z, rows, :] = new
                    pk = jnp.where(face_lane == z, new, pk)
            if fine.idx:
                zghost_tile(fine, dst, y0)
            else:
                xs[0, pl.ds(tile(t), SUB), :] = pk
        loop(fine.nyt, ytile)

    zface = jnp.where(pz == 0, LN, 1)
    zdst = LN + 1 - zface + jnp.where(pz == 0, -1, 1)
    yface = jnp.where(py == 0, 135, SUB)
    yghost = jnp.where(py == 0, 136, 7)

    def exchange0(buf, par):
        cx = remote(xs.at[par], xg.at[par], par, 1)
        cx.start()
        cz = remote(buf.at[zface, pl.ds(SUB, LN), :], buf.at[zdst, pl.ds(SUB, LN), :], 2 + par, 4)
        cz.start()

        def take_rows(i):
            for j in range(SUB):
                yp[par, pl.ds(SUB * i + j, 1), :] = buf[SUB * i + j + 1, pl.ds(yface, 1), :]
        loop(GRP, take_rows)
        cy = remote(yp.at[par], yg.at[par], 4 + par, 2)
        cy.start()
        cy.wait()

        def put_rows(i):
            for j in range(SUB):
                buf[SUB * i + j + 1, pl.ds(yghost, 1), :] = yg[par, pl.ds(SUB * i + j, 1), :]
        loop(GRP, put_rows)
        cx.wait()
        cz.wait()

    def exchange_wide(lev, ref, sendp, recvp, k):
        n, h = lev.n, HALO_PLANES[lev.idx]
        cx = remote(sendp, recvp, k, 1)
        cx.start()
        cx.wait()
        halo = jnp.where(low_x, lev.ox + n, lev.ox - SUB)
        inh = (lane >= halo) & (lane < halo + SUB)

        def ytile(t):
            rows = pl.ds(pl.multiple_of(lev.oy + SUB * t, SUB), SUB)
            for q in range(n // GRP):
                pk = recvp[q, pl.ds(tile(t), SUB), :]
                pk = pltpu.roll(pk, halo, 1)
                for i in range(GRP):
                    z = lev.oz + GRP * q + i
                    ref[z, rows, :] = jnp.where(inh, pltpu.roll(pk, (-SUB * i) % LN, 1), ref[z, rows, :])
        loop(n // SUB, ytile)
        fy = pl.multiple_of(jnp.where(py == 0, lev.oy + n - SUB, lev.oy), SUB)
        hy = pl.multiple_of(jnp.where(py == 0, lev.oy - SUB, lev.oy + n), SUB)
        fz = jnp.where(pz == 0, lev.oz + n - h, lev.oz)
        hz = jnp.where(pz == 0, lev.oz - h, lev.oz + n)
        copies = [
            remote(ref.at[pl.ds(lev.oz, n), pl.ds(fy, SUB), :], ref.at[pl.ds(lev.oz, n), pl.ds(hy, SUB), :], k + 1, 2),
            remote(ref.at[pl.ds(fz, h), pl.ds(lev.oy, n), :], ref.at[pl.ds(hz, h), pl.ds(lev.oy, n), :], k + 2, 4),
            remote(ref.at[pl.ds(fz, h), pl.ds(fy, SUB), :], ref.at[pl.ds(hz, h), pl.ds(hy, SUB), :], k + 3, 6),
        ]
        for c in copies:
            c.start()
        for c in copies:
            c.wait()
        zghost(lev, ref)

    me = 4 * pz + 2 * py + px

    def gather3():
        copies = [remote(g3.at[me], g3.at[me], 14 + code, code) for code in range(1, SUB)]
        for c in copies:
            c.start()
        for c in copies:
            c.wait()
        lev = levels[3]
        in_lo = (lane >= lev.ox) & (lane < lev.ox + GRP)
        in_hi = (lane >= lev.ox + GRP) & (lane < lev.ox + 32)

        def ytile(t):
            rows = pl.ds(pl.multiple_of(lev.oy + SUB * t, SUB), SUB)
            by = t // 2
            r0 = pl.ds(tile(t % 2), SUB)
            for q in range(4):
                lo = g3[4 * (q // 2) + 2 * by, q % 2, r0, :]
                hi = g3[4 * (q // 2) + 2 * by + 1, q % 2, r0, :]
                for i in range(SUB):
                    a = pltpu.roll(lo, (lev.ox - GRP * i) % LN, 1)
                    b = pltpu.roll(hi, (lev.ox + GRP - GRP * i) % LN, 1)
                    b3[lev.oz + SUB * q + i, rows, :] = jnp.where(in_lo, a, jnp.where(in_hi, b, 0.0))
        loop(4, ytile)
        zghost(lev, b3)

    def coarse_solve():
        lev = levels[5]

        def zstep(z, acc):
            b = b5[lev.oz + z, pl.ds(lev.oy, SUB), :] * 64.0
            acc = list(acc)
            for x in range(SUB):
                col = jnp.broadcast_to(b[:, lev.ox + x:lev.ox + x + 1], (SUB, LN))
                for j in range(4):
                    acc[j] = acc[j] + cinv[j, pl.ds(z * 64 + x, SUB, stride=SUB), :] * col
            return tuple(acc)
        acc = lax.fori_loop(0, SUB, zstep, (jnp.zeros((SUB, LN), F32),) * 4)
        lines = [jnp.broadcast_to(jnp.sum(a, axis=0, keepdims=True), (SUB, LN)) for a in acc]
        own = (lane >= lev.ox) & (lane < lev.ox + SUB)
        for z in range(SUB):
            idx = jnp.clip((z % 2) * 64 + row * SUB + lane - lev.ox, 0, 127)
            e5[lev.oz + z, pl.ds(lev.oy, SUB), :] = jnp.where(own, jnp.take_along_axis(lines[z // 2], idx, axis=1), 0.0)
        zghost(lev, e5)

    def base_of(lev):
        return (lev.oz, lev.oy, lev.ox)

    def local_visit(fine, v, rhs, descend, ecoarse, coarse, cbase):
        sweep(fine, rhs, v.at[0], None)
        zghost(fine, v.at[0])
        residual_pass(fine, v.at[0], rhs)
        descend()
        prolong_add(fine, coarse, ecoarse, v.at[0], cbase)
        loop(2, lambda i: sweep(fine, v.at[i], v.at[1 - i], rhs))

    def descend4():
        restrict_to(levels[4], levels[5], b5, None)
        coarse_solve()

    def descend3():
        restrict_to(levels[3], levels[4], b4, None)
        zghost(levels[4], b4)
        local_visit(levels[4], v4, b4, descend4, e5, levels[5], base_of(levels[5]))

    def descend2():
        restrict_packed(levels[2], me)
        gather3()
        local_visit(levels[3], v3, b3, descend3, v4.at[0], levels[4], base_of(levels[4]))

    def descend1():
        restrict_to(levels[1], levels[2], b2, p2s)
        exchange_wide(levels[2], b2, p2s, p2r, 10)
        oz, oy, ox = base_of(levels[3])
        local_visit(levels[2], v2, b2, descend2, v3.at[0], levels[3], (oz + GRP * pz, oy + GRP * py, ox + GRP * px))

    def skew_in(t):
        for copy in load(t):
            copy.wait()
        rows, frows = pl.ds(tile(t + 1), SUB), pl.ds(tile(t), SUB)
        pk = nil
        for z in range(LN):
            moved = pltpu.roll(ua[z + 1, rows, :], z, 1)
            ua[z + 1, rows, :] = moved
            pk = jnp.where(face_lane == z, moved, pk)
            fr[z, frows, :] = pltpu.roll(fr[z, frows, :] * INV_G2, z, 1)
        xs[0, frows, :] = pk
    loop(GRP, skew_in)
    for copy in load_c:
        copy.wait()

    def correct():
        exchange0(ua, 0)
        residual0()
        restrict_to(lev0, levels[1], b1, p1s)
        exchange_wide(levels[1], b1, p1s, p1r, 6)
        local_visit(levels[1], v1, b1, descend1, v2.at[0], levels[2], base_of(levels[2]))
        prolong_add(lev0, levels[1], v1.at[0], ua, base_of(levels[1]))

    def half_cycle(h):
        exchange0(ua, 0)
        sweep0(ua, ub, 0)
        exchange0(ub, 1)
        sweep0(ub, ua, 1)
        pl.when(h % 2 == 0)(correct)
    loop(2 * CYCLES, half_cycle)

    def store(t):
        return pltpu.make_async_copy(ub.at[pl.ds(1, LN), pl.ds(tile(t + 1), SUB), :], out_hbm.at[:, pl.ds(tile(t), SUB), :],
                                     lsem.at[t])

    def skew_out(t):
        rows = pl.ds(tile(t + 1), SUB)
        for z in range(LN):
            ub[z + 1, rows, :] = pltpu.roll(ua[z + 1, rows, :], -z % LN, 1)
        store(t).start()
    loop(GRP, skew_out)
    loop(GRP, lambda t: store(t).wait())


def solution(mesh):
    grid_spec = P(('batch', 'gz'), 'gy', 'gx')

    def vmem(*shape):
        return pltpu.VMEM(shape, F32)

    scratch = [vmem(130, 144, LN), vmem(130, 144, LN), vmem(LN, LN, LN), vmem(66, 144, LN), vmem(66, 80, LN), vmem(LN, SUB, LN)]
    for shape in ((82, 96), (50, 64), (34, 72), (18, 48)):
        scratch += [vmem(2, *shape, LN), vmem(*shape, LN)]
    scratch += [vmem(10, 32, LN), vmem(10, 32, LN), vmem(4, 512, LN)]
    scratch += [vmem(2, LN, LN)] * 4
    scratch += [vmem(4, 64, LN)] * 2 + [vmem(2, 32, LN)] * 2 + [vmem(SUB, 2, GRP, LN)]
    scratch += [pltpu.SemaphoreType.DMA((22,)), pltpu.SemaphoreType.DMA((22,)), pltpu.SemaphoreType.DMA((36,))]

    call = pl.pallas_call(
        solve_kernel,
        out_shape=jax.ShapeDtypeStruct((LN, LN, LN), F32),
        in_specs=[pl.BlockSpec(memory_space=pl.ANY)] * 3,
        out_specs=pl.BlockSpec(memory_space=pl.ANY),
        scratch_shapes=scratch,
        name='multigrid',
        compiler_params=pltpu.CompilerParams(collective_id=0, has_side_effects=True, vmem_limit_bytes=67043328),
    )
    return jax.shard_map(call, mesh=mesh, in_specs=(grid_spec, grid_spec, P()), out_specs=grid_spec, check_vma=False)
```

```python
import jax
import jax.numpy as jnp
from jax import lax
from jax.experimental import pallas as pl
from jax.experimental.pallas import tpu as pltpu
from jax.sharding import PartitionSpec as P

OMEGA = 2.0 / 3.0
C6 = OMEGA / 6.0
CYCLES = 2
MESH = pl.DeviceIdType.MESH
F32 = jnp.float32
SUB, GRP, LN = 8, 16, 128
HALO_PLANES = {1: 4, 2: 5}
BACK = LN - 1
INV_G2 = 1.0 / 65536.0


class Level:
    def __init__(self, idx, n, off, shape, pos, split):
        self.idx, self.n, self.shape = idx, n, shape
        self.oz, self.oy, self.ox = off
        self.split = split
        if split:
            self.lo = tuple(o - p * n for o, p in zip(off, pos))
            self.hi = tuple(l + 2 * n for l in self.lo)
        else:
            self.lo = off
            self.hi = tuple(o + n for o in off)
        wide = SUB if (split and idx > 0) else 0
        self.zs = self.oz - wide * pos[0] if wide else self.oz
        self.ys = self.oy - wide * pos[1] if wide else self.oy
        self.nzb = (n + wide) // SUB
        self.nyt = (n + wide) // SUB
        if split:
            self.ghosts = [(jnp.where(pos[0] == 0, self.oz - 1, self.oz + n), jnp.where(pos[0] == 0, self.oz, self.oz + n - 1))]
        else:
            self.ghosts = [(self.oz - 1, self.oz), (self.oz + n, self.oz + n - 1)]


def solve_kernel(f_hbm, u_hbm, c_hbm, out_hbm,
                 ua, ub, fr, tr, xr, sx, sy, v1, b1, v2, b2, v3, b3, v4, b4, e5, b5, cinv,
                 xs, xg, yp, yg, p1s, p1r, p2s, p2r, g3, ssem, rsem, xss, xrs, zss, zrs, lsem):
    pz, py, px = lax.axis_index('gz'), lax.axis_index('gy'), lax.axis_index('gx')
    pos = (pz, py, px)
    lane = lax.broadcasted_iota(jnp.int32, (SUB, LN), 1)
    row = lax.broadcasted_iota(jnp.int32, (SUB, LN), 0)
    nil = jnp.zeros((SUB, LN), F32)
    levels = [
        Level(0, LN, (1, SUB, 0), (130, 144), pos, True),
        Level(1, 64, (9, GRP, 32), (82, 96), pos, True),
        Level(2, 32, (9, GRP, 48), (50, 64), pos, True),
        Level(3, 32, (1, GRP, 48), (34, 72), pos, False),
        Level(4, GRP, (1, GRP, 48), (18, 48), pos, False),
        Level(5, SUB, (1, GRP, 48), (10, 32), pos, False),
    ]
    lev0 = levels[0]
    low_x = px == 0
    face_lane = jnp.where(low_x, (lane + 1) & BACK, lane)
    out_lane = jnp.where(low_x, lane, (lane + 1) & BACK)

    def dev(code):
        ids = {}
        if code & 4:
            ids['gz'] = 1 - pz
        if code & 2:
            ids['gy'] = 1 - py
        if code & 1:
            ids['gx'] = 1 - px
        return ids

    def remote(src, dst, k, code):
        return pltpu.make_async_remote_copy(src_ref=src, dst_ref=dst, send_sem=ssem.at[k], recv_sem=rsem.at[k],
                                            device_id=dev(code), device_id_type=MESH)

    def loop(n, body):
        lax.fori_loop(0, n, lambda i, c: (body(i), c)[1], 0)

    def tile(i):
        return pl.multiple_of(SUB * i, SUB)

    def load(t):
        rows = pl.ds(tile(t), SUB)
        return (pltpu.make_async_copy(u_hbm.at[:, rows, :], ua.at[pl.ds(1, LN), pl.ds(tile(t + 1), SUB), :], lsem.at[t]),
                pltpu.make_async_copy(f_hbm.at[:, rows, :], fr.at[:, rows, :], lsem.at[GRP + t]))

    def start_load(t):
        for copy in load(t):
            copy.start()
    loop(GRP, lambda t: start_load(jnp.where(py == 0, 15 - t, t)))
    load_c = [pltpu.make_async_copy(c_hbm.at[:, pl.ds(LN * j, LN)], cinv.at[j], lsem.at[32 + j]) for j in range(4)]
    for copy in load_c:
        copy.start()

    def zero(ref):
        def body(i):
            ref[i] = jnp.zeros(ref.shape[1:], F32)
        loop(ref.shape[0], body)

    for ref in (v1.at[0], v1.at[1], b1, v2.at[0], v2.at[1], b2, v3.at[0], v3.at[1], b3, v4.at[0], v4.at[1], b4, e5):
        zero(ref)

    def zero_rows(i):
        for buf in (ua, ub):
            buf[i, pl.ds(0, SUB), :] = nil
            buf[i, pl.ds(136, SUB), :] = nil
    loop(130, zero_rows)
    zout = jnp.where(pz == 0, 0, 129)

    def zero_plane(t):
        for buf in (ua, ub):
            buf[zout, pl.ds(tile(t), SUB), :] = nil
    loop(18, zero_plane)

    barrier = pltpu.get_barrier_semaphore()
    for code in range(1, SUB):
        pl.semaphore_signal(barrier, inc=1, device_id=dev(code), device_id_type=MESH)
    pl.semaphore_wait(barrier, 7)

    def coefs(lev, y0):
        r = row + y0
        inside = (r >= lev.lo[1]) & (r < lev.hi[1]) & (lane >= lev.lo[2]) & (lane < lev.hi[2])
        one = jnp.ones((SUB, LN), F32)
        nb = (jnp.where(r == lev.lo[1], one, nil) + jnp.where(r == lev.hi[1] - 1, one, nil)
              + jnp.where(lane == lev.lo[2], one, nil) + jnp.where(lane == lev.hi[2] - 1, one, nil))
        return inside, nb

    def zghost_tile(lev, ref, y0):
        for ghost, face in lev.ghosts:
            ref[ghost, pl.ds(y0, SUB), :] = -ref[face, pl.ds(y0, SUB), :]

    def zghost(lev, ref):
        loop(lev.shape[1] // SUB, lambda t: zghost_tile(lev, ref, tile(t)))

    def blocks(count, per, body):
        def step(i):
            for k in range(per):
                body(i * per + k)
        loop(count // per, step)

    def roll_sums(src, zs, nzb, y0):
        for z in range(SUB * nzb):
            c = src[zs + z, pl.ds(y0, SUB), :]
            sx[z] = pltpu.roll(c, 1, 1) + pltpu.roll(c, BACK, 1)

    def stencil(src, zs, k, y0):
        z0 = zs + SUB * k
        v = src[pl.ds(z0 - 1, SUB + 2), pl.ds(y0, SUB), :]
        s = v[0:SUB] + v[2:SUB + 2]
        s = s + src[pl.ds(z0, SUB), pl.ds(y0 - 1, SUB), :] + src[pl.ds(z0, SUB), pl.ds(y0 + 1, SUB), :]
        return v[1:SUB + 1], s + sx[pl.ds(SUB * k, SUB)]

    def sweep(lev, src, dst, rhs):
        first = rhs is None

        def ytile(t):
            y0 = pl.multiple_of(lev.ys + SUB * t, SUB)
            inside, nb = coefs(lev, y0)
            cc = (1.0 - OMEGA) - C6 * nb
            if first:
                ca, cb = jnp.where(inside, C6 * (cc + 1.0), 0.0), jnp.where(inside, C6 * C6, 0.0)
            else:
                ca, cb = jnp.where(inside, cc, 0.0), jnp.where(inside, C6, 0.0)
            roll_sums(src, lev.zs, lev.nzb, y0)

            def block(k):
                c, s = stencil(src, lev.zs, k, y0)
                z0 = lev.zs + SUB * k
                if not first:
                    s = s + rhs[pl.ds(z0, SUB), pl.ds(y0, SUB), :]
                dst[pl.ds(z0, SUB), pl.ds(y0, SUB), :] = ca * c + cb * s
            blocks(lev.nzb, 3 if lev.nzb == 9 else 2 if lev.nzb == 4 else 1, block)
            zghost_tile(lev, dst, y0)
        loop(lev.nyt, ytile)

    def residual_pass(lev, src, rhs):
        def ytile(t):
            y0 = pl.multiple_of(lev.oy + SUB * t, SUB)
            _, nb = coefs(lev, y0)
            dd = 6.0 + nb
            roll_sums(src, lev.oz, lev.n // SUB, y0)

            def block(k):
                c, s = stencil(src, lev.oz, k, y0)
                r = (rhs[pl.ds(lev.oz + SUB * k, SUB), pl.ds(y0, SUB), :] + (s - dd * c)).reshape(4, 2, SUB, LN)
                tr[pl.ds(4 * k, 4), pl.ds(tile(t), SUB), :] = r[:, 0] + r[:, 1]
            blocks(lev.n // SUB, max(1, lev.n // GRP // 2), block)
        loop(lev.n // SUB, ytile)

    zface = jnp.where(pz == 0, LN, 1)
    zdst = LN + 1 - zface + jnp.where(pz == 0, -1, 1)
    yface = jnp.where(py == 0, 135, SUB)
    yghost = jnp.where(py == 0, 136, 7)

    def order(t):
        return jnp.where(py == 0, 15 - t, t)

    def pieces(buf, par, o):
        rows, yrows = pl.ds(tile(o), SUB), pl.ds(tile(o + 1), SUB)
        return (pltpu.make_async_remote_copy(src_ref=xs.at[par, rows, :], dst_ref=xg.at[par, rows, :], send_sem=xss.at[par, o],
                                             recv_sem=xrs.at[par, o], device_id=dev(1), device_id_type=MESH),
                pltpu.make_async_remote_copy(src_ref=buf.at[zface, yrows, :], dst_ref=buf.at[zdst, yrows, :],
                                             send_sem=zss.at[par, o], recv_sem=zrs.at[par, o], device_id=dev(4),
                                             device_id_type=MESH))

    def face_rows(par):
        return remote(yp.at[par], yg.at[par], par, 2)

    def send(buf, par, t):
        for copy in pieces(buf, par, order(t)):
            copy.start()

        def first():
            def take_rows(i):
                for j in range(SUB):
                    yp[par, pl.ds(SUB * i + j, 1), :] = buf[SUB * i + j + 1, pl.ds(yface, 1), :]
            loop(GRP, take_rows)
            face_rows(par).start()
        pl.when(t == 0)(first)

    def receive(buf, par, t):
        def first():
            face_rows(par).wait()

            def put_rows(i):
                for j in range(SUB):
                    buf[SUB * i + j + 1, pl.ds(yghost, 1), :] = yg[par, pl.ds(SUB * i + j, 1), :]
            loop(GRP, put_rows)
        pl.when(t == 0)(first)
        for copy in pieces(buf, par, order(t)):
            copy.wait()

    def roll_sums0(src, par, t, sx):
        rows = pl.ds(tile(t + 1), SUB)
        ghost = xg[par, pl.ds(tile(t), SUB), :]
        left = jnp.where(low_x, 0.0, ghost)
        right = jnp.where(low_x, ghost, 0.0)
        zlow = jnp.where(pz == 0, 1.0, 0.0)
        below, here = src[0, rows, :], src[1, rows, :]
        for z in range(LN):
            above = src[z + 2, rows, :]
            a = jnp.where(lane == (z - 1) % LN, left, here) + below
            b = jnp.where(lane == z, right, here) + above
            s = pltpu.roll(a, 1, 1) + pltpu.roll(b, BACK, 1) - jnp.where(out_lane == z, here, 0.0)
            if z == 0:
                s = s - zlow * here
            if z == LN - 1:
                s = s - (1.0 - zlow) * here
            sx[z] = s
            below, here = here, above

    def cells0(src, t, z, sx):
        y0, planes = tile(t + 1), pl.ds(z + 1, GRP)
        s = sx[pl.ds(z, GRP)] + src[planes, pl.ds(y0 - 1, SUB), :] + src[planes, pl.ds(y0 + 1, SUB), :]
        return src[planes, pl.ds(y0, SUB), :], s + fr[pl.ds(z, GRP), pl.ds(tile(t), SUB), :]

    def yedge(t):
        r = row + tile(t + 1)
        return jnp.where((r == lev0.lo[1]) | (r == lev0.hi[1] - 1), 1.0, 0.0)

    def sweep0(src, dst, par):
        def ytile(t):
            receive(src, par, t)
            o = order(t)
            roll_sums0(src, par, o, sx)
            cc = (1.0 - OMEGA) - C6 * yedge(o)

            def block(k, pk):
                c, s = cells0(src, o, GRP * k, sx)
                new = cc * c + C6 * s
                dst[pl.ds(GRP * k + 1, GRP), pl.ds(tile(o + 1), SUB), :] = new
                for j in range(GRP):
                    pk = jnp.where(face_lane == GRP * k + j, new[j], pk)
                return pk
            xs[1 - par, pl.ds(tile(o), SUB), :] = lax.fori_loop(0, SUB, block, nil)
            send(dst, 1 - par, t)
        loop(GRP, ytile)

    def residual0():
        def ytile(t):
            receive(ua, 0, t)
            o = order(t)
            roll_sums0(ua, 0, o, sx)
            dd = 6.0 + yedge(o)

            def block(k):
                c, s = cells0(ua, o, GRP * k, sx)
                ub[pl.ds(GRP * k + 1, GRP), pl.ds(tile(o + 1), SUB), :] = s - dd * c
            loop(SUB, block)
        loop(GRP, ytile)

    def pair_sums(fine, j):
        for zc in range(fine.n // 2):
            lo, hi = pl.ds(GRP * j, SUB, stride=2), pl.ds(GRP * j + 1, SUB, stride=2)
            if fine.idx:
                s = tr[zc, lo, :] + tr[zc, hi, :]
                sx[zc] = 0.5 * (s + pltpu.roll(s, BACK, 1))
                continue
            lo, hi = pl.ds(GRP * j + SUB, SUB, stride=2), pl.ds(GRP * j + SUB + 1, SUB, stride=2)
            e = ub[2 * zc + 1, lo, :] + ub[2 * zc + 1, hi, :]
            o = ub[2 * zc + 2, lo, :] + ub[2 * zc + 2, hi, :]
            s = pltpu.roll(e, -2 * zc % LN, 1) + pltpu.roll(e + o, (-2 * zc - 1) % LN, 1)
            sx[zc] = 0.5 * (s + pltpu.roll(o, (-2 * zc - 2) % LN, 1))

    def restrict_to(fine, coarse, dst, pack):
        half = fine.n // 2
        own = (lane >= coarse.ox) & (lane < coarse.ox + half)
        idx = (fine.ox + 2 * (lane - coarse.ox)) & BACK
        pidx = fine.ox + 2 * (jnp.where(low_x, half - SUB, 0) + lane % SUB)
        group = lane // SUB
        step = min(GRP, half // 2)

        def ytile(j):
            rows = pl.ds(pl.multiple_of(coarse.oy + SUB * j, SUB), SUB)
            pair_sums(fine, j)

            def move(q):
                for i in range(step):
                    z = step * q + i
                    dst[coarse.oz + z, rows, :] = jnp.where(own, jnp.take_along_axis(sx[z], idx, axis=1), 0.0)
            loop(half // step, move)

            def collect(q):
                pk = nil
                for i in range(GRP):
                    pk = jnp.where(group == i, jnp.take_along_axis(sx[GRP * q + i], pidx, axis=1), pk)
                pack[q, pl.ds(tile(j), SUB), :] = pk
            if pack is not None:
                loop(half // GRP, collect)
        loop(half // SUB, ytile)

    def restrict_packed(fine, me):
        idx = fine.ox + 2 * (lane % GRP)
        group = lane // GRP

        def ytile(j):
            pair_sums(fine, j)

            def collect(q):
                pk = nil
                for i in range(SUB):
                    pk = jnp.where(group == i, jnp.take_along_axis(sx[SUB * q + i], idx, axis=1), pk)
                g3[me, q, pl.ds(tile(j), SUB), :] = pk
            loop(2, collect)
        loop(2, ytile)

    def prolong_add(fine, coarse, esrc, dst, cbase):
        back_z = (fine.oz - fine.zs) // 2
        back_y = (fine.oy - fine.ys) // 2
        nct = fine.n // GRP + (0 if fine.nyt * SUB == fine.n else 1)
        cy_s = cbase[1] - 2 * back_y
        fy_s = fine.oy - 4 * back_y
        cz_s = cbase[0] - back_z - 1
        ncz = 4 * fine.nzb + 2
        xf = lane - fine.ox
        half = lax.shift_right_arithmetic(xf, 1)
        odd = xf - 2 * half
        i0 = half + cbase[2]
        i1 = jnp.clip(i0 + 2 * odd - 1, 0, BACK)
        i0 = jnp.clip(i0, 0, BACK)
        inx = (lane >= fine.lo[2]) & (lane < fine.hi[2])
        edge = (lane == fine.lo[2]) | (lane == fine.hi[2] - 1)
        wx = jnp.where(inx, jnp.where(edge, 0.5, 0.75), 0.0)
        wn = jnp.where(inx, 0.25, 0.0)

        def spread(z):
            for t in range(nct + 2):
                v = esrc[cz_s + z, pl.ds(pl.multiple_of(cy_s + SUB * (t - 1), SUB), SUB), :]
                xr[z, pl.ds(SUB * t, SUB), :] = (wx * jnp.take_along_axis(v, i0, axis=1)
                                                 + wn * jnp.take_along_axis(v, i1, axis=1))

        per = 6 if ncz % 6 == 0 else 2

        def spread_some(i):
            for q in range(per):
                spread(per * i + q)
        loop(ncz // per, spread_some)

        def ctile(t):
            fy = pl.multiple_of(fy_s + GRP * t, SUB)
            r = row + (cy_s + SUB * t)
            iny = (r >= coarse.lo[1]) & (r < coarse.hi[1])
            wny = jnp.where(iny, 0.25, 0.0)
            wde = jnp.where(iny, jnp.where(r == coarse.lo[1], 0.5, 0.75), 0.0)
            wdo = jnp.where(iny, jnp.where(r == coarse.hi[1] - 1, 0.5, 0.75), 0.0)

            def plane(i):
                for q in range(per):
                    z = per * i + q
                    e = xr[z, pl.ds(tile(t + 1), SUB), :]
                    tr[z, pl.ds(fy, SUB, stride=2), :] = wde * e + wny * xr[z, pl.ds(tile(t + 1) - 1, SUB), :]
                    tr[z, pl.ds(fy + 1, SUB, stride=2), :] = wdo * e + wny * xr[z, pl.ds(tile(t + 1) + 1, SUB), :]
            loop(ncz // per, plane)
        loop(nct, ctile)

        def ytile(t):
            o = t if fine.idx else order(t)
            y0 = pl.multiple_of(fine.ys + SUB * o, SUB)
            rows = pl.ds(y0, SUB)
            pk = nil
            for k in range(fine.nzb):
                z0 = fine.zs + SUB * k
                tb = tr[pl.ds(4 * k, 6), rows, :]
                mid = 0.75 * tb[1:5]
                add = jnp.stack([mid + 0.25 * tb[0:4], mid + 0.25 * tb[2:6]], axis=1).reshape(SUB, SUB, LN)
                if fine.idx:
                    dst[pl.ds(z0, SUB), rows, :] = dst[pl.ds(z0, SUB), rows, :] + add
                    continue
                for j in range(SUB):
                    z = SUB * k + j
                    new = dst[1 + z, rows, :] + pltpu.roll(add[j], z, 1)
                    dst[1 + z, rows, :] = new
                    pk = jnp.where(face_lane == z, new, pk)
            if fine.idx:
                zghost_tile(fine, dst, y0)
            else:
                xs[0, pl.ds(tile(o), SUB), :] = pk
                send(dst, 0, t)
        loop(fine.nyt, ytile)

    def exchange_wide(lev, ref, sendp, recvp, k):
        n, h = lev.n, HALO_PLANES[lev.idx]
        cx = remote(sendp, recvp, k, 1)
        cx.start()
        cx.wait()
        halo = jnp.where(low_x, lev.ox + n, lev.ox - SUB)
        inh = (lane >= halo) & (lane < halo + SUB)

        def ytile(t):
            rows = pl.ds(pl.multiple_of(lev.oy + SUB * t, SUB), SUB)
            for q in range(n // GRP):
                pk = recvp[q, pl.ds(tile(t), SUB), :]
                pk = pltpu.roll(pk, halo, 1)
                for i in range(GRP):
                    z = lev.oz + GRP * q + i
                    ref[z, rows, :] = jnp.where(inh, pltpu.roll(pk, (-SUB * i) % LN, 1), ref[z, rows, :])
        loop(n // SUB, ytile)
        fy = pl.multiple_of(jnp.where(py == 0, lev.oy + n - SUB, lev.oy), SUB)
        hy = pl.multiple_of(jnp.where(py == 0, lev.oy - SUB, lev.oy + n), SUB)
        fz = jnp.where(pz == 0, lev.oz + n - h, lev.oz)
        hz = jnp.where(pz == 0, lev.oz - h, lev.oz + n)
        copies = [
            remote(ref.at[pl.ds(lev.oz, n), pl.ds(fy, SUB), :], ref.at[pl.ds(lev.oz, n), pl.ds(hy, SUB), :], k + 1, 2),
            remote(ref.at[pl.ds(fz, h), pl.ds(lev.oy, n), :], ref.at[pl.ds(hz, h), pl.ds(lev.oy, n), :], k + 2, 4),
            remote(ref.at[pl.ds(fz, h), pl.ds(fy, SUB), :], ref.at[pl.ds(hz, h), pl.ds(hy, SUB), :], k + 3, 6),
        ]
        for c in copies:
            c.start()
        for c in copies:
            c.wait()
        zghost(lev, ref)

    me = 4 * pz + 2 * py + px

    def gather3():
        copies = [remote(g3.at[me], g3.at[me], 14 + code, code) for code in range(1, SUB)]
        for c in copies:
            c.start()
        for c in copies:
            c.wait()
        lev = levels[3]
        in_lo = (lane >= lev.ox) & (lane < lev.ox + GRP)
        in_hi = (lane >= lev.ox + GRP) & (lane < lev.ox + 32)

        def ytile(t):
            rows = pl.ds(pl.multiple_of(lev.oy + SUB * t, SUB), SUB)
            by = t // 2
            r0 = pl.ds(tile(t % 2), SUB)
            for q in range(4):
                lo = g3[4 * (q // 2) + 2 * by, q % 2, r0, :]
                hi = g3[4 * (q // 2) + 2 * by + 1, q % 2, r0, :]
                for i in range(SUB):
                    a = pltpu.roll(lo, (lev.ox - GRP * i) % LN, 1)
                    b = pltpu.roll(hi, (lev.ox + GRP - GRP * i) % LN, 1)
                    b3[lev.oz + SUB * q + i, rows, :] = jnp.where(in_lo, a, jnp.where(in_hi, b, 0.0))
        loop(4, ytile)
        zghost(lev, b3)

    def coarse_solve():
        lev = levels[5]

        def zstep(z, acc):
            b = b5[lev.oz + z, pl.ds(lev.oy, SUB), :] * 64.0
            acc = list(acc)
            for x in range(SUB):
                col = jnp.broadcast_to(b[:, lev.ox + x:lev.ox + x + 1], (SUB, LN))
                for j in range(4):
                    acc[j] = acc[j] + cinv[j, pl.ds(z * 64 + x, SUB, stride=SUB), :] * col
            return tuple(acc)
        acc = lax.fori_loop(0, SUB, zstep, (jnp.zeros((SUB, LN), F32),) * 4)
        lines = [jnp.broadcast_to(jnp.sum(a, axis=0, keepdims=True), (SUB, LN)) for a in acc]
        own = (lane >= lev.ox) & (lane < lev.ox + SUB)
        for z in range(SUB):
            idx = jnp.clip((z % 2) * 64 + row * SUB + lane - lev.ox, 0, 127)
            e5[lev.oz + z, pl.ds(lev.oy, SUB), :] = jnp.where(own, jnp.take_along_axis(lines[z // 2], idx, axis=1), 0.0)
        zghost(lev, e5)

    def base_of(lev):
        return (lev.oz, lev.oy, lev.ox)

    def local_visit(fine, v, rhs, descend, ecoarse, coarse, cbase):
        sweep(fine, rhs, v.at[0], None)
        zghost(fine, v.at[0])
        residual_pass(fine, v.at[0], rhs)
        descend()
        prolong_add(fine, coarse, ecoarse, v.at[0], cbase)
        loop(2, lambda i: sweep(fine, v.at[i], v.at[1 - i], rhs))

    def descend4():
        restrict_to(levels[4], levels[5], b5, None)
        coarse_solve()

    def descend3():
        restrict_to(levels[3], levels[4], b4, None)
        zghost(levels[4], b4)
        local_visit(levels[4], v4, b4, descend4, e5, levels[5], base_of(levels[5]))

    def descend2():
        restrict_packed(levels[2], me)
        gather3()
        local_visit(levels[3], v3, b3, descend3, v4.at[0], levels[4], base_of(levels[4]))

    def descend1():
        restrict_to(levels[1], levels[2], b2, p2s)
        exchange_wide(levels[2], b2, p2s, p2r, 10)
        oz, oy, ox = base_of(levels[3])
        local_visit(levels[2], v2, b2, descend2, v3.at[0], levels[3], (oz + GRP * pz, oy + GRP * py, ox + GRP * px))

    def skew_in(t):
        o = order(t)
        for copy in load(o):
            copy.wait()
        rows, frows = pl.ds(tile(o + 1), SUB), pl.ds(tile(o), SUB)
        pk = nil
        for z in range(LN):
            moved = pltpu.roll(ua[z + 1, rows, :], z, 1)
            ua[z + 1, rows, :] = moved
            pk = jnp.where(face_lane == z, moved, pk)
            fr[z, frows, :] = pltpu.roll(fr[z, frows, :] * INV_G2, z, 1)
        xs[0, frows, :] = pk
        send(ua, 0, t)
    loop(GRP, skew_in)
    for copy in load_c:
        copy.wait()

    def correct():
        residual0()
        restrict_to(lev0, levels[1], b1, p1s)
        exchange_wide(levels[1], b1, p1s, p1r, 6)
        local_visit(levels[1], v1, b1, descend1, v2.at[0], levels[2], base_of(levels[2]))
        prolong_add(lev0, levels[1], v1.at[0], ua, base_of(levels[1]))

    def half_cycle(h):
        sweep0(ua, ub, 0)
        sweep0(ub, ua, 1)
        pl.when(h % 2 == 0)(correct)
    loop(2 * CYCLES, half_cycle)
    loop(GRP, lambda t: receive(ua, 0, t))

    def store(t):
        return pltpu.make_async_copy(ub.at[pl.ds(1, LN), pl.ds(tile(t + 1), SUB), :], out_hbm.at[:, pl.ds(tile(t), SUB), :],
                                     lsem.at[t])

    def skew_out(t):
        rows = pl.ds(tile(t + 1), SUB)
        for z in range(LN):
            ub[z + 1, rows, :] = pltpu.roll(ua[z + 1, rows, :], -z % LN, 1)
        store(t).start()
    loop(GRP, skew_out)
    loop(GRP, lambda t: store(t).wait())


def solution(mesh):
    grid_spec = P(('batch', 'gz'), 'gy', 'gx')

    def vmem(*shape):
        return pltpu.VMEM(shape, F32)

    scratch = [vmem(130, 144, LN), vmem(130, 144, LN), vmem(LN, LN, LN), vmem(66, 144, LN), vmem(66, 80, LN), vmem(LN, SUB, LN), vmem(LN, SUB, LN)]
    for shape in ((82, 96), (50, 64), (34, 72), (18, 48)):
        scratch += [vmem(2, *shape, LN), vmem(*shape, LN)]
    scratch += [vmem(10, 32, LN), vmem(10, 32, LN), vmem(4, 512, LN)]
    scratch += [vmem(2, LN, LN)] * 4
    scratch += [vmem(4, 64, LN)] * 2 + [vmem(2, 32, LN)] * 2 + [vmem(SUB, 2, GRP, LN)]
    scratch += [pltpu.SemaphoreType.DMA((22,)), pltpu.SemaphoreType.DMA((22,))]
    scratch += [pltpu.SemaphoreType.DMA((2, GRP))] * 4 + [pltpu.SemaphoreType.DMA((36,))]

    call = pl.pallas_call(
        solve_kernel,
        out_shape=jax.ShapeDtypeStruct((LN, LN, LN), F32),
        in_specs=[pl.BlockSpec(memory_space=pl.ANY)] * 3,
        out_specs=pl.BlockSpec(memory_space=pl.ANY),
        scratch_shapes=scratch,
        name='multigrid',
        compiler_params=pltpu.CompilerParams(collective_id=0, has_side_effects=True, vmem_limit_bytes=67043328),
    )
    return jax.shard_map(call, mesh=mesh, in_specs=(grid_spec, grid_spec, P()), out_specs=grid_spec, check_vma=False)
```

```python
import jax
import jax.numpy as jnp
from jax import lax
from jax.experimental import pallas as pl
from jax.experimental.pallas import tpu as pltpu
from jax.sharding import PartitionSpec as P

OMEGA = 2.0 / 3.0
C6 = OMEGA / 6.0
CYCLES = 2
MESH = pl.DeviceIdType.MESH
F32 = jnp.float32
SUB, GRP, LN = 8, 16, 128
HALO_PLANES = {1: 4, 2: 5}
BACK = LN - 1
INV_G2 = 1.0 / 65536.0


class Level:
    def __init__(self, idx, n, off, shape, pos, split):
        self.idx, self.n, self.shape = idx, n, shape
        self.oz, self.oy, self.ox = off
        self.split = split
        if split:
            self.lo = tuple(o - p * n for o, p in zip(off, pos))
            self.hi = tuple(l + 2 * n for l in self.lo)
        else:
            self.lo = off
            self.hi = tuple(o + n for o in off)
        wide = SUB if (split and idx > 0) else 0
        self.zs = self.oz - wide * pos[0] if wide else self.oz
        self.ys = self.oy - wide * pos[1] if wide else self.oy
        self.nzb = (n + wide) // SUB
        self.nyt = (n + wide) // SUB
        if split:
            self.ghosts = [(jnp.where(pos[0] == 0, self.oz - 1, self.oz + n), jnp.where(pos[0] == 0, self.oz, self.oz + n - 1))]
        else:
            self.ghosts = [(self.oz - 1, self.oz), (self.oz + n, self.oz + n - 1)]


def solve_kernel(f_hbm, u_hbm, c_hbm, out_hbm,
                 ua, ub, fr, tr, xr, sx, sy, v1, b1, v2, b2, v3, b3, v4, b4, e5, b5, cinv,
                 xs, xg, yp, yg, p1s, p1r, p2s, p2r, g3, ssem, rsem, xss, xrs, zss, zrs, lsem):
    pz, py, px = lax.axis_index('gz'), lax.axis_index('gy'), lax.axis_index('gx')
    pos = (pz, py, px)
    lane = lax.broadcasted_iota(jnp.int32, (SUB, LN), 1)
    row = lax.broadcasted_iota(jnp.int32, (SUB, LN), 0)
    nil = jnp.zeros((SUB, LN), F32)
    levels = [
        Level(0, LN, (1, SUB, 0), (130, 144), pos, True),
        Level(1, 64, (9, GRP, 32), (82, 96), pos, True),
        Level(2, 32, (9, GRP, 48), (50, 64), pos, True),
        Level(3, 32, (1, GRP, 48), (34, 72), pos, False),
        Level(4, GRP, (1, GRP, 48), (18, 48), pos, False),
        Level(5, SUB, (1, GRP, 48), (10, 32), pos, False),
    ]
    lev0 = levels[0]
    low_x = px == 0
    face_lane = jnp.where(low_x, (lane + 1) & BACK, lane)
    out_lane = jnp.where(low_x, lane, (lane + 1) & BACK)

    skew = (lax.broadcasted_iota(jnp.int32, (SUB, SUB, LN), 2) - lax.broadcasted_iota(jnp.int32, (SUB, SUB, LN), 0)) & BACK
    out_skew = jnp.where(low_x, skew, (skew + 1) & BACK)

    def dev(code):
        ids = {}
        if code & 4:
            ids['gz'] = 1 - pz
        if code & 2:
            ids['gy'] = 1 - py
        if code & 1:
            ids['gx'] = 1 - px
        return ids

    def remote(src, dst, k, code):
        return pltpu.make_async_remote_copy(src_ref=src, dst_ref=dst, send_sem=ssem.at[k], recv_sem=rsem.at[k],
                                            device_id=dev(code), device_id_type=MESH)

    def loop(n, body):
        lax.fori_loop(0, n, lambda i, c: (body(i), c)[1], 0)

    def tile(i):
        return pl.multiple_of(SUB * i, SUB)

    def load(t):
        rows = pl.ds(tile(t), SUB)
        return (pltpu.make_async_copy(u_hbm.at[:, rows, :], ua.at[pl.ds(1, LN), pl.ds(tile(t + 1), SUB), :], lsem.at[t]),
                pltpu.make_async_copy(f_hbm.at[:, rows, :], fr.at[:, rows, :], lsem.at[GRP + t]))

    def start_load(t):
        for copy in load(t):
            copy.start()
    loop(GRP, lambda t: start_load(jnp.where(py == 0, 15 - t, t)))
    load_c = [pltpu.make_async_copy(c_hbm.at[:, pl.ds(LN * j, LN)], cinv.at[j], lsem.at[32 + j]) for j in range(4)]
    for copy in load_c:
        copy.start()

    def zero(ref):
        def body(i):
            ref[i] = jnp.zeros(ref.shape[1:], F32)
        loop(ref.shape[0], body)

    for ref in (v1.at[0], v1.at[1], b1, v2.at[0], v2.at[1], b2, v3.at[0], v3.at[1], b3, v4.at[0], v4.at[1], b4, e5):
        zero(ref)

    def zero_rows(i):
        for buf in (ua, ub):
            buf[i, pl.ds(0, SUB), :] = nil
            buf[i, pl.ds(136, SUB), :] = nil
    loop(130, zero_rows)
    zout = jnp.where(pz == 0, 0, 129)

    def zero_plane(t):
        for buf in (ua, ub):
            buf[zout, pl.ds(tile(t), SUB), :] = nil
    loop(18, zero_plane)

    barrier = pltpu.get_barrier_semaphore()
    for code in range(1, SUB):
        pl.semaphore_signal(barrier, inc=1, device_id=dev(code), device_id_type=MESH)
    pl.semaphore_wait(barrier, 7)

    def coefs(lev, y0):
        r = row + y0
        inside = (r >= lev.lo[1]) & (r < lev.hi[1]) & (lane >= lev.lo[2]) & (lane < lev.hi[2])
        one = jnp.ones((SUB, LN), F32)
        nb = (jnp.where(r == lev.lo[1], one, nil) + jnp.where(r == lev.hi[1] - 1, one, nil)
              + jnp.where(lane == lev.lo[2], one, nil) + jnp.where(lane == lev.hi[2] - 1, one, nil))
        return inside, nb

    def zghost_tile(lev, ref, y0):
        for ghost, face in lev.ghosts:
            ref[ghost, pl.ds(y0, SUB), :] = -ref[face, pl.ds(y0, SUB), :]

    def zghost(lev, ref):
        loop(lev.shape[1] // SUB, lambda t: zghost_tile(lev, ref, tile(t)))

    def blocks(count, per, body):
        def step(i):
            for k in range(per):
                body(i * per + k)
        loop(count // per, step)

    def roll_sums(src, zs, nzb, y0):
        for z in range(SUB * nzb):
            c = src[zs + z, pl.ds(y0, SUB), :]
            sx[z] = pltpu.roll(c, 1, 1) + pltpu.roll(c, BACK, 1)

    def stencil(src, zs, k, y0):
        z0 = zs + SUB * k
        v = src[pl.ds(z0 - 1, SUB + 2), pl.ds(y0, SUB), :]
        s = v[0:SUB] + v[2:SUB + 2]
        s = s + src[pl.ds(z0, SUB), pl.ds(y0 - 1, SUB), :] + src[pl.ds(z0, SUB), pl.ds(y0 + 1, SUB), :]
        return v[1:SUB + 1], s + sx[pl.ds(SUB * k, SUB)]

    def sweep(lev, src, dst, rhs):
        first = rhs is None

        def ytile(t):
            y0 = pl.multiple_of(lev.ys + SUB * t, SUB)
            inside, nb = coefs(lev, y0)
            cc = (1.0 - OMEGA) - C6 * nb
            if first:
                ca, cb = jnp.where(inside, C6 * (cc + 1.0), 0.0), jnp.where(inside, C6 * C6, 0.0)
            else:
                ca, cb = jnp.where(inside, cc, 0.0), jnp.where(inside, C6, 0.0)
            roll_sums(src, lev.zs, lev.nzb, y0)

            def block(k):
                c, s = stencil(src, lev.zs, k, y0)
                z0 = lev.zs + SUB * k
                if not first:
                    s = s + rhs[pl.ds(z0, SUB), pl.ds(y0, SUB), :]
                dst[pl.ds(z0, SUB), pl.ds(y0, SUB), :] = ca * c + cb * s
            blocks(lev.nzb, 3 if lev.nzb == 9 else 2 if lev.nzb == 4 else 1, block)
            zghost_tile(lev, dst, y0)
        loop(lev.nyt, ytile)

    def residual_pass(lev, src, rhs):
        def ytile(t):
            y0 = pl.multiple_of(lev.oy + SUB * t, SUB)
            _, nb = coefs(lev, y0)
            dd = 6.0 + nb
            roll_sums(src, lev.oz, lev.n // SUB, y0)

            def block(k):
                c, s = stencil(src, lev.oz, k, y0)
                r = (rhs[pl.ds(lev.oz + SUB * k, SUB), pl.ds(y0, SUB), :] + (s - dd * c)).reshape(4, 2, SUB, LN)
                tr[pl.ds(4 * k, 4), pl.ds(tile(t), SUB), :] = r[:, 0] + r[:, 1]
            blocks(lev.n // SUB, max(1, lev.n // GRP // 2), block)
        loop(lev.n // SUB, ytile)

    zface = jnp.where(pz == 0, LN, 1)
    zdst = LN + 1 - zface + jnp.where(pz == 0, -1, 1)
    yface = jnp.where(py == 0, 135, SUB)
    yghost = jnp.where(py == 0, 136, 7)

    def order(t):
        return jnp.where(py == 0, 15 - t, t)

    def pieces(buf, par, o):
        rows, yrows = pl.ds(tile(o), SUB), pl.ds(tile(o + 1), SUB)
        return (pltpu.make_async_remote_copy(src_ref=xs.at[par, rows, :], dst_ref=xg.at[par, rows, :], send_sem=xss.at[par, o],
                                             recv_sem=xrs.at[par, o], device_id=dev(1), device_id_type=MESH),
                pltpu.make_async_remote_copy(src_ref=buf.at[zface, yrows, :], dst_ref=buf.at[zdst, yrows, :],
                                             send_sem=zss.at[par, o], recv_sem=zrs.at[par, o], device_id=dev(4),
                                             device_id_type=MESH))

    def face_rows(par):
        return remote(yp.at[par], yg.at[par], par, 2)

    def send(buf, par, t):
        for copy in pieces(buf, par, order(t)):
            copy.start()

        def first():
            def take_rows(i):
                for j in range(SUB):
                    yp[par, pl.ds(SUB * i + j, 1), :] = buf[SUB * i + j + 1, pl.ds(yface, 1), :]
            loop(GRP, take_rows)
            face_rows(par).start()
        pl.when(t == 0)(first)

    def receive(buf, par, t):
        def first():
            face_rows(par).wait()

            def put_rows(i):
                for j in range(SUB):
                    buf[SUB * i + j + 1, pl.ds(yghost, 1), :] = yg[par, pl.ds(SUB * i + j, 1), :]
            loop(GRP, put_rows)
        pl.when(t == 0)(first)
        for copy in pieces(buf, par, order(t)):
            copy.wait()

    def roll_sums0(src, par, t, sx):
        rows = pl.ds(tile(t + 1), SUB)
        ghost = xg[par, pl.ds(tile(t), SUB), :]
        left = jnp.where(low_x, 0.0, ghost)
        right = jnp.where(low_x, ghost, 0.0)
        zlow = jnp.where(pz == 0, 1.0, 0.0)
        for k in range(GRP):
            z = SUB * k
            v = src[pl.ds(z, SUB + 2), rows, :]
            here = v[1:SUB + 1]
            a = jnp.where(skew == (z - 1) % LN, left[None], here) + v[0:SUB]
            b = jnp.where(skew == z, right[None], here) + v[2:SUB + 2]
            s = pltpu.roll(a, 1, 2) + pltpu.roll(b, BACK, 2) - jnp.where(out_skew == z, here, 0.0)
            sx[pl.ds(z, SUB)] = s
        sx[0] = sx[0] - zlow * src[1, rows, :]
        sx[BACK] = sx[BACK] - (1.0 - zlow) * src[LN, rows, :]

    def cells0(src, t, z, sx):
        y0, planes = tile(t + 1), pl.ds(z + 1, GRP)
        s = sx[pl.ds(z, GRP)] + src[planes, pl.ds(y0 - 1, SUB), :] + src[planes, pl.ds(y0 + 1, SUB), :]
        return src[planes, pl.ds(y0, SUB), :], s + fr[pl.ds(z, GRP), pl.ds(tile(t), SUB), :]

    def yedge(t):
        r = row + tile(t + 1)
        return jnp.where((r == lev0.lo[1]) | (r == lev0.hi[1] - 1), 1.0, 0.0)

    def tiles0(src, par, work):
        receive(src, par, 0)
        roll_sums0(src, par, order(0), sx)

        def step(t):
            pl.when(t < 15)(lambda: receive(src, par, t + 1))

            def both(now, later):
                roll_sums0(src, par, order(t + 1 - (t + 1) // GRP), later)
                work(order(t), now)
            pl.when(t % 2 == 0)(lambda: both(sx, sy))
            pl.when(t % 2 == 1)(lambda: both(sy, sx))
            work_done(t)

        work_done = work.done
        loop(GRP, step)

    def sweep0(src, dst, par):
        def work(o, sums):
            cc = (1.0 - OMEGA) - C6 * yedge(o)
            pk = nil
            for k in range(SUB):
                c, s = cells0(src, o, GRP * k, sums)
                new = cc * c + C6 * s
                dst[pl.ds(GRP * k + 1, GRP), pl.ds(tile(o + 1), SUB), :] = new
                for j in range(GRP):
                    pk = jnp.where(face_lane == GRP * k + j, new[j], pk)
            xs[1 - par, pl.ds(tile(o), SUB), :] = pk
        work.done = lambda t: send(dst, 1 - par, t)
        tiles0(src, par, work)

    def residual0():
        def work(o, sums):
            dd = 6.0 + yedge(o)
            for k in range(SUB):
                c, s = cells0(ua, o, GRP * k, sums)
                ub[pl.ds(GRP * k + 1, GRP), pl.ds(tile(o + 1), SUB), :] = s - dd * c
        work.done = lambda t: None
        tiles0(ua, 0, work)

    def pair_sums(fine, j):
        for zc in range(fine.n // 2):
            lo, hi = pl.ds(GRP * j, SUB, stride=2), pl.ds(GRP * j + 1, SUB, stride=2)
            if fine.idx:
                s = tr[zc, lo, :] + tr[zc, hi, :]
                sx[zc] = 0.5 * (s + pltpu.roll(s, BACK, 1))
                continue
            lo, hi = pl.ds(GRP * j + SUB, SUB, stride=2), pl.ds(GRP * j + SUB + 1, SUB, stride=2)
            e = ub[2 * zc + 1, lo, :] + ub[2 * zc + 1, hi, :]
            o = ub[2 * zc + 2, lo, :] + ub[2 * zc + 2, hi, :]
            s = pltpu.roll(e, -2 * zc % LN, 1) + pltpu.roll(e + o, (-2 * zc - 1) % LN, 1)
            sx[zc] = 0.5 * (s + pltpu.roll(o, (-2 * zc - 2) % LN, 1))

    def restrict_to(fine, coarse, dst, pack):
        half = fine.n // 2
        own = (lane >= coarse.ox) & (lane < coarse.ox + half)
        idx = (fine.ox + 2 * (lane - coarse.ox)) & BACK
        pidx = fine.ox + 2 * (jnp.where(low_x, half - SUB, 0) + lane % SUB)
        group = lane // SUB
        step = half // 2

        def ytile(j):
            rows = pl.ds(pl.multiple_of(coarse.oy + SUB * j, SUB), SUB)
            pair_sums(fine, j)

            def move(q):
                pk = nil
                for i in range(step):
                    z = step * q + i
                    v = sx[z]
                    dst[coarse.oz + z, rows, :] = jnp.where(own, jnp.take_along_axis(v, idx, axis=1), 0.0)
                    if pack is not None:
                        pk = jnp.where(group == i % GRP, jnp.take_along_axis(v, pidx, axis=1), pk)
                        if i % GRP == GRP - 1:
                            pack[q * (step // GRP) + i // GRP, pl.ds(tile(j), SUB), :] = pk
            loop(2, move)
        loop(half // SUB, ytile)

    def restrict_packed(fine, me):
        idx = fine.ox + 2 * (lane % GRP)
        group = lane // GRP

        def ytile(j):
            pair_sums(fine, j)

            def collect(q):
                pk = nil
                for i in range(SUB):
                    pk = jnp.where(group == i, jnp.take_along_axis(sx[SUB * q + i], idx, axis=1), pk)
                g3[me, q, pl.ds(tile(j), SUB), :] = pk
            loop(2, collect)
        loop(2, ytile)

    def prolong_add(fine, coarse, esrc, dst, cbase):
        back_z = (fine.oz - fine.zs) // 2
        back_y = (fine.oy - fine.ys) // 2
        nct = fine.n // GRP + (0 if fine.nyt * SUB == fine.n else 1)
        cy_s = cbase[1] - 2 * back_y
        fy_s = fine.oy - 4 * back_y
        cz_s = cbase[0] - back_z - 1
        ncz = 4 * fine.nzb + 2
        xf = lane - fine.ox
        half = lax.shift_right_arithmetic(xf, 1)
        odd = xf - 2 * half
        i0 = half + cbase[2]
        i1 = jnp.clip(i0 + 2 * odd - 1, 0, BACK)
        i0 = jnp.clip(i0, 0, BACK)
        inx = (lane >= fine.lo[2]) & (lane < fine.hi[2])
        edge = (lane == fine.lo[2]) | (lane == fine.hi[2] - 1)
        wx = jnp.where(inx, jnp.where(edge, 0.5, 0.75), 0.0)
        wn = jnp.where(inx, 0.25, 0.0)

        def spread(z):
            for t in range(nct + 2):
                v = esrc[cz_s + z, pl.ds(pl.multiple_of(cy_s + SUB * (t - 1), SUB), SUB), :]
                xr[z, pl.ds(SUB * t, SUB), :] = (wx * jnp.take_along_axis(v, i0, axis=1)
                                                 + wn * jnp.take_along_axis(v, i1, axis=1))

        per = 6 if ncz % 6 == 0 else 2

        def spread_some(i):
            for q in range(per):
                spread(per * i + q)
        loop(ncz // per, spread_some)

        def ctile(t):
            fy = pl.multiple_of(fy_s + GRP * t, SUB)
            r = row + (cy_s + SUB * t)
            iny = (r >= coarse.lo[1]) & (r < coarse.hi[1])
            wny = jnp.where(iny, 0.25, 0.0)
            wde = jnp.where(iny, jnp.where(r == coarse.lo[1], 0.5, 0.75), 0.0)
            wdo = jnp.where(iny, jnp.where(r == coarse.hi[1] - 1, 0.5, 0.75), 0.0)

            def plane(i):
                for q in range(per):
                    z = per * i + q
                    e = xr[z, pl.ds(tile(t + 1), SUB), :]
                    tr[z, pl.ds(fy, SUB, stride=2), :] = wde * e + wny * xr[z, pl.ds(tile(t + 1) - 1, SUB), :]
                    tr[z, pl.ds(fy + 1, SUB, stride=2), :] = wdo * e + wny * xr[z, pl.ds(tile(t + 1) + 1, SUB), :]
            loop(ncz // per, plane)
        loop(nct, ctile)

        def ytile(t):
            o = t if fine.idx else order(t)
            y0 = pl.multiple_of(fine.ys + SUB * o, SUB)
            rows = pl.ds(y0, SUB)
            pk = nil
            for k in range(fine.nzb):
                z0 = fine.zs + SUB * k
                tb = tr[pl.ds(4 * k, 6), rows, :]
                mid = 0.75 * tb[1:5]
                add = jnp.stack([mid + 0.25 * tb[0:4], mid + 0.25 * tb[2:6]], axis=1).reshape(SUB, SUB, LN)
                if fine.idx:
                    dst[pl.ds(z0, SUB), rows, :] = dst[pl.ds(z0, SUB), rows, :] + add
                    continue
                for j in range(SUB):
                    z = SUB * k + j
                    new = dst[1 + z, rows, :] + pltpu.roll(add[j], z, 1)
                    dst[1 + z, rows, :] = new
                    pk = jnp.where(face_lane == z, new, pk)
            if fine.idx:
                zghost_tile(fine, dst, y0)
            else:
                xs[0, pl.ds(tile(o), SUB), :] = pk
                send(dst, 0, t)
        loop(fine.nyt, ytile)

    def exchange_wide(lev, ref, sendp, recvp, k):
        n, h = lev.n, HALO_PLANES[lev.idx]
        cx = remote(sendp, recvp, k, 1)
        cx.start()
        cx.wait()
        halo = jnp.where(low_x, lev.ox + n, lev.ox - SUB)
        inh = (lane >= halo) & (lane < halo + SUB)

        def ytile(t):
            rows = pl.ds(pl.multiple_of(lev.oy + SUB * t, SUB), SUB)
            for q in range(n // GRP):
                pk = recvp[q, pl.ds(tile(t), SUB), :]
                pk = pltpu.roll(pk, halo, 1)
                for i in range(GRP):
                    z = lev.oz + GRP * q + i
                    ref[z, rows, :] = jnp.where(inh, pltpu.roll(pk, (-SUB * i) % LN, 1), ref[z, rows, :])
        loop(n // SUB, ytile)
        fy = pl.multiple_of(jnp.where(py == 0, lev.oy + n - SUB, lev.oy), SUB)
        hy = pl.multiple_of(jnp.where(py == 0, lev.oy - SUB, lev.oy + n), SUB)
        fz = jnp.where(pz == 0, lev.oz + n - h, lev.oz)
        hz = jnp.where(pz == 0, lev.oz - h, lev.oz + n)
        copies = [
            remote(ref.at[pl.ds(lev.oz, n), pl.ds(fy, SUB), :], ref.at[pl.ds(lev.oz, n), pl.ds(hy, SUB), :], k + 1, 2),
            remote(ref.at[pl.ds(fz, h), pl.ds(lev.oy, n), :], ref.at[pl.ds(hz, h), pl.ds(lev.oy, n), :], k + 2, 4),
            remote(ref.at[pl.ds(fz, h), pl.ds(fy, SUB), :], ref.at[pl.ds(hz, h), pl.ds(hy, SUB), :], k + 3, 6),
        ]
        for c in copies:
            c.start()
        for c in copies:
            c.wait()
        zghost(lev, ref)

    me = 4 * pz + 2 * py + px

    def gather3():
        copies = [remote(g3.at[me], g3.at[me], 14 + code, code) for code in range(1, SUB)]
        for c in copies:
            c.start()
        for c in copies:
            c.wait()
        lev = levels[3]
        in_lo = (lane >= lev.ox) & (lane < lev.ox + GRP)
        in_hi = (lane >= lev.ox + GRP) & (lane < lev.ox + 32)

        def ytile(t):
            rows = pl.ds(pl.multiple_of(lev.oy + SUB * t, SUB), SUB)
            by = t // 2
            r0 = pl.ds(tile(t % 2), SUB)
            for q in range(4):
                lo = g3[4 * (q // 2) + 2 * by, q % 2, r0, :]
                hi = g3[4 * (q // 2) + 2 * by + 1, q % 2, r0, :]
                for i in range(SUB):
                    a = pltpu.roll(lo, (lev.ox - GRP * i) % LN, 1)
                    b = pltpu.roll(hi, (lev.ox + GRP - GRP * i) % LN, 1)
                    b3[lev.oz + SUB * q + i, rows, :] = jnp.where(in_lo, a, jnp.where(in_hi, b, 0.0))
        loop(4, ytile)
        zghost(lev, b3)

    def coarse_solve():
        lev = levels[5]

        def zstep(z, acc):
            b = b5[lev.oz + z, pl.ds(lev.oy, SUB), :] * 64.0
            acc = list(acc)
            for x in range(SUB):
                col = jnp.broadcast_to(b[:, lev.ox + x:lev.ox + x + 1], (SUB, LN))
                for j in range(4):
                    acc[j] = acc[j] + cinv[j, pl.ds(z * 64 + x, SUB, stride=SUB), :] * col
            return tuple(acc)
        acc = lax.fori_loop(0, SUB, zstep, (jnp.zeros((SUB, LN), F32),) * 4)
        lines = [jnp.broadcast_to(jnp.sum(a, axis=0, keepdims=True), (SUB, LN)) for a in acc]
        own = (lane >= lev.ox) & (lane < lev.ox + SUB)
        for z in range(SUB):
            idx = jnp.clip((z % 2) * 64 + row * SUB + lane - lev.ox, 0, 127)
            e5[lev.oz + z, pl.ds(lev.oy, SUB), :] = jnp.where(own, jnp.take_along_axis(lines[z // 2], idx, axis=1), 0.0)
        zghost(lev, e5)

    def base_of(lev):
        return (lev.oz, lev.oy, lev.ox)

    def local_visit(fine, v, rhs, descend, ecoarse, coarse, cbase):
        sweep(fine, rhs, v.at[0], None)
        zghost(fine, v.at[0])
        residual_pass(fine, v.at[0], rhs)
        descend()
        prolong_add(fine, coarse, ecoarse, v.at[0], cbase)
        loop(2, lambda i: sweep(fine, v.at[i], v.at[1 - i], rhs))

    def descend4():
        restrict_to(levels[4], levels[5], b5, None)
        coarse_solve()

    def descend3():
        restrict_to(levels[3], levels[4], b4, None)
        zghost(levels[4], b4)
        local_visit(levels[4], v4, b4, descend4, e5, levels[5], base_of(levels[5]))

    def descend2():
        restrict_packed(levels[2], me)
        gather3()
        local_visit(levels[3], v3, b3, descend3, v4.at[0], levels[4], base_of(levels[4]))

    def descend1():
        restrict_to(levels[1], levels[2], b2, p2s)
        exchange_wide(levels[2], b2, p2s, p2r, 10)
        oz, oy, ox = base_of(levels[3])
        local_visit(levels[2], v2, b2, descend2, v3.at[0], levels[3], (oz + GRP * pz, oy + GRP * py, ox + GRP * px))

    def skew_in(t):
        o = order(t)
        for copy in load(o):
            copy.wait()
        rows, frows = pl.ds(tile(o + 1), SUB), pl.ds(tile(o), SUB)
        pk = nil
        for z in range(LN):
            moved = pltpu.roll(ua[z + 1, rows, :], z, 1)
            ua[z + 1, rows, :] = moved
            pk = jnp.where(face_lane == z, moved, pk)
            fr[z, frows, :] = pltpu.roll(fr[z, frows, :] * INV_G2, z, 1)
        xs[0, frows, :] = pk
        send(ua, 0, t)
    loop(GRP, skew_in)
    for copy in load_c:
        copy.wait()

    def correct():
        residual0()
        restrict_to(lev0, levels[1], b1, p1s)
        exchange_wide(levels[1], b1, p1s, p1r, 6)
        local_visit(levels[1], v1, b1, descend1, v2.at[0], levels[2], base_of(levels[2]))
        prolong_add(lev0, levels[1], v1.at[0], ua, base_of(levels[1]))

    def half_cycle(h):
        sweep0(ua, ub, 0)
        sweep0(ub, ua, 1)
        pl.when(h % 2 == 0)(correct)
    loop(2 * CYCLES, half_cycle)
    loop(GRP, lambda t: receive(ua, 0, t))

    def store(t):
        return pltpu.make_async_copy(ub.at[pl.ds(1, LN), pl.ds(tile(t + 1), SUB), :], out_hbm.at[:, pl.ds(tile(t), SUB), :],
                                     lsem.at[t])

    def skew_out(t):
        rows = pl.ds(tile(t + 1), SUB)
        for z in range(LN):
            ub[z + 1, rows, :] = pltpu.roll(ua[z + 1, rows, :], -z % LN, 1)
        store(t).start()
    loop(GRP, skew_out)
    loop(GRP, lambda t: store(t).wait())


def solution(mesh):
    grid_spec = P(('batch', 'gz'), 'gy', 'gx')

    def vmem(*shape):
        return pltpu.VMEM(shape, F32)

    scratch = [vmem(130, 144, LN), vmem(130, 144, LN), vmem(LN, LN, LN), vmem(66, 144, LN), vmem(66, 80, LN), vmem(LN, SUB, LN), vmem(LN, SUB, LN)]
    for shape in ((82, 96), (50, 64), (34, 72), (18, 48)):
        scratch += [vmem(2, *shape, LN), vmem(*shape, LN)]
    scratch += [vmem(10, 32, LN), vmem(10, 32, LN), vmem(4, 512, LN)]
    scratch += [vmem(2, LN, LN)] * 4
    scratch += [vmem(4, 64, LN)] * 2 + [vmem(2, 32, LN)] * 2 + [vmem(SUB, 2, GRP, LN)]
    scratch += [pltpu.SemaphoreType.DMA((22,)), pltpu.SemaphoreType.DMA((22,))]
    scratch += [pltpu.SemaphoreType.DMA((2, GRP))] * 4 + [pltpu.SemaphoreType.DMA((36,))]

    call = pl.pallas_call(
        solve_kernel,
        out_shape=jax.ShapeDtypeStruct((LN, LN, LN), F32),
        in_specs=[pl.BlockSpec(memory_space=pl.ANY)] * 3,
        out_specs=pl.BlockSpec(memory_space=pl.ANY),
        scratch_shapes=scratch,
        name='multigrid',
        compiler_params=pltpu.CompilerParams(collective_id=0, has_side_effects=True, vmem_limit_bytes=67043328),
    )
    return jax.shard_map(call, mesh=mesh, in_specs=(grid_spec, grid_spec, P()), out_specs=grid_spec, check_vma=False)
```

```python
import jax
import jax.numpy as jnp
from jax import lax
from jax.experimental import pallas as pl
from jax.experimental.pallas import tpu as pltpu
from jax.sharding import PartitionSpec as P

OMEGA = 2.0 / 3.0
C6 = OMEGA / 6.0
CYCLES = 2
MESH = pl.DeviceIdType.MESH
F32 = jnp.float32
PAIR, SUB, GRP, LN = 2, 8, 16, 128
HALO_PLANES = {1: 4, 2: 5}
BACK = LN - 1
INV_G2 = 1.0 / 65536.0


class Level:
    def __init__(self, idx, n, off, shape, pos, split):
        self.idx, self.n, self.shape = idx, n, shape
        self.oz, self.oy, self.ox = off
        self.split = split
        if split:
            self.lo = tuple(o - p * n for o, p in zip(off, pos))
            self.hi = tuple(l + PAIR * n for l in self.lo)
        else:
            self.lo = off
            self.hi = tuple(o + n for o in off)
        wide = SUB if (split and idx > 0) else 0
        self.zs = self.oz - wide * pos[0] if wide else self.oz
        self.ys = self.oy - wide * pos[1] if wide else self.oy
        self.nzb = (n + wide) // SUB
        self.nyt = (n + wide) // SUB
        if split:
            self.ghosts = [(jnp.where(pos[0] == 0, self.oz - 1, self.oz + n), jnp.where(pos[0] == 0, self.oz, self.oz + n - 1))]
        else:
            self.ghosts = [(self.oz - 1, self.oz), (self.oz + n, self.oz + n - 1)]


def solve_kernel(f_hbm, u_hbm, c_hbm, out_hbm,
                 ua, ub, fr, tr, xr, sx, sy, v1, b1, v2, b2, v3, b3, v4, b4, e5, b5, cinv,
                 xs, xg, yp, yg, p1s, p1r, p2s, p2r, h1s, h1r, h2s, h2r, g3, ssem, rsem, xss, xrs, zss, zrs, wss, wrs, lsem):
    pz, py, px = lax.axis_index('gz'), lax.axis_index('gy'), lax.axis_index('gx')
    pos = (pz, py, px)
    lane = lax.broadcasted_iota(jnp.int32, (SUB, LN), 1)
    row = lax.broadcasted_iota(jnp.int32, (SUB, LN), 0)
    nil = jnp.zeros((SUB, LN), F32)
    levels = [
        Level(0, LN, (1, SUB, 0), (130, 144), pos, True),
        Level(1, 64, (9, GRP, 32), (82, 96), pos, True),
        Level(PAIR, 32, (9, GRP, 48), (50, 64), pos, True),
        Level(3, 32, (1, GRP, 48), (34, 72), pos, False),
        Level(4, GRP, (1, GRP, 48), (18, 48), pos, False),
        Level(5, SUB, (1, GRP, 48), (10, 32), pos, False),
    ]
    lev0 = levels[0]
    low_x = px == 0
    face_lane = jnp.where(low_x, (lane + 1) & BACK, lane)
    out_lane = jnp.where(low_x, lane, (lane + 1) & BACK)

    skew = (lax.broadcasted_iota(jnp.int32, (SUB, SUB, LN), PAIR) - lax.broadcasted_iota(jnp.int32, (SUB, SUB, LN), 0)) & BACK
    out_skew = jnp.where(low_x, skew, (skew + 1) & BACK)

    def dev(code):
        ids = {}
        if code & 4:
            ids['gz'] = 1 - pz
        if code & PAIR:
            ids['gy'] = 1 - py
        if code & 1:
            ids['gx'] = 1 - px
        return ids

    def remote(src, dst, k, code):
        return pltpu.make_async_remote_copy(src_ref=src, dst_ref=dst, send_sem=ssem.at[k], recv_sem=rsem.at[k],
                                            device_id=dev(code), device_id_type=MESH)

    def loop(n, body):
        lax.fori_loop(0, n, lambda i, c: (body(i), c)[1], 0)

    def tile(i):
        return pl.multiple_of(SUB * i, SUB)

    def load(t):
        rows = pl.ds(tile(t), SUB)
        return (pltpu.make_async_copy(u_hbm.at[:, rows, :], ua.at[pl.ds(1, LN), pl.ds(tile(t + 1), SUB), :], lsem.at[t]),
                pltpu.make_async_copy(f_hbm.at[:, rows, :], fr.at[:, rows, :], lsem.at[GRP + t]))

    def start_load(t):
        for copy in load(t):
            copy.start()
    loop(GRP, lambda t: start_load(jnp.where(py == 0, 15 - t, t)))
    load_c = [pltpu.make_async_copy(c_hbm.at[:, pl.ds(LN * j, LN)], cinv.at[j], lsem.at[32 + j]) for j in range(4)]
    for copy in load_c:
        copy.start()

    def zero(ref):
        def body(i):
            ref[i] = jnp.zeros(ref.shape[1:], F32)
        loop(ref.shape[0], body)

    for ref in (v1.at[0], v1.at[1], b1, v2.at[0], v2.at[1], b2, v3.at[0], v3.at[1], b3, v4.at[0], v4.at[1], b4, e5):
        zero(ref)

    def zero_rows(i):
        for buf in (ua, ub):
            buf[i, pl.ds(0, SUB), :] = nil
            buf[i, pl.ds(136, SUB), :] = nil
    loop(130, zero_rows)
    zout = jnp.where(pz == 0, 0, 129)

    def zero_plane(t):
        for buf in (ua, ub):
            buf[zout, pl.ds(tile(t), SUB), :] = nil
    loop(18, zero_plane)

    barrier = pltpu.get_barrier_semaphore()
    for code in range(1, SUB):
        pl.semaphore_signal(barrier, inc=1, device_id=dev(code), device_id_type=MESH)
    pl.semaphore_wait(barrier, 7)

    def coefs(lev, y0):
        r = row + y0
        inside = (r >= lev.lo[1]) & (r < lev.hi[1]) & (lane >= lev.lo[PAIR]) & (lane < lev.hi[PAIR])
        one = jnp.ones((SUB, LN), F32)
        nb = (jnp.where(r == lev.lo[1], one, nil) + jnp.where(r == lev.hi[1] - 1, one, nil)
              + jnp.where(lane == lev.lo[PAIR], one, nil) + jnp.where(lane == lev.hi[PAIR] - 1, one, nil))
        return inside, nb

    def zghost_tile(lev, ref, y0):
        for ghost, face in lev.ghosts:
            ref[ghost, pl.ds(y0, SUB), :] = -ref[face, pl.ds(y0, SUB), :]

    def zghost(lev, ref):
        loop(lev.shape[1] // SUB, lambda t: zghost_tile(lev, ref, tile(t)))

    def several(count, per, body):
        def step(i):
            for k in range(per):
                body(i * per + k)
        loop(count // per, step)

    def roll_sums(src, zs, nzb, y0):
        for k in range(nzb):
            c = src[pl.ds(zs + SUB * k, SUB), pl.ds(y0, SUB), :]
            sx[pl.ds(SUB * k, SUB)] = pltpu.roll(c, 1, PAIR) + pltpu.roll(c, BACK, PAIR)

    def stencil(src, zs, k, y0):
        z0 = zs + SUB * k
        v = src[pl.ds(z0 - 1, SUB + PAIR), pl.ds(y0, SUB), :]
        s = v[0:SUB] + v[PAIR:SUB + PAIR]
        s = s + src[pl.ds(z0, SUB), pl.ds(y0 - 1, SUB), :] + src[pl.ds(z0, SUB), pl.ds(y0 + 1, SUB), :]
        return v[1:SUB + 1], s + sx[pl.ds(SUB * k, SUB)]

    def sweep(lev, src, dst, rhs):
        first = rhs is None

        def ytile(t):
            y0 = pl.multiple_of(lev.ys + SUB * t, SUB)
            inside, nb = coefs(lev, y0)
            cc = (1.0 - OMEGA) - C6 * nb
            if first:
                ca, cb = jnp.where(inside, C6 * (cc + 1.0), 0.0), jnp.where(inside, C6 * C6, 0.0)
            else:
                ca, cb = jnp.where(inside, cc, 0.0), jnp.where(inside, C6, 0.0)
            roll_sums(src, lev.zs, lev.nzb, y0)

            def block(k):
                c, s = stencil(src, lev.zs, k, y0)
                z0 = lev.zs + SUB * k
                if not first:
                    s = s + rhs[pl.ds(z0, SUB), pl.ds(y0, SUB), :]
                dst[pl.ds(z0, SUB), pl.ds(y0, SUB), :] = ca * c + cb * s
            several(lev.nzb, 3 if lev.nzb == 9 else PAIR if lev.nzb == 4 else 1, block)
            zghost_tile(lev, dst, y0)
        loop(lev.nyt, ytile)

    def residual_pass(lev, src, rhs):
        def ytile(t):
            y0 = pl.multiple_of(lev.oy + SUB * t, SUB)
            _, nb = coefs(lev, y0)
            dd = 6.0 + nb
            roll_sums(src, lev.oz, lev.n // SUB, y0)

            def block(k):
                c, s = stencil(src, lev.oz, k, y0)
                r = (rhs[pl.ds(lev.oz + SUB * k, SUB), pl.ds(y0, SUB), :] + (s - dd * c)).reshape(4, PAIR, SUB, LN)
                tr[pl.ds(4 * k, 4), pl.ds(tile(t), SUB), :] = r[:, 0] + r[:, 1]
            several(lev.n // SUB, max(1, lev.n // GRP // PAIR), block)
        loop(lev.n // SUB, ytile)

    zface = jnp.where(pz == 0, LN, 1)
    zdst = LN + 1 - zface + jnp.where(pz == 0, -1, 1)
    yface = jnp.where(py == 0, 135, SUB)
    yghost = jnp.where(py == 0, 136, 7)

    def order(t):
        return jnp.where(py == 0, 15 - t, t)

    def pieces(buf, par, o):
        rows, yrows = pl.ds(tile(o), SUB), pl.ds(tile(o + 1), SUB)
        return (pltpu.make_async_remote_copy(src_ref=xs.at[par, rows, :], dst_ref=xg.at[par, rows, :], send_sem=xss.at[par, o],
                                             recv_sem=xrs.at[par, o], device_id=dev(1), device_id_type=MESH),
                pltpu.make_async_remote_copy(src_ref=buf.at[zface, yrows, :], dst_ref=buf.at[zdst, yrows, :],
                                             send_sem=zss.at[par, o], recv_sem=zrs.at[par, o], device_id=dev(4),
                                             device_id_type=MESH))

    def face_rows(par):
        return remote(yp.at[par], yg.at[par], par, PAIR)

    def send(buf, par, t):
        for copy in pieces(buf, par, order(t)):
            copy.start()

        def first():
            def take_rows(i):
                for j in range(SUB):
                    yp[par, pl.ds(SUB * i + j, 1), :] = buf[SUB * i + j + 1, pl.ds(yface, 1), :]
            loop(GRP, take_rows)
            face_rows(par).start()
        pl.when(t == 0)(first)

    def receive(buf, par, t):
        def first():
            face_rows(par).wait()

            def put_rows(i):
                for j in range(SUB):
                    buf[SUB * i + j + 1, pl.ds(yghost, 1), :] = yg[par, pl.ds(SUB * i + j, 1), :]
            loop(GRP, put_rows)
        pl.when(t == 0)(first)
        for copy in pieces(buf, par, order(t)):
            copy.wait()

    def roll_sums0(src, par, t, sx):
        rows = pl.ds(tile(t + 1), SUB)
        ghost = xg[par, pl.ds(tile(t), SUB), :]
        left = jnp.where(low_x, 0.0, ghost)
        right = jnp.where(low_x, ghost, 0.0)
        zlow = jnp.where(pz == 0, 1.0, 0.0)
        for k in range(GRP):
            z = SUB * k
            v = src[pl.ds(z, SUB + PAIR), rows, :]
            here = v[1:SUB + 1]
            a = jnp.where(skew == (z - 1) % LN, left[None], here) + v[0:SUB]
            b = jnp.where(skew == z, right[None], here) + v[PAIR:SUB + PAIR]
            s = pltpu.roll(a, 1, PAIR) + pltpu.roll(b, BACK, PAIR) - jnp.where(out_skew == z, here, 0.0)
            sx[pl.ds(z, SUB)] = s
        sx[0] = sx[0] - zlow * src[1, rows, :]
        sx[BACK] = sx[BACK] - (1.0 - zlow) * src[LN, rows, :]

    def cells0(src, t, z, sx):
        y0, planes = tile(t + 1), pl.ds(z + 1, GRP)
        s = sx[pl.ds(z, GRP)] + src[planes, pl.ds(y0 - 1, SUB), :] + src[planes, pl.ds(y0 + 1, SUB), :]
        return src[planes, pl.ds(y0, SUB), :], s + fr[pl.ds(z, GRP), pl.ds(tile(t), SUB), :]

    def yedge(t):
        r = row + tile(t + 1)
        return jnp.where((r == lev0.lo[1]) | (r == lev0.hi[1] - 1), 1.0, 0.0)

    def tiles0(src, par, work):
        receive(src, par, 0)
        roll_sums0(src, par, order(0), sx)

        def step(t):
            pl.when(t < 15)(lambda: receive(src, par, t + 1))

            def both(now, later):
                roll_sums0(src, par, order(t + 1 - (t + 1) // GRP), later)
                work(order(t), now)
            pl.when(t % PAIR == 0)(lambda: both(sx, sy))
            pl.when(t % PAIR == 1)(lambda: both(sy, sx))
            work_done(t)

        work_done = work.done
        loop(GRP, step)

    def sweep0(src, dst, par):
        def work(o, sums):
            cc = (1.0 - OMEGA) - C6 * yedge(o)
            pk = nil
            for k in range(SUB):
                c, s = cells0(src, o, GRP * k, sums)
                new = cc * c + C6 * s
                dst[pl.ds(GRP * k + 1, GRP), pl.ds(tile(o + 1), SUB), :] = new
                for j in range(GRP):
                    pk = jnp.where(face_lane == GRP * k + j, new[j], pk)
            xs[1 - par, pl.ds(tile(o), SUB), :] = pk
        work.done = lambda t: send(dst, 1 - par, t)
        tiles0(src, par, work)

    def residual0():
        def work(o, sums):
            dd = 6.0 + yedge(o)
            for k in range(SUB):
                c, s = cells0(ua, o, GRP * k, sums)
                ub[pl.ds(GRP * k + 1, GRP), pl.ds(tile(o + 1), SUB), :] = s - dd * c
        work.done = lambda t: None
        tiles0(ua, 0, work)

    def pair_sums(fine, j):
        for zc in range(fine.n // PAIR):
            lo, hi = pl.ds(GRP * j, SUB, stride=PAIR), pl.ds(GRP * j + 1, SUB, stride=PAIR)
            if fine.idx:
                s = tr[zc, lo, :] + tr[zc, hi, :]
                sx[zc] = 0.5 * (s + pltpu.roll(s, BACK, 1))
                continue
            lo, hi = pl.ds(GRP * j + SUB, SUB, stride=PAIR), pl.ds(GRP * j + SUB + 1, SUB, stride=PAIR)
            e = ub[PAIR * zc + 1, lo, :] + ub[PAIR * zc + 1, hi, :]
            o = ub[PAIR * zc + PAIR, lo, :] + ub[PAIR * zc + PAIR, hi, :]
            s = pltpu.roll(e, -PAIR * zc % LN, 1) + pltpu.roll(e + o, (-PAIR * zc - 1) % LN, 1)
            sx[zc] = 0.5 * (s + pltpu.roll(o, (-PAIR * zc - PAIR) % LN, 1))

    def restrict_to(fine, coarse, dst, pack=None):
        half = fine.n // PAIR
        own = (lane >= coarse.ox) & (lane < coarse.ox + half)
        idx = (fine.ox + PAIR * (lane - coarse.ox)) & BACK
        pidx = fine.ox + PAIR * (jnp.where(low_x, half - SUB, 0) + lane % SUB)
        group = lane // SUB
        step = half // PAIR

        def ytile(t):
            j = t if pack is None else jnp.where(py == 0, half // SUB - 1 - t, t)
            rows = pl.ds(pl.multiple_of(coarse.oy + SUB * j, SUB), SUB)
            pair_sums(fine, j)

            def move(q):
                pk = nil
                for i in range(step):
                    z = step * q + i
                    v = sx[z]
                    dst[coarse.oz + z, rows, :] = jnp.where(own, jnp.take_along_axis(v, idx, axis=1), 0.0)
                    if pack is not None:
                        pk = jnp.where(group == i % GRP, jnp.take_along_axis(v, pidx, axis=1), pk)
                        if i % GRP == GRP - 1:
                            pack[q * (step // GRP) + i // GRP, pl.ds(tile(j), SUB), :] = pk
            loop(PAIR, move)
            if pack is not None:
                copies = edge_pieces(coarse, dst, j)
                copies[0].start()

                def start_rest():
                    for copy in copies[1:]:
                        copy.start()
                pl.when(t == 0)(start_rest)
        loop(half // SUB, ytile)

    def wide_spans(lev):
        n, h = lev.n, HALO_PLANES[lev.idx]
        fy = pl.multiple_of(jnp.where(py == 0, lev.oy + n - SUB, lev.oy), SUB)
        hy = pl.multiple_of(jnp.where(py == 0, lev.oy - SUB, lev.oy + n), SUB)
        fz = jnp.where(pz == 0, lev.oz + n - h, lev.oz)
        hz = jnp.where(pz == 0, lev.oz - h, lev.oz + n)
        return fy, hy, pl.ds(fz, h), pl.ds(hz, h)

    def edge_pieces(lev, ref, j):
        fy, hy, fz, hz = wide_spans(lev)
        rows, own, k = pl.ds(pl.multiple_of(lev.oy + SUB * j, SUB), SUB), pl.ds(lev.oz, lev.n), lev.idx
        piece = pltpu.make_async_remote_copy(src_ref=ref.at[fz, rows, :], dst_ref=ref.at[hz, rows, :],
                                             send_sem=wss.at[k - 1, j], recv_sem=wrs.at[k - 1, j], device_id=dev(4),
                                             device_id_type=MESH)
        return (piece, remote(ref.at[own, pl.ds(fy, SUB), :], ref.at[own, pl.ds(hy, SUB), :], 4 * k + 3, PAIR),
                remote(ref.at[fz, pl.ds(fy, SUB), :], ref.at[hz, pl.ds(hy, SUB), :], 4 * k + 4, 6))

    def restrict_packed(fine, me):
        idx = fine.ox + PAIR * (lane % GRP)
        group = lane // GRP

        def ytile(j):
            pair_sums(fine, j)

            def collect(q):
                pk = nil
                for i in range(SUB):
                    pk = jnp.where(group == i, jnp.take_along_axis(sx[SUB * q + i], idx, axis=1), pk)
                g3[me, q, pl.ds(tile(j), SUB), :] = pk
            loop(PAIR, collect)
        loop(PAIR, ytile)

    def prolong_add(fine, coarse, esrc, dst, cbase):
        back_z = (fine.oz - fine.zs) // PAIR
        back_y = (fine.oy - fine.ys) // PAIR
        nct = fine.n // GRP + (0 if fine.nyt * SUB == fine.n else 1)
        cy_s = cbase[1] - PAIR * back_y
        fy_s = fine.oy - 4 * back_y
        cz_s = cbase[0] - back_z - 1
        ncz = 4 * fine.nzb + PAIR
        xf = lane - fine.ox
        half = lax.shift_right_arithmetic(xf, 1)
        odd = xf - PAIR * half
        i0 = half + cbase[PAIR]
        i1 = jnp.clip(i0 + PAIR * odd - 1, 0, BACK)
        i0 = jnp.clip(i0, 0, BACK)
        inx = (lane >= fine.lo[PAIR]) & (lane < fine.hi[PAIR])
        edge = (lane == fine.lo[PAIR]) | (lane == fine.hi[PAIR] - 1)
        wx = jnp.where(inx, jnp.where(edge, 0.5, 0.75), 0.0)
        wn = jnp.where(inx, 0.25, 0.0)

        def spread(z):
            for t in range(nct + PAIR):
                v = esrc[cz_s + z, pl.ds(pl.multiple_of(cy_s + SUB * (t - 1), SUB), SUB), :]
                xr[z, pl.ds(SUB * t, SUB), :] = (wx * jnp.take_along_axis(v, i0, axis=1)
                                                 + wn * jnp.take_along_axis(v, i1, axis=1))

        per = 6 if ncz % 6 == 0 else PAIR

        def spread_some(i):
            for q in range(per):
                spread(per * i + q)
        loop(ncz // per, spread_some)

        def ctile(t):
            fy = pl.multiple_of(fy_s + GRP * t, SUB)
            r = row + (cy_s + SUB * t)
            iny = (r >= coarse.lo[1]) & (r < coarse.hi[1])
            wny = jnp.where(iny, 0.25, 0.0)
            wde = jnp.where(iny, jnp.where(r == coarse.lo[1], 0.5, 0.75), 0.0)
            wdo = jnp.where(iny, jnp.where(r == coarse.hi[1] - 1, 0.5, 0.75), 0.0)

            def plane(i):
                for q in range(per):
                    z = per * i + q
                    e = xr[z, pl.ds(tile(t + 1), SUB), :]
                    tr[z, pl.ds(fy, SUB, stride=PAIR), :] = wde * e + wny * xr[z, pl.ds(tile(t + 1) - 1, SUB), :]
                    tr[z, pl.ds(fy + 1, SUB, stride=PAIR), :] = wdo * e + wny * xr[z, pl.ds(tile(t + 1) + 1, SUB), :]
            loop(ncz // per, plane)
        loop(nct, ctile)

        def ytile(t):
            o = t if fine.idx else order(t)
            y0 = pl.multiple_of(fine.ys + SUB * o, SUB)
            rows = pl.ds(y0, SUB)
            pk = nil
            for k in range(fine.nzb):
                z0 = fine.zs + SUB * k
                tb = tr[pl.ds(4 * k, 6), rows, :]
                mid = 0.75 * tb[1:5]
                add = jnp.stack([mid + 0.25 * tb[0:4], mid + 0.25 * tb[PAIR:6]], axis=1).reshape(SUB, SUB, LN)
                if fine.idx:
                    dst[pl.ds(z0, SUB), rows, :] = dst[pl.ds(z0, SUB), rows, :] + add
                    continue
                for j in range(SUB):
                    z = SUB * k + j
                    new = dst[1 + z, rows, :] + pltpu.roll(add[j], z, 1)
                    dst[1 + z, rows, :] = new
                    pk = jnp.where(face_lane == z, new, pk)
            if fine.idx:
                zghost_tile(fine, dst, y0)
            else:
                xs[0, pl.ds(tile(o), SUB), :] = pk
                send(dst, 0, t)
        loop(fine.nyt, ytile)

    def exchange_wide(lev, ref, sendp, recvp, sendh, recvh):
        n, h, k = lev.n, HALO_PLANES[lev.idx], lev.idx
        hy = pl.multiple_of(jnp.where(py == 0, lev.oy + n, lev.oy - SUB), SUB)
        hz = jnp.where(pz == 0, lev.oz + n, lev.oz - h)
        cx = remote(sendp, recvp, 4 * k + 1, 1)
        cx.start()
        for copy in edge_pieces(lev, ref, 0)[1:]:
            copy.wait()
        loop(n // SUB, lambda j: edge_pieces(lev, ref, j)[0].wait())
        group = lane // SUB
        face = jnp.where(low_x, lev.ox + n - SUB, lev.ox)
        halo = jnp.where(low_x, lev.ox + n, lev.ox - SUB)
        inh = (lane >= halo) & (lane < halo + SUB)

        def spots(q):
            return pl.ds(pl.multiple_of(jnp.where(q < n // SUB, lev.oy + SUB * q, hy), SUB), SUB)

        def gather_faces(z, planes, rows):
            pk = nil
            for i in range(planes):
                pk = jnp.where(group == i, pltpu.roll(ref[z + i, rows, :], (SUB * i - face) & BACK, 1), pk)
            return pk
        nq = n // GRP

        def collect_y(q):
            sendh[q] = gather_faces(lev.oz + GRP * q, GRP, pl.ds(hy, SUB))

        def collect_z(q):
            sendh[nq + q] = gather_faces(hz, h, spots(q))
        zper = 3 if n // SUB == SUB else n // SUB + 1
        several(nq, PAIR, collect_y)
        several(n // SUB + 1, zper, collect_z)
        ch = remote(sendh, recvh, 4 * k + PAIR, 1)
        ch.start()
        cx.wait()

        def put(pk, z, planes, rows):
            pk = pltpu.roll(pk, halo, 1)
            for i in range(planes):
                ref[z + i, rows, :] = jnp.where(inh, pltpu.roll(pk, (-SUB * i) % LN, 1), ref[z + i, rows, :])

        def ytile(t):
            rows = pl.ds(pl.multiple_of(lev.oy + SUB * t, SUB), SUB)
            for q in range(nq):
                put(recvp[q, pl.ds(tile(t), SUB), :], lev.oz + GRP * q, GRP, rows)
        loop(n // SUB, ytile)
        ch.wait()

        several(nq, PAIR, lambda q: put(recvh[q], lev.oz + GRP * q, GRP, pl.ds(hy, SUB)))
        several(n // SUB + 1, zper, lambda q: put(recvh[nq + q], hz, h, spots(q)))
        zghost(lev, ref)

    me = 4 * pz + PAIR * py + px

    def gather3():
        copies = [remote(g3.at[me], g3.at[me], 13 + code, code) for code in range(1, SUB)]
        for c in copies:
            c.start()
        for c in copies:
            c.wait()
        lev = levels[3]
        in_lo = (lane >= lev.ox) & (lane < lev.ox + GRP)
        in_hi = (lane >= lev.ox + GRP) & (lane < lev.ox + 32)

        def ytile(t):
            rows = pl.ds(pl.multiple_of(lev.oy + SUB * t, SUB), SUB)
            by = t // PAIR
            r0 = pl.ds(tile(t % PAIR), SUB)
            for q in range(4):
                lo = g3[4 * (q // PAIR) + PAIR * by, q % PAIR, r0, :]
                hi = g3[4 * (q // PAIR) + PAIR * by + 1, q % PAIR, r0, :]
                for i in range(SUB):
                    a = pltpu.roll(lo, (lev.ox - GRP * i) % LN, 1)
                    b = pltpu.roll(hi, (lev.ox + GRP - GRP * i) % LN, 1)
                    b3[lev.oz + SUB * q + i, rows, :] = jnp.where(in_lo, a, jnp.where(in_hi, b, 0.0))
        loop(4, ytile)
        zghost(lev, b3)

    def coarse_solve():
        lev = levels[5]

        def zstep(z, acc):
            b = b5[lev.oz + z, pl.ds(lev.oy, SUB), :] * 64.0
            acc = list(acc)
            for x in range(SUB):
                col = jnp.broadcast_to(b[:, lev.ox + x:lev.ox + x + 1], (SUB, LN))
                for j in range(4):
                    acc[j] = acc[j] + cinv[j, pl.ds(z * 64 + x, SUB, stride=SUB), :] * col
            return tuple(acc)
        acc = lax.fori_loop(0, SUB, zstep, (jnp.zeros((SUB, LN), F32),) * 4)
        lines = [jnp.broadcast_to(jnp.sum(a, axis=0, keepdims=True), (SUB, LN)) for a in acc]
        own = (lane >= lev.ox) & (lane < lev.ox + SUB)
        for z in range(SUB):
            idx = jnp.clip((z % PAIR) * 64 + row * SUB + lane - lev.ox, 0, 127)
            e5[lev.oz + z, pl.ds(lev.oy, SUB), :] = jnp.where(own, jnp.take_along_axis(lines[z // PAIR], idx, axis=1), 0.0)
        zghost(lev, e5)

    def base_of(lev):
        return (lev.oz, lev.oy, lev.ox)

    def local_visit(fine, v, rhs, descend, ecoarse, coarse, cbase):
        sweep(fine, rhs, v.at[0], None)
        zghost(fine, v.at[0])
        residual_pass(fine, v.at[0], rhs)
        descend()
        prolong_add(fine, coarse, ecoarse, v.at[0], cbase)
        loop(PAIR, lambda i: sweep(fine, v.at[i], v.at[1 - i], rhs))

    def descend4():
        restrict_to(levels[4], levels[5], b5)
        coarse_solve()

    def descend3():
        restrict_to(levels[3], levels[4], b4)
        zghost(levels[4], b4)
        local_visit(levels[4], v4, b4, descend4, e5, levels[5], base_of(levels[5]))

    def descend2():
        restrict_packed(levels[PAIR], me)
        gather3()
        local_visit(levels[3], v3, b3, descend3, v4.at[0], levels[4], base_of(levels[4]))

    def descend1():
        restrict_to(levels[1], levels[PAIR], b2, p2s)
        exchange_wide(levels[PAIR], b2, p2s, p2r, h2s, h2r)
        oz, oy, ox = base_of(levels[3])
        local_visit(levels[PAIR], v2, b2, descend2, v3.at[0], levels[3], (oz + GRP * pz, oy + GRP * py, ox + GRP * px))

    def skew_in(t):
        o = order(t)
        for copy in load(o):
            copy.wait()
        rows, frows = pl.ds(tile(o + 1), SUB), pl.ds(tile(o), SUB)
        pk = nil
        for z in range(LN):
            moved = pltpu.roll(ua[z + 1, rows, :], z, 1)
            ua[z + 1, rows, :] = moved
            pk = jnp.where(face_lane == z, moved, pk)
            fr[z, frows, :] = pltpu.roll(fr[z, frows, :] * INV_G2, z, 1)
        xs[0, frows, :] = pk
        send(ua, 0, t)
    loop(GRP, skew_in)
    for copy in load_c:
        copy.wait()

    def correct():
        residual0()
        restrict_to(lev0, levels[1], b1, p1s)
        exchange_wide(levels[1], b1, p1s, p1r, h1s, h1r)
        local_visit(levels[1], v1, b1, descend1, v2.at[0], levels[PAIR], base_of(levels[PAIR]))
        prolong_add(lev0, levels[1], v1.at[0], ua, base_of(levels[1]))

    def half_cycle(h):
        sweep0(ua, ub, 0)
        sweep0(ub, ua, 1)
        pl.when(h % PAIR == 0)(correct)
    loop(PAIR * CYCLES, half_cycle)
    loop(GRP, lambda t: receive(ua, 0, t))

    def store(t):
        return pltpu.make_async_copy(ub.at[pl.ds(1, LN), pl.ds(tile(t + 1), SUB), :], out_hbm.at[:, pl.ds(tile(t), SUB), :],
                                     lsem.at[t])

    def skew_out(t):
        rows = pl.ds(tile(t + 1), SUB)
        for z in range(LN):
            ub[z + 1, rows, :] = pltpu.roll(ua[z + 1, rows, :], -z % LN, 1)
        store(t).start()
    loop(GRP, skew_out)
    loop(GRP, lambda t: store(t).wait())


def solution(mesh):
    grid_spec = P(('batch', 'gz'), 'gy', 'gx')

    def vmem(*shape):
        return pltpu.VMEM(shape, F32)

    scratch = [vmem(130, 144, LN), vmem(130, 144, LN), vmem(LN, LN, LN), vmem(66, 144, LN), vmem(66, 80, LN), vmem(LN, SUB, LN), vmem(LN, SUB, LN)]
    for shape in ((82, 96), (50, 64), (34, 72), (18, 48)):
        scratch += [vmem(PAIR, *shape, LN), vmem(*shape, LN)]
    scratch += [vmem(10, 32, LN), vmem(10, 32, LN), vmem(4, 512, LN)]
    scratch += [vmem(PAIR, LN, LN)] * 4
    scratch += [vmem(4, 64, LN)] * PAIR + [vmem(PAIR, 32, LN)] * PAIR
    scratch += [vmem(13, SUB, LN)] * PAIR + [vmem(7, SUB, LN)] * PAIR + [vmem(SUB, PAIR, GRP, LN)]
    scratch += [pltpu.SemaphoreType.DMA((22,)), pltpu.SemaphoreType.DMA((22,))]
    scratch += [pltpu.SemaphoreType.DMA((PAIR, GRP))] * 6 + [pltpu.SemaphoreType.DMA((36,))]

    call = pl.pallas_call(
        solve_kernel,
        out_shape=jax.ShapeDtypeStruct((LN, LN, LN), F32),
        in_specs=[pl.BlockSpec(memory_space=pl.ANY)] * 3,
        out_specs=pl.BlockSpec(memory_space=pl.ANY),
        scratch_shapes=scratch,
        name='multigrid',
        compiler_params=pltpu.CompilerParams(collective_id=0, has_side_effects=True, vmem_limit_bytes=67043328),
    )
    return jax.shard_map(call, mesh=mesh, in_specs=(grid_spec, grid_spec, P()), out_specs=grid_spec, check_vma=False)
```

```python
import jax
import jax.numpy as jnp
from jax import lax
from jax.experimental import pallas as pl
from jax.experimental.pallas import tpu as pltpu
from jax.sharding import PartitionSpec as P

OMEGA = 2.0 / 3.0
C6 = OMEGA / 6.0
CYCLES = 2
MESH = pl.DeviceIdType.MESH
F32 = jnp.float32
PAIR, SUB, GRP, LN = 2, 8, 16, 128
HALO_PLANES = {1: 4, 2: 5}
BACK = LN - 1
INV_G2 = 1.0 / 65536.0


class Level:
    def __init__(self, idx, n, off, shape, pos, split):
        self.idx, self.n, self.shape = idx, n, shape
        self.oz, self.oy, self.ox = off
        self.split = split
        if split:
            self.lo = tuple(o - p * n for o, p in zip(off, pos))
            self.hi = tuple(l + PAIR * n for l in self.lo)
        else:
            self.lo = off
            self.hi = tuple(o + n for o in off)
        wide = SUB if (split and idx > 0) else 0
        self.zs = self.oz - wide * pos[0] if wide else self.oz
        self.ys = self.oy - wide * pos[1] if wide else self.oy
        self.nzb = (n + wide) // SUB
        self.nyt = (n + wide) // SUB
        if split:
            self.ghosts = [(jnp.where(pos[0] == 0, self.oz - 1, self.oz + n), jnp.where(pos[0] == 0, self.oz, self.oz + n - 1))]
        else:
            self.ghosts = [(self.oz - 1, self.oz), (self.oz + n, self.oz + n - 1)]


def solve_kernel(f_hbm, u_hbm, c_hbm, out_hbm,
                 ua, ub, fr, tr, xr, sx, sy, v1, w1, b1, v2, w2, b2, v3, w3, b3, v4, w4, b4, e5, b5, cinv,
                 xs, xg, yp, yg, p1s, p1r, p2s, p2r, h1s, h1r, h2s, h2r, g3, ssem, rsem, xss, xrs, zss, zrs, wss, wrs, lsem):
    pz, py, px = lax.axis_index('gz'), lax.axis_index('gy'), lax.axis_index('gx')
    pos = (pz, py, px)
    lane = lax.broadcasted_iota(jnp.int32, (SUB, LN), 1)
    row = lax.broadcasted_iota(jnp.int32, (SUB, LN), 0)
    nil = jnp.zeros((SUB, LN), F32)
    levels = [
        Level(0, LN, (1, SUB, 0), (130, 144), pos, True),
        Level(1, 64, (9, GRP, 32), (82, 96), pos, True),
        Level(PAIR, 32, (9, GRP, 48), (50, 64), pos, True),
        Level(3, 32, (1, GRP, 48), (34, 72), pos, False),
        Level(4, GRP, (1, GRP, 48), (18, 48), pos, False),
        Level(5, SUB, (1, GRP, 48), (10, 32), pos, False),
    ]
    lev0 = levels[0]
    low_x = px == 0
    face_lane = jnp.where(low_x, (lane + 1) & BACK, lane)
    out_lane = jnp.where(low_x, lane, (lane + 1) & BACK)

    skew = (lax.broadcasted_iota(jnp.int32, (SUB, SUB, LN), PAIR) - lax.broadcasted_iota(jnp.int32, (SUB, SUB, LN), 0)) & BACK
    out_skew = jnp.where(low_x, skew, (skew + 1) & BACK)

    def dev(code):
        ids = {}
        if code & 4:
            ids['gz'] = 1 - pz
        if code & PAIR:
            ids['gy'] = 1 - py
        if code & 1:
            ids['gx'] = 1 - px
        return ids

    def remote(src, dst, k, code):
        return pltpu.make_async_remote_copy(src_ref=src, dst_ref=dst, send_sem=ssem.at[k], recv_sem=rsem.at[k],
                                            device_id=dev(code), device_id_type=MESH)

    def loop(n, body):
        lax.fori_loop(0, n, lambda i, c: (body(i), c)[1], 0)

    def tile(i):
        return pl.multiple_of(SUB * i, SUB)

    def load(t):
        rows = pl.ds(tile(t), SUB)
        return (pltpu.make_async_copy(u_hbm.at[:, rows, :], ua.at[pl.ds(1, LN), pl.ds(tile(t + 1), SUB), :], lsem.at[t]),
                pltpu.make_async_copy(f_hbm.at[:, rows, :], fr.at[:, rows, :], lsem.at[GRP + t]))

    def start_load(t):
        for copy in load(t):
            copy.start()
    loop(GRP, lambda t: start_load(jnp.where(py == 0, 15 - t, t)))
    load_c = [pltpu.make_async_copy(c_hbm.at[:, pl.ds(LN * j, LN)], cinv.at[j], lsem.at[32 + j]) for j in range(4)]
    for copy in load_c:
        copy.start()

    def zero(ref):
        def body(i):
            ref[i] = jnp.zeros(ref.shape[1:], F32)
        loop(ref.shape[0], body)

    for ref in (v1, w1, b1, v2, w2, b2, v3, w3, b3, v4, w4, b4, e5):
        zero(ref)

    def zero_rows(i):
        for buf in (ua, ub):
            buf[i, pl.ds(0, SUB), :] = nil
            buf[i, pl.ds(136, SUB), :] = nil
    loop(130, zero_rows)
    zout = jnp.where(pz == 0, 0, 129)

    def zero_plane(t):
        for buf in (ua, ub):
            buf[zout, pl.ds(tile(t), SUB), :] = nil
    loop(18, zero_plane)

    barrier = pltpu.get_barrier_semaphore()
    for code in range(1, SUB):
        pl.semaphore_signal(barrier, inc=1, device_id=dev(code), device_id_type=MESH)
    pl.semaphore_wait(barrier, 7)

    def coefs(lev, y0):
        r = row + y0
        inside = (r >= lev.lo[1]) & (r < lev.hi[1]) & (lane >= lev.lo[PAIR]) & (lane < lev.hi[PAIR])
        one = jnp.ones((SUB, LN), F32)
        nb = (jnp.where(r == lev.lo[1], one, nil) + jnp.where(r == lev.hi[1] - 1, one, nil)
              + jnp.where(lane == lev.lo[PAIR], one, nil) + jnp.where(lane == lev.hi[PAIR] - 1, one, nil))
        return inside, nb

    def zghost_tile(lev, ref, y0):
        for ghost, face in lev.ghosts:
            ref[ghost, pl.ds(y0, SUB), :] = -ref[face, pl.ds(y0, SUB), :]

    def zghost(lev, ref):
        loop(lev.shape[1] // SUB, lambda t: zghost_tile(lev, ref, tile(t)))

    def several(count, per, body):
        def step(i):
            for k in range(per):
                body(i * per + k)
        loop(count // per, step)

    def roll_sums(src, zs, nzb, y0, sx):
        for k in range(nzb):
            c = src[pl.ds(zs + SUB * k, SUB), pl.ds(y0, SUB), :]
            sx[pl.ds(SUB * k, SUB)] = pltpu.roll(c, 1, PAIR) + pltpu.roll(c, BACK, PAIR)

    def stencil(src, zs, k, y0, sx):
        z0 = zs + SUB * k
        v = src[pl.ds(z0 - 1, SUB + PAIR), pl.ds(y0, SUB), :]
        s = v[0:SUB] + v[PAIR:SUB + PAIR]
        s = s + src[pl.ds(z0, SUB), pl.ds(y0 - 1, SUB), :] + src[pl.ds(z0, SUB), pl.ds(y0 + 1, SUB), :]
        return v[1:SUB + 1], s + sx[pl.ds(SUB * k, SUB)]

    def tiles(lev, src, span, count, body):
        ys, zs, nzb = span

        def at(t):
            return pl.multiple_of(ys + SUB * t, SUB)
        if lev.idx != 1:
            def alone(t):
                roll_sums(src, zs, nzb, at(t), sx)
                body(at(t), lambda block: several(nzb, PAIR if nzb == 4 else 1, block), sx)
            loop(count, alone)
            return
        roll_sums(src, zs, nzb, at(0), sx)

        def step(t):
            def both(now, later):
                roll_sums(src, zs, nzb, at(t + 1 - (t + 1) // count), later)
                body(at(t), lambda block: [block(k) for k in range(nzb)], now)
            pl.when(t % PAIR == 0)(lambda: both(sx, sy))
            pl.when(t % PAIR == 1)(lambda: both(sy, sx))
        loop(count, step)

    def sweep(lev, src, dst, rhs):
        first = rhs is None

        def body(y0, each, sums):
            inside, nb = coefs(lev, y0)
            cc = (1.0 - OMEGA) - C6 * nb
            if first:
                ca, cb = jnp.where(inside, C6 * (cc + 1.0), 0.0), jnp.where(inside, C6 * C6, 0.0)
            else:
                ca, cb = jnp.where(inside, cc, 0.0), jnp.where(inside, C6, 0.0)

            def block(k):
                c, s = stencil(src, lev.zs, k, y0, sums)
                z0 = lev.zs + SUB * k
                if not first:
                    s = s + rhs[pl.ds(z0, SUB), pl.ds(y0, SUB), :]
                dst[pl.ds(z0, SUB), pl.ds(y0, SUB), :] = ca * c + cb * s
            each(block)
            zghost_tile(lev, dst, y0)
        tiles(lev, src, (lev.ys, lev.zs, lev.nzb), lev.nyt, body)

    def residual_pass(lev, src, rhs):
        def body(y0, each, sums):
            _, nb = coefs(lev, y0)
            dd = 6.0 + nb

            def block(k):
                c, s = stencil(src, lev.oz, k, y0, sums)
                r = (rhs[pl.ds(lev.oz + SUB * k, SUB), pl.ds(y0, SUB), :] + (s - dd * c)).reshape(4, PAIR, SUB, LN)
                tr[pl.ds(4 * k, 4), pl.ds(pl.multiple_of(y0 - lev.oy, SUB), SUB), :] = r[:, 0] + r[:, 1]
            each(block)
        tiles(lev, src, (lev.oy, lev.oz, lev.n // SUB), lev.n // SUB, body)

    zface = jnp.where(pz == 0, LN, 1)
    zdst = LN + 1 - zface + jnp.where(pz == 0, -1, 1)
    yface = jnp.where(py == 0, 135, SUB)
    yghost = jnp.where(py == 0, 136, 7)

    def order(t):
        return jnp.where(py == 0, 15 - t, t)

    def pieces(buf, par, o):
        rows, yrows = pl.ds(tile(o), SUB), pl.ds(tile(o + 1), SUB)
        return (pltpu.make_async_remote_copy(src_ref=xs.at[par, rows, :], dst_ref=xg.at[par, rows, :], send_sem=xss.at[par, o],
                                             recv_sem=xrs.at[par, o], device_id=dev(1), device_id_type=MESH),
                pltpu.make_async_remote_copy(src_ref=buf.at[zface, yrows, :], dst_ref=buf.at[zdst, yrows, :],
                                             send_sem=zss.at[par, o], recv_sem=zrs.at[par, o], device_id=dev(4),
                                             device_id_type=MESH))

    def face_rows(par):
        return remote(yp.at[par], yg.at[par], par, PAIR)

    def send(buf, par, t):
        for copy in pieces(buf, par, order(t)):
            copy.start()

        def first():
            def take_rows(i):
                for j in range(SUB):
                    yp[par, pl.ds(SUB * i + j, 1), :] = buf[SUB * i + j + 1, pl.ds(yface, 1), :]
            loop(GRP, take_rows)
            face_rows(par).start()
        pl.when(t == 0)(first)

    def receive(buf, par, t):
        def first():
            face_rows(par).wait()

            def put_rows(i):
                for j in range(SUB):
                    buf[SUB * i + j + 1, pl.ds(yghost, 1), :] = yg[par, pl.ds(SUB * i + j, 1), :]
            loop(GRP, put_rows)
        pl.when(t == 0)(first)
        for copy in pieces(buf, par, order(t)):
            copy.wait()

    def roll_sums0(src, par, t, sx):
        rows = pl.ds(tile(t + 1), SUB)
        ghost = xg[par, pl.ds(tile(t), SUB), :]
        left = jnp.where(low_x, 0.0, ghost)
        right = jnp.where(low_x, ghost, 0.0)
        zlow = jnp.where(pz == 0, 1.0, 0.0)
        for k in range(GRP):
            z = SUB * k
            v = src[pl.ds(z, SUB + PAIR), rows, :]
            here = v[1:SUB + 1]
            a = jnp.where(skew == (z - 1) % LN, left[None], here) + v[0:SUB]
            b = jnp.where(skew == z, right[None], here) + v[PAIR:SUB + PAIR]
            s = pltpu.roll(a, 1, PAIR) + pltpu.roll(b, BACK, PAIR) - jnp.where(out_skew == z, here, 0.0)
            sx[pl.ds(z, SUB)] = s
        sx[0] = sx[0] - zlow * src[1, rows, :]
        sx[BACK] = sx[BACK] - (1.0 - zlow) * src[LN, rows, :]

    def cells0(src, t, z, sx):
        y0, planes = tile(t + 1), pl.ds(z + 1, GRP)
        s = sx[pl.ds(z, GRP)] + src[planes, pl.ds(y0 - 1, SUB), :] + src[planes, pl.ds(y0 + 1, SUB), :]
        return src[planes, pl.ds(y0, SUB), :], s + fr[pl.ds(z, GRP), pl.ds(tile(t), SUB), :]

    def yedge(t):
        r = row + tile(t + 1)
        return jnp.where((r == lev0.lo[1]) | (r == lev0.hi[1] - 1), 1.0, 0.0)

    def tiles0(src, par, work):
        receive(src, par, 0)
        roll_sums0(src, par, order(0), sx)

        def step(t):
            pl.when(t < 15)(lambda: receive(src, par, t + 1))

            def both(now, later):
                roll_sums0(src, par, order(t + 1 - (t + 1) // GRP), later)
                work(order(t), now)
            pl.when(t % PAIR == 0)(lambda: both(sx, sy))
            pl.when(t % PAIR == 1)(lambda: both(sy, sx))
            work_done(t)

        work_done = work.done
        loop(GRP, step)

    def sweep0(src, dst, par):
        def work(o, sums):
            cc = (1.0 - OMEGA) - C6 * yedge(o)
            pk = nil
            for k in range(SUB):
                c, s = cells0(src, o, GRP * k, sums)
                new = cc * c + C6 * s
                dst[pl.ds(GRP * k + 1, GRP), pl.ds(tile(o + 1), SUB), :] = new
                for j in range(GRP):
                    pk = jnp.where(face_lane == GRP * k + j, new[j], pk)
            xs[1 - par, pl.ds(tile(o), SUB), :] = pk
        work.done = lambda t: send(dst, 1 - par, t)
        tiles0(src, par, work)

    def residual0():
        def work(o, sums):
            dd = 6.0 + yedge(o)
            for k in range(SUB):
                c, s = cells0(ua, o, GRP * k, sums)
                ub[pl.ds(GRP * k + 1, GRP), pl.ds(tile(o + 1), SUB), :] = s - dd * c
        work.done = lambda t: None
        tiles0(ua, 0, work)

    def pair_sums(fine, j):
        for zc in range(fine.n // PAIR):
            lo, hi = pl.ds(GRP * j, SUB, stride=PAIR), pl.ds(GRP * j + 1, SUB, stride=PAIR)
            if fine.idx:
                s = tr[zc, lo, :] + tr[zc, hi, :]
                sx[zc] = 0.5 * (s + pltpu.roll(s, BACK, 1))
                continue
            lo, hi = pl.ds(GRP * j + SUB, SUB, stride=PAIR), pl.ds(GRP * j + SUB + 1, SUB, stride=PAIR)
            e = ub[PAIR * zc + 1, lo, :] + ub[PAIR * zc + 1, hi, :]
            o = ub[PAIR * zc + PAIR, lo, :] + ub[PAIR * zc + PAIR, hi, :]
            s = pltpu.roll(e, -PAIR * zc % LN, 1) + pltpu.roll(e + o, (-PAIR * zc - 1) % LN, 1)
            sx[zc] = 0.5 * (s + pltpu.roll(o, (-PAIR * zc - PAIR) % LN, 1))

    def restrict_to(fine, coarse, dst, pack=None):
        half = fine.n // PAIR
        own = (lane >= coarse.ox) & (lane < coarse.ox + half)
        idx = (fine.ox + PAIR * (lane - coarse.ox)) & BACK
        pidx = fine.ox + PAIR * (jnp.where(low_x, half - SUB, 0) + lane % SUB)
        group = lane // SUB
        step = half // PAIR

        def ytile(t):
            j = t if pack is None else jnp.where(py == 0, half // SUB - 1 - t, t)
            rows = pl.ds(pl.multiple_of(coarse.oy + SUB * j, SUB), SUB)
            pair_sums(fine, j)

            def move(q):
                pk = nil
                for i in range(step):
                    z = step * q + i
                    v = sx[z]
                    dst[coarse.oz + z, rows, :] = jnp.where(own, jnp.take_along_axis(v, idx, axis=1), 0.0)
                    if pack is not None:
                        pk = jnp.where(group == i % GRP, jnp.take_along_axis(v, pidx, axis=1), pk)
                        if i % GRP == GRP - 1:
                            pack[q * (step // GRP) + i // GRP, pl.ds(tile(j), SUB), :] = pk
            loop(PAIR, move)
            if pack is not None:
                copies = edge_pieces(coarse, dst, j)
                copies[0].start()

                def start_rest():
                    for copy in copies[1:]:
                        copy.start()
                pl.when(t == 0)(start_rest)
        loop(half // SUB, ytile)

    def wide_spans(lev):
        n, h = lev.n, HALO_PLANES[lev.idx]
        fy = pl.multiple_of(jnp.where(py == 0, lev.oy + n - SUB, lev.oy), SUB)
        hy = pl.multiple_of(jnp.where(py == 0, lev.oy - SUB, lev.oy + n), SUB)
        fz = jnp.where(pz == 0, lev.oz + n - h, lev.oz)
        hz = jnp.where(pz == 0, lev.oz - h, lev.oz + n)
        return fy, hy, pl.ds(fz, h), pl.ds(hz, h)

    def edge_pieces(lev, ref, j):
        fy, hy, fz, hz = wide_spans(lev)
        rows, own, k = pl.ds(pl.multiple_of(lev.oy + SUB * j, SUB), SUB), pl.ds(lev.oz, lev.n), lev.idx
        piece = pltpu.make_async_remote_copy(src_ref=ref.at[fz, rows, :], dst_ref=ref.at[hz, rows, :],
                                             send_sem=wss.at[k - 1, j], recv_sem=wrs.at[k - 1, j], device_id=dev(4),
                                             device_id_type=MESH)
        return (piece, remote(ref.at[own, pl.ds(fy, SUB), :], ref.at[own, pl.ds(hy, SUB), :], 4 * k + 3, PAIR),
                remote(ref.at[fz, pl.ds(fy, SUB), :], ref.at[hz, pl.ds(hy, SUB), :], 4 * k + 4, 6))

    def restrict_packed(fine, me):
        idx = fine.ox + PAIR * (lane % GRP)
        group = lane // GRP

        def ytile(j):
            pair_sums(fine, j)

            def collect(q):
                pk = nil
                for i in range(SUB):
                    pk = jnp.where(group == i, jnp.take_along_axis(sx[SUB * q + i], idx, axis=1), pk)
                g3[me, q, pl.ds(tile(j), SUB), :] = pk
            loop(PAIR, collect)
        loop(PAIR, ytile)

    def prolong_add(fine, coarse, esrc, dst, cbase):
        back_z = (fine.oz - fine.zs) // PAIR
        back_y = (fine.oy - fine.ys) // PAIR
        nct = fine.n // GRP + (0 if fine.nyt * SUB == fine.n else 1)
        cy_s = cbase[1] - PAIR * back_y
        fy_s = fine.oy - 4 * back_y
        cz_s = cbase[0] - back_z - 1
        ncz = 4 * fine.nzb + PAIR
        xf = lane - fine.ox
        half = lax.shift_right_arithmetic(xf, 1)
        odd = xf - PAIR * half
        i0 = half + cbase[PAIR]
        i1 = jnp.clip(i0 + PAIR * odd - 1, 0, BACK)
        i0 = jnp.clip(i0, 0, BACK)
        inx = (lane >= fine.lo[PAIR]) & (lane < fine.hi[PAIR])
        edge = (lane == fine.lo[PAIR]) | (lane == fine.hi[PAIR] - 1)
        wx = jnp.where(inx, jnp.where(edge, 0.5, 0.75), 0.0)
        wn = jnp.where(inx, 0.25, 0.0)

        def spread(z):
            for t in range(nct + PAIR):
                v = esrc[cz_s + z, pl.ds(pl.multiple_of(cy_s + SUB * (t - 1), SUB), SUB), :]
                xr[z, pl.ds(SUB * t, SUB), :] = (wx * jnp.take_along_axis(v, i0, axis=1)
                                                 + wn * jnp.take_along_axis(v, i1, axis=1))

        per = 6 if ncz % 6 == 0 else PAIR

        def spread_some(i):
            for q in range(per):
                spread(per * i + q)
        loop(ncz // per, spread_some)

        def ctile(t):
            fy = pl.multiple_of(fy_s + GRP * t, SUB)
            r = row + (cy_s + SUB * t)
            iny = (r >= coarse.lo[1]) & (r < coarse.hi[1])
            wny = jnp.where(iny, 0.25, 0.0)
            wde = jnp.where(iny, jnp.where(r == coarse.lo[1], 0.5, 0.75), 0.0)
            wdo = jnp.where(iny, jnp.where(r == coarse.hi[1] - 1, 0.5, 0.75), 0.0)

            def plane(i):
                for q in range(per):
                    z = per * i + q
                    e = xr[z, pl.ds(tile(t + 1), SUB), :]
                    tr[z, pl.ds(fy, SUB, stride=PAIR), :] = wde * e + wny * xr[z, pl.ds(tile(t + 1) - 1, SUB), :]
                    tr[z, pl.ds(fy + 1, SUB, stride=PAIR), :] = wdo * e + wny * xr[z, pl.ds(tile(t + 1) + 1, SUB), :]
            loop(ncz // per, plane)
        loop(nct, ctile)

        def ytile(t):
            o = t if fine.idx else order(t)
            y0 = pl.multiple_of(fine.ys + SUB * o, SUB)
            rows = pl.ds(y0, SUB)
            pk = nil
            for k in range(fine.nzb):
                z0 = fine.zs + SUB * k
                tb = tr[pl.ds(4 * k, 6), rows, :]
                mid = 0.75 * tb[1:5]
                add = jnp.stack([mid + 0.25 * tb[0:4], mid + 0.25 * tb[PAIR:6]], axis=1).reshape(SUB, SUB, LN)
                if fine.idx:
                    dst[pl.ds(z0, SUB), rows, :] = dst[pl.ds(z0, SUB), rows, :] + add
                    continue
                for j in range(SUB):
                    z = SUB * k + j
                    new = dst[1 + z, rows, :] + pltpu.roll(add[j], z, 1)
                    dst[1 + z, rows, :] = new
                    pk = jnp.where(face_lane == z, new, pk)
            if fine.idx:
                zghost_tile(fine, dst, y0)
            else:
                xs[0, pl.ds(tile(o), SUB), :] = pk
                send(dst, 0, t)
        loop(fine.nyt, ytile)

    def exchange_wide(lev, ref, sendp, recvp, sendh, recvh):
        n, h, k = lev.n, HALO_PLANES[lev.idx], lev.idx
        hy = pl.multiple_of(jnp.where(py == 0, lev.oy + n, lev.oy - SUB), SUB)
        hz = jnp.where(pz == 0, lev.oz + n, lev.oz - h)
        cx = remote(sendp, recvp, 4 * k + 1, 1)
        cx.start()
        for copy in edge_pieces(lev, ref, 0)[1:]:
            copy.wait()
        loop(n // SUB, lambda j: edge_pieces(lev, ref, j)[0].wait())
        group = lane // SUB
        face = jnp.where(low_x, lev.ox + n - SUB, lev.ox)
        halo = jnp.where(low_x, lev.ox + n, lev.ox - SUB)
        inh = (lane >= halo) & (lane < halo + SUB)

        def spots(q):
            return pl.ds(pl.multiple_of(jnp.where(q < n // SUB, lev.oy + SUB * q, hy), SUB), SUB)

        def gather_faces(z, planes, rows):
            pk = nil
            for i in range(planes):
                pk = jnp.where(group == i, pltpu.roll(ref[z + i, rows, :], (SUB * i - face) & BACK, 1), pk)
            return pk
        nq = n // GRP

        def collect_y(q):
            sendh[q] = gather_faces(lev.oz + GRP * q, GRP, pl.ds(hy, SUB))

        def collect_z(q):
            sendh[nq + q] = gather_faces(hz, h, spots(q))
        zper = 3 if n // SUB == SUB else n // SUB + 1
        several(nq, PAIR, collect_y)
        several(n // SUB + 1, zper, collect_z)
        ch = remote(sendh, recvh, 4 * k + PAIR, 1)
        ch.start()
        cx.wait()

        def put(pk, z, planes, rows):
            pk = pltpu.roll(pk, halo, 1)
            for i in range(planes):
                ref[z + i, rows, :] = jnp.where(inh, pltpu.roll(pk, (-SUB * i) % LN, 1), ref[z + i, rows, :])

        def ytile(t):
            rows = pl.ds(pl.multiple_of(lev.oy + SUB * t, SUB), SUB)
            for q in range(nq):
                put(recvp[q, pl.ds(tile(t), SUB), :], lev.oz + GRP * q, GRP, rows)
        loop(n // SUB, ytile)
        ch.wait()

        several(nq, PAIR, lambda q: put(recvh[q], lev.oz + GRP * q, GRP, pl.ds(hy, SUB)))
        several(n // SUB + 1, zper, lambda q: put(recvh[nq + q], hz, h, spots(q)))
        zghost(lev, ref)

    me = 4 * pz + PAIR * py + px

    def gather3():
        copies = [remote(g3.at[me], g3.at[me], 13 + code, code) for code in range(1, SUB)]
        for c in copies:
            c.start()
        for c in copies:
            c.wait()
        lev = levels[3]
        in_lo = (lane >= lev.ox) & (lane < lev.ox + GRP)
        in_hi = (lane >= lev.ox + GRP) & (lane < lev.ox + 32)

        def ytile(t):
            rows = pl.ds(pl.multiple_of(lev.oy + SUB * t, SUB), SUB)
            by = t // PAIR
            r0 = pl.ds(tile(t % PAIR), SUB)
            for q in range(4):
                lo = g3[4 * (q // PAIR) + PAIR * by, q % PAIR, r0, :]
                hi = g3[4 * (q // PAIR) + PAIR * by + 1, q % PAIR, r0, :]
                for i in range(SUB):
                    a = pltpu.roll(lo, (lev.ox - GRP * i) % LN, 1)
                    b = pltpu.roll(hi, (lev.ox + GRP - GRP * i) % LN, 1)
                    b3[lev.oz + SUB * q + i, rows, :] = jnp.where(in_lo, a, jnp.where(in_hi, b, 0.0))
        loop(4, ytile)
        zghost(lev, b3)

    def coarse_solve():
        lev = levels[5]

        def zstep(z, acc):
            b = b5[lev.oz + z, pl.ds(lev.oy, SUB), :] * 64.0
            acc = list(acc)
            for x in range(SUB):
                col = jnp.broadcast_to(b[:, lev.ox + x:lev.ox + x + 1], (SUB, LN))
                for j in range(4):
                    acc[j] = acc[j] + cinv[j, pl.ds(z * 64 + x, SUB, stride=SUB), :] * col
            return tuple(acc)
        acc = lax.fori_loop(0, SUB, zstep, (jnp.zeros((SUB, LN), F32),) * 4)
        lines = [jnp.broadcast_to(jnp.sum(a, axis=0, keepdims=True), (SUB, LN)) for a in acc]
        own = (lane >= lev.ox) & (lane < lev.ox + SUB)
        for z in range(SUB):
            idx = jnp.clip((z % PAIR) * 64 + row * SUB + lane - lev.ox, 0, 127)
            e5[lev.oz + z, pl.ds(lev.oy, SUB), :] = jnp.where(own, jnp.take_along_axis(lines[z // PAIR], idx, axis=1), 0.0)
        zghost(lev, e5)

    def base_of(lev):
        return (lev.oz, lev.oy, lev.ox)

    def local_visit(fine, v, w, rhs, descend, ecoarse, coarse, cbase):
        sweep(fine, rhs, v, None)
        zghost(fine, v)
        residual_pass(fine, v, rhs)
        descend()
        prolong_add(fine, coarse, ecoarse, v, cbase)
        sweep(fine, v, w, rhs)
        sweep(fine, w, v, rhs)

    def descend4():
        restrict_to(levels[4], levels[5], b5)
        coarse_solve()

    def descend3():
        restrict_to(levels[3], levels[4], b4)
        zghost(levels[4], b4)
        local_visit(levels[4], v4, w4, b4, descend4, e5, levels[5], base_of(levels[5]))

    def descend2():
        restrict_packed(levels[PAIR], me)
        gather3()
        local_visit(levels[3], v3, w3, b3, descend3, v4, levels[4], base_of(levels[4]))

    def descend1():
        restrict_to(levels[1], levels[PAIR], b2, p2s)
        exchange_wide(levels[PAIR], b2, p2s, p2r, h2s, h2r)
        oz, oy, ox = base_of(levels[3])
        local_visit(levels[PAIR], v2, w2, b2, descend2, v3, levels[3], (oz + GRP * pz, oy + GRP * py, ox + GRP * px))

    def skew_in(t):
        o = order(t)
        for copy in load(o):
            copy.wait()
        rows, frows = pl.ds(tile(o + 1), SUB), pl.ds(tile(o), SUB)
        pk = nil
        for z in range(LN):
            moved = pltpu.roll(ua[z + 1, rows, :], z, 1)
            ua[z + 1, rows, :] = moved
            pk = jnp.where(face_lane == z, moved, pk)
            fr[z, frows, :] = pltpu.roll(fr[z, frows, :] * INV_G2, z, 1)
        xs[0, frows, :] = pk
        send(ua, 0, t)
    loop(GRP, skew_in)
    for copy in load_c:
        copy.wait()

    def correct():
        residual0()
        restrict_to(lev0, levels[1], b1, p1s)
        exchange_wide(levels[1], b1, p1s, p1r, h1s, h1r)
        local_visit(levels[1], v1, w1, b1, descend1, v2, levels[PAIR], base_of(levels[PAIR]))
        prolong_add(lev0, levels[1], v1, ua, base_of(levels[1]))

    def half_cycle(h):
        sweep0(ua, ub, 0)
        sweep0(ub, ua, 1)
        pl.when(h % PAIR == 0)(correct)
    loop(PAIR * CYCLES, half_cycle)

    def store(t):
        return pltpu.make_async_copy(ub.at[pl.ds(1, LN), pl.ds(tile(t + 1), SUB), :], out_hbm.at[:, pl.ds(tile(t), SUB), :],
                                     lsem.at[t])

    def skew_out(t):
        rows = pl.ds(tile(t + 1), SUB)
        for z in range(LN):
            ub[z + 1, rows, :] = pltpu.roll(ua[z + 1, rows, :], -z % LN, 1)
        store(t).start()
    loop(GRP, skew_out)
    loop(GRP, lambda t: receive(ua, 0, t))
    loop(GRP, lambda t: store(t).wait())


def solution(mesh):
    grid_spec = P(('batch', 'gz'), 'gy', 'gx')

    def vmem(*shape):
        return pltpu.VMEM(shape, F32)

    scratch = [vmem(130, 144, LN), vmem(130, 144, LN), vmem(LN, LN, LN), vmem(66, 144, LN), vmem(66, 80, LN), vmem(LN, SUB, LN), vmem(LN, SUB, LN)]
    for shape in ((82, 96), (50, 64), (34, 72), (18, 48)):
        scratch += [vmem(*shape, LN)] * 3
    scratch += [vmem(10, 32, LN), vmem(10, 32, LN), vmem(4, 512, LN)]
    scratch += [vmem(PAIR, LN, LN)] * 4
    scratch += [vmem(4, 64, LN)] * PAIR + [vmem(PAIR, 32, LN)] * PAIR
    scratch += [vmem(13, SUB, LN)] * PAIR + [vmem(7, SUB, LN)] * PAIR + [vmem(SUB, PAIR, GRP, LN)]
    scratch += [pltpu.SemaphoreType.DMA((22,)), pltpu.SemaphoreType.DMA((22,))]
    scratch += [pltpu.SemaphoreType.DMA((PAIR, GRP))] * 6 + [pltpu.SemaphoreType.DMA((36,))]

    call = pl.pallas_call(
        solve_kernel,
        out_shape=jax.ShapeDtypeStruct((LN, LN, LN), F32),
        in_specs=[pl.BlockSpec(memory_space=pl.ANY)] * 3,
        out_specs=pl.BlockSpec(memory_space=pl.ANY),
        scratch_shapes=scratch,
        name='multigrid',
        compiler_params=pltpu.CompilerParams(collective_id=0, has_side_effects=True, vmem_limit_bytes=67043328),
    )
    return jax.shard_map(call, mesh=mesh, in_specs=(grid_spec, grid_spec, P()), out_specs=grid_spec, check_vma=False)
```

```python
import jax
import jax.numpy as jnp
from jax import lax
from jax.experimental import pallas as pl
from jax.experimental.pallas import tpu as pltpu
from jax.sharding import PartitionSpec as P

OMEGA = 2.0 / 3.0
C6 = OMEGA / 6.0
CYCLES = 2
MESH = pl.DeviceIdType.MESH
F32 = jnp.float32
PAIR, SUB, GRP, LN = 2, 8, 16, 128
HALO_PLANES = {1: 4, 2: 5}
BACK = LN - 1
INV_G2 = 1.0 / 65536.0


class Level:
    def __init__(self, idx, n, off, shape, pos, split):
        self.idx, self.n, self.shape = idx, n, shape
        self.oz, self.oy, self.ox = off
        self.split = split
        if split:
            self.lo = tuple(o - p * n for o, p in zip(off, pos))
            self.hi = tuple(l + PAIR * n for l in self.lo)
        else:
            self.lo = off
            self.hi = tuple(o + n for o in off)
        wide = SUB if (split and idx > 0) else 0
        self.zs = self.oz - wide * pos[0] if wide else self.oz
        self.ys = self.oy - wide * pos[1] if wide else self.oy
        self.nzb = (n + wide) // SUB
        self.nyt = (n + wide) // SUB
        if split:
            self.ghosts = [(jnp.where(pos[0] == 0, self.oz - 1, self.oz + n), jnp.where(pos[0] == 0, self.oz, self.oz + n - 1))]
        else:
            self.ghosts = [(self.oz - 1, self.oz), (self.oz + n, self.oz + n - 1)]


def solve_kernel(f_hbm, u_hbm, c_hbm, out_hbm,
                 ua, ub, fr, tr, xr, sx, sy, v1, w1, b1, v2, w2, b2, v3, w3, b3, v4, w4, b4, e5, b5, cinv,
                 xs, xg, yp, yg, p1s, p1r, p2s, p2r, h1s, h1r, h2s, h2r, g3, ssem, rsem, xss, xrs, zss, zrs, wss, wrs, lsem):
    pz, py, px = lax.axis_index('gz'), lax.axis_index('gy'), lax.axis_index('gx')
    pos = (pz, py, px)
    lane = lax.broadcasted_iota(jnp.int32, (SUB, LN), 1)
    row = lax.broadcasted_iota(jnp.int32, (SUB, LN), 0)
    nil = jnp.zeros((SUB, LN), F32)
    levels = [
        Level(0, LN, (1, SUB, 0), (130, 144), pos, True),
        Level(1, 64, (9, GRP, 32), (82, 96), pos, True),
        Level(PAIR, 32, (9, GRP, 48), (50, 64), pos, True),
        Level(3, 32, (1, GRP, 48), (34, 72), pos, False),
        Level(4, GRP, (1, GRP, 48), (18, 48), pos, False),
        Level(5, SUB, (1, GRP, 48), (10, 32), pos, False),
    ]
    lev0 = levels[0]
    low_x = px == 0
    face_lane = jnp.where(low_x, (lane + 1) & BACK, lane)
    out_lane = jnp.where(low_x, lane, (lane + 1) & BACK)

    skew = (lax.broadcasted_iota(jnp.int32, (SUB, SUB, LN), PAIR) - lax.broadcasted_iota(jnp.int32, (SUB, SUB, LN), 0)) & BACK
    out_skew = jnp.where(low_x, skew, (skew + 1) & BACK)

    def dev(code):
        ids = {}
        if code & 4:
            ids['gz'] = 1 - pz
        if code & PAIR:
            ids['gy'] = 1 - py
        if code & 1:
            ids['gx'] = 1 - px
        return ids

    def remote(src, dst, k, code):
        return pltpu.make_async_remote_copy(src_ref=src, dst_ref=dst, send_sem=ssem.at[k], recv_sem=rsem.at[k],
                                            device_id=dev(code), device_id_type=MESH)

    def loop(n, body):
        lax.fori_loop(0, n, lambda i, c: (body(i), c)[1], 0)

    def several(count, per, body):
        def step(i):
            for k in range(per):
                body(i * per + k)
        loop(count // per, step)

    def tile(i):
        return pl.multiple_of(SUB * i, SUB)

    def load(t):
        rows = pl.ds(tile(t), SUB)
        return (pltpu.make_async_copy(u_hbm.at[:, rows, :], ua.at[pl.ds(1, LN), pl.ds(tile(t + 1), SUB), :], lsem.at[t]),
                pltpu.make_async_copy(f_hbm.at[:, rows, :], fr.at[:, rows, :], lsem.at[GRP + t]))

    def start_load(t):
        for copy in load(t):
            copy.start()
    loop(GRP, lambda t: start_load(jnp.where(py == 0, 15 - t, t)))
    load_c = [pltpu.make_async_copy(c_hbm.at[:, pl.ds(LN * j, LN)], cinv.at[j], lsem.at[32 + j]) for j in range(4)]
    for copy in load_c:
        copy.start()

    def zero(ref):
        def body(i):
            ref[i] = jnp.zeros(ref.shape[1:], F32)
        several(ref.shape[0], PAIR, body)

    for ref in (v1, w1, b1, v2, w2, b2, v3, w3, b3, v4, w4, b4, e5):
        zero(ref)

    def zero_rows(i):
        for buf in (ua, ub):
            buf[i, pl.ds(0, SUB), :] = nil
            buf[i, pl.ds(136, SUB), :] = nil
    loop(130, zero_rows)
    zout = jnp.where(pz == 0, 0, 129)

    def zero_plane(t):
        for buf in (ua, ub):
            buf[zout, pl.ds(tile(t), SUB), :] = nil
    loop(18, zero_plane)

    barrier = pltpu.get_barrier_semaphore()
    for code in range(1, SUB):
        pl.semaphore_signal(barrier, inc=1, device_id=dev(code), device_id_type=MESH)
    pl.semaphore_wait(barrier, 7)

    def coefs(lev, y0):
        r = row + y0
        inside = (r >= lev.lo[1]) & (r < lev.hi[1]) & (lane >= lev.lo[PAIR]) & (lane < lev.hi[PAIR])
        one = jnp.ones((SUB, LN), F32)
        nb = (jnp.where(r == lev.lo[1], one, nil) + jnp.where(r == lev.hi[1] - 1, one, nil)
              + jnp.where(lane == lev.lo[PAIR], one, nil) + jnp.where(lane == lev.hi[PAIR] - 1, one, nil))
        return inside, nb

    def zghost_tile(lev, ref, y0):
        for ghost, face in lev.ghosts:
            ref[ghost, pl.ds(y0, SUB), :] = -ref[face, pl.ds(y0, SUB), :]

    def zghost(lev, ref):
        loop(lev.shape[1] // SUB, lambda t: zghost_tile(lev, ref, tile(t)))

    def roll_sums(src, zs, nzb, y0, sx):
        for k in range(nzb):
            c = src[pl.ds(zs + SUB * k, SUB), pl.ds(y0, SUB), :]
            sx[pl.ds(SUB * k, SUB)] = pltpu.roll(c, 1, PAIR) + pltpu.roll(c, BACK, PAIR)

    def stencil(src, zs, k, y0, sx):
        z0 = zs + SUB * k
        v = src[pl.ds(z0 - 1, SUB + PAIR), pl.ds(y0, SUB), :]
        s = v[0:SUB] + v[PAIR:SUB + PAIR]
        s = s + src[pl.ds(z0, SUB), pl.ds(y0 - 1, SUB), :] + src[pl.ds(z0, SUB), pl.ds(y0 + 1, SUB), :]
        return v[1:SUB + 1], s + sx[pl.ds(SUB * k, SUB)]

    def tiles(lev, src, span, count, body):
        ys, zs, nzb = span

        def at(t):
            return pl.multiple_of(ys + SUB * t, SUB)
        if lev.idx > PAIR:
            def alone(t):
                roll_sums(src, zs, nzb, at(t), sx)
                body(at(t), lambda block: several(nzb, PAIR if nzb == 4 else 1, block), sx)
            loop(count, alone)
            return
        roll_sums(src, zs, nzb, at(0), sx)

        def step(t):
            def both(now, later):
                roll_sums(src, zs, nzb, at(t + 1 - (t + 1) // count), later)
                body(at(t), lambda block: [block(k) for k in range(nzb)], now)
            pl.when(t % PAIR == 0)(lambda: both(sx, sy))
            pl.when(t % PAIR == 1)(lambda: both(sy, sx))
        loop(count, step)

    def sweep(lev, src, dst, rhs):
        first = rhs is None

        def body(y0, each, sums):
            inside, nb = coefs(lev, y0)
            cc = (1.0 - OMEGA) - C6 * nb
            if first:
                ca, cb = jnp.where(inside, C6 * (cc + 1.0), 0.0), jnp.where(inside, C6 * C6, 0.0)
            else:
                ca, cb = jnp.where(inside, cc, 0.0), jnp.where(inside, C6, 0.0)

            def block(k):
                c, s = stencil(src, lev.zs, k, y0, sums)
                z0 = lev.zs + SUB * k
                if not first:
                    s = s + rhs[pl.ds(z0, SUB), pl.ds(y0, SUB), :]
                dst[pl.ds(z0, SUB), pl.ds(y0, SUB), :] = ca * c + cb * s
            each(block)
            zghost_tile(lev, dst, y0)
        tiles(lev, src, (lev.ys, lev.zs, lev.nzb), lev.nyt, body)

    def residual_pass(lev, src, rhs):
        def body(y0, each, sums):
            _, nb = coefs(lev, y0)
            dd = 6.0 + nb

            def block(k):
                c, s = stencil(src, lev.oz, k, y0, sums)
                r = (rhs[pl.ds(lev.oz + SUB * k, SUB), pl.ds(y0, SUB), :] + (s - dd * c)).reshape(4, PAIR, SUB, LN)
                tr[pl.ds(4 * k, 4), pl.ds(pl.multiple_of(y0 - lev.oy, SUB), SUB), :] = r[:, 0] + r[:, 1]
            each(block)
        tiles(lev, src, (lev.oy, lev.oz, lev.n // SUB), lev.n // SUB, body)

    zface = jnp.where(pz == 0, LN, 1)
    zdst = LN + 1 - zface + jnp.where(pz == 0, -1, 1)
    yface = jnp.where(py == 0, 135, SUB)
    yghost = jnp.where(py == 0, 136, 7)

    def order(t):
        return jnp.where(py == 0, 15 - t, t)

    def pieces(buf, par, o):
        rows, yrows = pl.ds(tile(o), SUB), pl.ds(tile(o + 1), SUB)
        return (pltpu.make_async_remote_copy(src_ref=xs.at[par, rows, :], dst_ref=xg.at[par, rows, :], send_sem=xss.at[par, o],
                                             recv_sem=xrs.at[par, o], device_id=dev(1), device_id_type=MESH),
                pltpu.make_async_remote_copy(src_ref=buf.at[zface, yrows, :], dst_ref=buf.at[zdst, yrows, :],
                                             send_sem=zss.at[par, o], recv_sem=zrs.at[par, o], device_id=dev(4),
                                             device_id_type=MESH))

    def face_rows(par):
        return remote(yp.at[par], yg.at[par], par, PAIR)

    def send(buf, par, t):
        for copy in pieces(buf, par, order(t)):
            copy.start()

        def first():
            def take_rows(i):
                for j in range(SUB):
                    yp[par, pl.ds(SUB * i + j, 1), :] = buf[SUB * i + j + 1, pl.ds(yface, 1), :]
            loop(GRP, take_rows)
            face_rows(par).start()
        pl.when(t == 0)(first)

    def receive(buf, par, t):
        def first():
            face_rows(par).wait()

            def put_rows(i):
                for j in range(SUB):
                    buf[SUB * i + j + 1, pl.ds(yghost, 1), :] = yg[par, pl.ds(SUB * i + j, 1), :]
            loop(GRP, put_rows)
        pl.when(t == 0)(first)
        for copy in pieces(buf, par, order(t)):
            copy.wait()

    def roll_sums0(src, par, t, sx):
        rows = pl.ds(tile(t + 1), SUB)
        ghost = xg[par, pl.ds(tile(t), SUB), :]
        left = jnp.where(low_x, 0.0, ghost)
        right = jnp.where(low_x, ghost, 0.0)
        zlow = jnp.where(pz == 0, 1.0, 0.0)
        for k in range(GRP):
            z = SUB * k
            v = src[pl.ds(z, SUB + PAIR), rows, :]
            here = v[1:SUB + 1]
            a = jnp.where(skew == (z - 1) % LN, left[None], here) + v[0:SUB]
            b = jnp.where(skew == z, right[None], here) + v[PAIR:SUB + PAIR]
            s = pltpu.roll(a, 1, PAIR) + pltpu.roll(b, BACK, PAIR) - jnp.where(out_skew == z, here, 0.0)
            sx[pl.ds(z, SUB)] = s
        sx[0] = sx[0] - zlow * src[1, rows, :]
        sx[BACK] = sx[BACK] - (1.0 - zlow) * src[LN, rows, :]

    def cells0(src, t, z, sx):
        y0, planes = tile(t + 1), pl.ds(z + 1, GRP)
        s = sx[pl.ds(z, GRP)] + src[planes, pl.ds(y0 - 1, SUB), :] + src[planes, pl.ds(y0 + 1, SUB), :]
        return src[planes, pl.ds(y0, SUB), :], s + fr[pl.ds(z, GRP), pl.ds(tile(t), SUB), :]

    def yedge(t):
        r = row + tile(t + 1)
        return jnp.where((r == lev0.lo[1]) | (r == lev0.hi[1] - 1), 1.0, 0.0)

    def tiles0(src, par, work):
        receive(src, par, 0)
        roll_sums0(src, par, order(0), sx)

        def step(t):
            pl.when(t < 15)(lambda: receive(src, par, t + 1))

            def both(now, later):
                roll_sums0(src, par, order(t + 1 - (t + 1) // GRP), later)
                work(order(t), now)
            pl.when(t % PAIR == 0)(lambda: both(sx, sy))
            pl.when(t % PAIR == 1)(lambda: both(sy, sx))
            work_done(t)

        work_done = work.done
        loop(GRP, step)

    def sweep0(src, dst, par):
        def work(o, sums):
            cc = (1.0 - OMEGA) - C6 * yedge(o)
            pk = nil
            for k in range(SUB):
                c, s = cells0(src, o, GRP * k, sums)
                new = cc * c + C6 * s
                dst[pl.ds(GRP * k + 1, GRP), pl.ds(tile(o + 1), SUB), :] = new
                for j in range(GRP):
                    pk = jnp.where(face_lane == GRP * k + j, new[j], pk)
            xs[1 - par, pl.ds(tile(o), SUB), :] = pk
        work.done = lambda t: send(dst, 1 - par, t)
        tiles0(src, par, work)

    def residual0():
        def work(o, sums):
            dd = 6.0 + yedge(o)
            for k in range(SUB):
                c, s = cells0(ua, o, GRP * k, sums)
                ub[pl.ds(GRP * k + 1, GRP), pl.ds(tile(o + 1), SUB), :] = s - dd * c
        work.done = lambda t: None
        tiles0(ua, 0, work)

    def pair_sums(fine, j):
        for zc in range(fine.n // PAIR):
            lo, hi = pl.ds(GRP * j, SUB, stride=PAIR), pl.ds(GRP * j + 1, SUB, stride=PAIR)
            if fine.idx:
                s = tr[zc, lo, :] + tr[zc, hi, :]
                sx[zc] = 0.5 * (s + pltpu.roll(s, BACK, 1))
                continue
            lo, hi = pl.ds(GRP * j + SUB, SUB, stride=PAIR), pl.ds(GRP * j + SUB + 1, SUB, stride=PAIR)
            e = ub[PAIR * zc + 1, lo, :] + ub[PAIR * zc + 1, hi, :]
            o = ub[PAIR * zc + PAIR, lo, :] + ub[PAIR * zc + PAIR, hi, :]
            s = pltpu.roll(e, -PAIR * zc % LN, 1) + pltpu.roll(e + o, (-PAIR * zc - 1) % LN, 1)
            sx[zc] = 0.5 * (s + pltpu.roll(o, (-PAIR * zc - PAIR) % LN, 1))

    def restrict_to(fine, coarse, dst, pack=None):
        half = fine.n // PAIR
        own = (lane >= coarse.ox) & (lane < coarse.ox + half)
        idx = (fine.ox + PAIR * (lane - coarse.ox)) & BACK
        pidx = fine.ox + PAIR * (jnp.where(low_x, half - SUB, 0) + lane % SUB)
        group = lane // SUB
        step = half // PAIR

        def ytile(t):
            j = t if pack is None else jnp.where(py == 0, half // SUB - 1 - t, t)
            rows = pl.ds(pl.multiple_of(coarse.oy + SUB * j, SUB), SUB)
            pair_sums(fine, j)

            def move(q):
                pk = nil
                for i in range(step):
                    z = step * q + i
                    v = sx[z]
                    dst[coarse.oz + z, rows, :] = jnp.where(own, jnp.take_along_axis(v, idx, axis=1), 0.0)
                    if pack is not None:
                        pk = jnp.where(group == i % GRP, jnp.take_along_axis(v, pidx, axis=1), pk)
                        if i % GRP == GRP - 1:
                            pack[q * (step // GRP) + i // GRP, pl.ds(tile(j), SUB), :] = pk
            loop(PAIR, move)
            if pack is not None:
                copies = edge_pieces(coarse, dst, j)
                copies[0].start()

                def start_rest():
                    for copy in copies[1:]:
                        copy.start()
                pl.when(t == 0)(start_rest)
        loop(half // SUB, ytile)

    def wide_spans(lev):
        n, h = lev.n, HALO_PLANES[lev.idx]
        fy = pl.multiple_of(jnp.where(py == 0, lev.oy + n - SUB, lev.oy), SUB)
        hy = pl.multiple_of(jnp.where(py == 0, lev.oy - SUB, lev.oy + n), SUB)
        fz = jnp.where(pz == 0, lev.oz + n - h, lev.oz)
        hz = jnp.where(pz == 0, lev.oz - h, lev.oz + n)
        return fy, hy, pl.ds(fz, h), pl.ds(hz, h)

    def edge_pieces(lev, ref, j):
        fy, hy, fz, hz = wide_spans(lev)
        rows, own, k = pl.ds(pl.multiple_of(lev.oy + SUB * j, SUB), SUB), pl.ds(lev.oz, lev.n), lev.idx
        piece = pltpu.make_async_remote_copy(src_ref=ref.at[fz, rows, :], dst_ref=ref.at[hz, rows, :],
                                             send_sem=wss.at[k - 1, j], recv_sem=wrs.at[k - 1, j], device_id=dev(4),
                                             device_id_type=MESH)
        return (piece, remote(ref.at[own, pl.ds(fy, SUB), :], ref.at[own, pl.ds(hy, SUB), :], 4 * k + 3, PAIR),
                remote(ref.at[fz, pl.ds(fy, SUB), :], ref.at[hz, pl.ds(hy, SUB), :], 4 * k + 4, 6))

    def restrict_packed(fine, me):
        idx = fine.ox + PAIR * (lane % GRP)
        group = lane // GRP

        def ytile(j):
            pair_sums(fine, j)

            def collect(q):
                pk = nil
                for i in range(SUB):
                    pk = jnp.where(group == i, jnp.take_along_axis(sx[SUB * q + i], idx, axis=1), pk)
                g3[me, q, pl.ds(tile(j), SUB), :] = pk
            loop(PAIR, collect)
        loop(PAIR, ytile)

    def prolong_add(fine, coarse, esrc, dst, cbase):
        back_z = (fine.oz - fine.zs) // PAIR
        back_y = (fine.oy - fine.ys) // PAIR
        nct = fine.n // GRP + (0 if fine.nyt * SUB == fine.n else 1)
        cy_s = cbase[1] - PAIR * back_y
        fy_s = fine.oy - 4 * back_y
        cz_s = cbase[0] - back_z - 1
        ncz = 4 * fine.nzb + PAIR
        xf = lane - fine.ox
        half = lax.shift_right_arithmetic(xf, 1)
        odd = xf - PAIR * half
        i0 = half + cbase[PAIR]
        i1 = jnp.clip(i0 + PAIR * odd - 1, 0, BACK)
        i0 = jnp.clip(i0, 0, BACK)
        inx = (lane >= fine.lo[PAIR]) & (lane < fine.hi[PAIR])
        edge = (lane == fine.lo[PAIR]) | (lane == fine.hi[PAIR] - 1)
        wx = jnp.where(inx, jnp.where(edge, 0.5, 0.75), 0.0)
        wn = jnp.where(inx, 0.25, 0.0)

        def spread(z):
            for t in range(nct + PAIR):
                v = esrc[cz_s + z, pl.ds(pl.multiple_of(cy_s + SUB * (t - 1), SUB), SUB), :]
                xr[z, pl.ds(SUB * t, SUB), :] = (wx * jnp.take_along_axis(v, i0, axis=1)
                                                 + wn * jnp.take_along_axis(v, i1, axis=1))

        per = 6 if ncz % 6 == 0 else PAIR

        def spread_some(i):
            for q in range(per):
                spread(per * i + q)
        loop(ncz // per, spread_some)

        def ctile(t):
            fy = pl.multiple_of(fy_s + GRP * t, SUB)
            r = row + (cy_s + SUB * t)
            iny = (r >= coarse.lo[1]) & (r < coarse.hi[1])
            wny = jnp.where(iny, 0.25, 0.0)
            wde = jnp.where(iny, jnp.where(r == coarse.lo[1], 0.5, 0.75), 0.0)
            wdo = jnp.where(iny, jnp.where(r == coarse.hi[1] - 1, 0.5, 0.75), 0.0)

            def plane(i):
                for q in range(per):
                    z = per * i + q
                    e = xr[z, pl.ds(tile(t + 1), SUB), :]
                    tr[z, pl.ds(fy, SUB, stride=PAIR), :] = wde * e + wny * xr[z, pl.ds(tile(t + 1) - 1, SUB), :]
                    tr[z, pl.ds(fy + 1, SUB, stride=PAIR), :] = wdo * e + wny * xr[z, pl.ds(tile(t + 1) + 1, SUB), :]
            loop(ncz // per, plane)
        loop(nct, ctile)

        def ytile(t):
            o = t if fine.idx else order(t)
            y0 = pl.multiple_of(fine.ys + SUB * o, SUB)
            rows = pl.ds(y0, SUB)
            pk = nil
            for k in range(fine.nzb):
                z0 = fine.zs + SUB * k
                tb = tr[pl.ds(4 * k, 6), rows, :]
                mid = 0.75 * tb[1:5]
                add = jnp.stack([mid + 0.25 * tb[0:4], mid + 0.25 * tb[PAIR:6]], axis=1).reshape(SUB, SUB, LN)
                if fine.idx:
                    dst[pl.ds(z0, SUB), rows, :] = dst[pl.ds(z0, SUB), rows, :] + add
                    continue
                for j in range(SUB):
                    z = SUB * k + j
                    new = dst[1 + z, rows, :] + pltpu.roll(add[j], z, 1)
                    dst[1 + z, rows, :] = new
                    pk = jnp.where(face_lane == z, new, pk)
            if fine.idx:
                zghost_tile(fine, dst, y0)
            else:
                xs[0, pl.ds(tile(o), SUB), :] = pk
                send(dst, 0, t)
        loop(fine.nyt, ytile)

    def exchange_wide(lev, ref, sendp, recvp, sendh, recvh):
        n, h, k = lev.n, HALO_PLANES[lev.idx], lev.idx
        hy = pl.multiple_of(jnp.where(py == 0, lev.oy + n, lev.oy - SUB), SUB)
        hz = jnp.where(pz == 0, lev.oz + n, lev.oz - h)
        cx = remote(sendp, recvp, 4 * k + 1, 1)
        cx.start()
        for copy in edge_pieces(lev, ref, 0)[1:]:
            copy.wait()
        loop(n // SUB, lambda j: edge_pieces(lev, ref, j)[0].wait())
        group = lane // SUB
        face = jnp.where(low_x, lev.ox + n - SUB, lev.ox)
        halo = jnp.where(low_x, lev.ox + n, lev.ox - SUB)
        inh = (lane >= halo) & (lane < halo + SUB)

        def spots(q):
            return pl.ds(pl.multiple_of(jnp.where(q < n // SUB, lev.oy + SUB * q, hy), SUB), SUB)

        def gather_faces(z, planes, rows):
            pk = nil
            for i in range(planes):
                pk = jnp.where(group == i, pltpu.roll(ref[z + i, rows, :], (SUB * i - face) & BACK, 1), pk)
            return pk
        nq = n // GRP

        def collect_y(q):
            sendh[q] = gather_faces(lev.oz + GRP * q, GRP, pl.ds(hy, SUB))

        def collect_z(q):
            sendh[nq + q] = gather_faces(hz, h, spots(q))
        zper = 3 if n // SUB == SUB else n // SUB + 1
        several(nq, PAIR, collect_y)
        several(n // SUB + 1, zper, collect_z)
        ch = remote(sendh, recvh, 4 * k + PAIR, 1)
        ch.start()
        cx.wait()

        def put(pk, z, planes, rows):
            pk = pltpu.roll(pk, halo, 1)
            for i in range(planes):
                ref[z + i, rows, :] = jnp.where(inh, pltpu.roll(pk, (-SUB * i) % LN, 1), ref[z + i, rows, :])

        def ytile(t):
            rows = pl.ds(pl.multiple_of(lev.oy + SUB * t, SUB), SUB)
            for q in range(nq):
                put(recvp[q, pl.ds(tile(t), SUB), :], lev.oz + GRP * q, GRP, rows)
        loop(n // SUB, ytile)
        ch.wait()

        several(nq, PAIR, lambda q: put(recvh[q], lev.oz + GRP * q, GRP, pl.ds(hy, SUB)))
        several(n // SUB + 1, zper, lambda q: put(recvh[nq + q], hz, h, spots(q)))
        zghost(lev, ref)

    me = 4 * pz + PAIR * py + px

    def gather3():
        copies = [remote(g3.at[me], g3.at[me], 13 + code, code) for code in range(1, SUB)]
        for c in copies:
            c.start()
        for c in copies:
            c.wait()
        lev = levels[3]
        in_lo = (lane >= lev.ox) & (lane < lev.ox + GRP)
        in_hi = (lane >= lev.ox + GRP) & (lane < lev.ox + 32)

        def ytile(t):
            rows = pl.ds(pl.multiple_of(lev.oy + SUB * t, SUB), SUB)
            by = t // PAIR
            r0 = pl.ds(tile(t % PAIR), SUB)
            for q in range(4):
                lo = g3[4 * (q // PAIR) + PAIR * by, q % PAIR, r0, :]
                hi = g3[4 * (q // PAIR) + PAIR * by + 1, q % PAIR, r0, :]
                for i in range(SUB):
                    a = pltpu.roll(lo, (lev.ox - GRP * i) % LN, 1)
                    b = pltpu.roll(hi, (lev.ox + GRP - GRP * i) % LN, 1)
                    b3[lev.oz + SUB * q + i, rows, :] = jnp.where(in_lo, a, jnp.where(in_hi, b, 0.0))
        loop(4, ytile)
        zghost(lev, b3)

    def coarse_solve():
        lev = levels[5]

        def zstep(z, acc):
            b = b5[lev.oz + z, pl.ds(lev.oy, SUB), :] * 64.0
            acc = list(acc)
            for x in range(SUB):
                col = jnp.broadcast_to(b[:, lev.ox + x:lev.ox + x + 1], (SUB, LN))
                for j in range(4):
                    acc[j] = acc[j] + cinv[j, pl.ds(z * 64 + x, SUB, stride=SUB), :] * col
            return tuple(acc)
        acc = lax.fori_loop(0, SUB, zstep, (jnp.zeros((SUB, LN), F32),) * 4)
        lines = [jnp.broadcast_to(jnp.sum(a, axis=0, keepdims=True), (SUB, LN)) for a in acc]
        own = (lane >= lev.ox) & (lane < lev.ox + SUB)
        for z in range(SUB):
            idx = jnp.clip((z % PAIR) * 64 + row * SUB + lane - lev.ox, 0, 127)
            e5[lev.oz + z, pl.ds(lev.oy, SUB), :] = jnp.where(own, jnp.take_along_axis(lines[z // PAIR], idx, axis=1), 0.0)
        zghost(lev, e5)

    def base_of(lev):
        return (lev.oz, lev.oy, lev.ox)

    def local_visit(fine, v, w, rhs, descend, ecoarse, coarse, cbase):
        sweep(fine, rhs, v, None)
        zghost(fine, v)
        residual_pass(fine, v, rhs)
        descend()
        prolong_add(fine, coarse, ecoarse, v, cbase)
        sweep(fine, v, w, rhs)
        sweep(fine, w, v, rhs)

    def descend4():
        restrict_to(levels[4], levels[5], b5)
        coarse_solve()

    def descend3():
        restrict_to(levels[3], levels[4], b4)
        zghost(levels[4], b4)
        local_visit(levels[4], v4, w4, b4, descend4, e5, levels[5], base_of(levels[5]))

    def descend2():
        restrict_packed(levels[PAIR], me)
        gather3()
        local_visit(levels[3], v3, w3, b3, descend3, v4, levels[4], base_of(levels[4]))

    def descend1():
        restrict_to(levels[1], levels[PAIR], b2, p2s)
        exchange_wide(levels[PAIR], b2, p2s, p2r, h2s, h2r)
        oz, oy, ox = base_of(levels[3])
        local_visit(levels[PAIR], v2, w2, b2, descend2, v3, levels[3], (oz + GRP * pz, oy + GRP * py, ox + GRP * px))

    def skew_in(t):
        o = order(t)
        for copy in load(o):
            copy.wait()
        rows, frows = pl.ds(tile(o + 1), SUB), pl.ds(tile(o), SUB)
        pk = nil
        for z in range(LN):
            moved = pltpu.roll(ua[z + 1, rows, :], z, 1)
            ua[z + 1, rows, :] = moved
            pk = jnp.where(face_lane == z, moved, pk)
            fr[z, frows, :] = pltpu.roll(fr[z, frows, :] * INV_G2, z, 1)
        xs[0, frows, :] = pk
        send(ua, 0, t)
    loop(GRP, skew_in)
    for copy in load_c:
        copy.wait()

    def correct():
        residual0()
        restrict_to(lev0, levels[1], b1, p1s)
        exchange_wide(levels[1], b1, p1s, p1r, h1s, h1r)
        local_visit(levels[1], v1, w1, b1, descend1, v2, levels[PAIR], base_of(levels[PAIR]))
        prolong_add(lev0, levels[1], v1, ua, base_of(levels[1]))

    def half_cycle(h):
        sweep0(ua, ub, 0)
        sweep0(ub, ua, 1)
        pl.when(h % PAIR == 0)(correct)
    loop(PAIR * CYCLES, half_cycle)

    def store(t):
        return pltpu.make_async_copy(ub.at[pl.ds(1, LN), pl.ds(tile(t + 1), SUB), :], out_hbm.at[:, pl.ds(tile(t), SUB), :],
                                     lsem.at[t])

    def skew_out(t):
        rows = pl.ds(tile(t + 1), SUB)
        for z in range(LN):
            ub[z + 1, rows, :] = pltpu.roll(ua[z + 1, rows, :], -z % LN, 1)
        store(t).start()
    loop(GRP, skew_out)
    loop(GRP, lambda t: receive(ua, 0, t))
    loop(GRP, lambda t: store(t).wait())


def solution(mesh):
    grid_spec = P(('batch', 'gz'), 'gy', 'gx')

    def vmem(*shape):
        return pltpu.VMEM(shape, F32)

    scratch = [vmem(130, 144, LN), vmem(130, 144, LN), vmem(LN, LN, LN), vmem(66, 144, LN), vmem(66, 80, LN), vmem(LN, SUB, LN), vmem(LN, SUB, LN)]
    for shape in ((82, 96), (50, 64), (34, 72), (18, 48)):
        scratch += [vmem(*shape, LN)] * 3
    scratch += [vmem(10, 32, LN), vmem(10, 32, LN), vmem(4, 512, LN)]
    scratch += [vmem(PAIR, LN, LN)] * 4
    scratch += [vmem(4, 64, LN)] * PAIR + [vmem(PAIR, 32, LN)] * PAIR
    scratch += [vmem(13, SUB, LN)] * PAIR + [vmem(7, SUB, LN)] * PAIR + [vmem(SUB, PAIR, GRP, LN)]
    scratch += [pltpu.SemaphoreType.DMA((22,)), pltpu.SemaphoreType.DMA((22,))]
    scratch += [pltpu.SemaphoreType.DMA((PAIR, GRP))] * 6 + [pltpu.SemaphoreType.DMA((36,))]

    call = pl.pallas_call(
        solve_kernel,
        out_shape=jax.ShapeDtypeStruct((LN, LN, LN), F32),
        in_specs=[pl.BlockSpec(memory_space=pl.ANY)] * 3,
        out_specs=pl.BlockSpec(memory_space=pl.ANY),
        scratch_shapes=scratch,
        name='multigrid',
        compiler_params=pltpu.CompilerParams(collective_id=0, has_side_effects=True, vmem_limit_bytes=67043328),
    )
    return jax.shard_map(call, mesh=mesh, in_specs=(grid_spec, grid_spec, P()), out_specs=grid_spec, check_vma=False)
```
